128 devices in a mesh: seq: 16 (over x_lo, y, core), hid: 8 (over x_hi, z).
Axes of the slice: x: 4 (x_hi: 2, x_lo: 2; x = x_hi * 2 + x_lo), y: 4, z: 4, core: 2. Of those that a mesh axis runs over, the one named last changes fastest.
Arguments:
- hidden: bfloat16 [8192, 4096], P('seq', 'hid'), may hold values from -6 to 6
- w_in: bfloat16 [2, 4096, 1024], P(None, 'hid'), may hold values from -0.09863281 to 0.09863281
- embedding: bfloat16 [1, 2048, 1024], replicated, may hold values from -6 to 6
- depth_gain: float32 [2, 1024], replicated, may hold values from 0.25 to 1.75
- w_out: bfloat16 [1024, 2, 2048], P(('seq', 'hid')), may hold values from -0.43554688 to 0.43554688
- codebook_ids: int32 [2, 8192], P(None, ('seq', 'hid')), may hold values from 0 to 2047
Outputs:
- grad_hidden: bfloat16 [8192, 4096], P('seq', 'hid')
- grad_in: float32 [2, 4096, 1024], P(None, 'hid', 'seq')
- grad_out: float32 [1024, 2, 2048], P(('seq', 'hid'))
The draws below stay inside these ranges and needn't reach their ends.
All inputs are finite; a program needn't handle non-finite values.
Results may differ from the reference program's by a relative error of at most 0.01.
Values may be sent and summed in bfloat16 or wider, within the bound.
A program may use at most 128 MiB of HBM per device.

```python
import jax
import jax.numpy as jnp
from jax import lax

DT = 4096
DD = 1024
CARD = 2048
STEPS = 2
FRAMES = 8192


def draw_hidden(key, part):
    values = jnp.clip(jax.random.normal(jax.random.fold_in(key, 11), (FRAMES, DT), jnp.float32), -6.0, 6.0)
    return values.astype(jnp.bfloat16)


def draw_w_in(key, part):
    values = jnp.clip(jax.random.normal(jax.random.fold_in(key, 21), (STEPS, DT, DD), jnp.float32), -6.0, 6.0) * DT ** (-0.5)
    return values.astype(jnp.bfloat16)


def draw_embedding(key, part):
    values = jnp.clip(jax.random.normal(jax.random.fold_in(key, 41), (STEPS - 1, CARD, DD), jnp.float32), -6.0, 6.0)
    return values.astype(jnp.bfloat16)


def draw_w_out(key, part):
    values = jnp.clip(jax.random.normal(jax.random.fold_in(key, 31), (DD, STEPS, CARD), jnp.float32), -6.0, 6.0) * DD ** (-0.5)
    return values.astype(jnp.bfloat16)


def touch_ends(values, stream_key, smallest, top_value):
    longest = values.shape.index(max(values.shape))
    spots = []
    for shift in (0, 1):
        where = [jax.random.randint(jax.random.fold_in(stream_key, axis), (), 0, length) for axis, length in enumerate(values.shape)]
        where[longest] = (where[longest] + shift) % values.shape[longest]
        spots.append(tuple(where))
    return values.at[spots[0]].set(smallest).at[spots[1]].set(top_value)


def setup_inputs(seed: int = 0) -> dict:
    seeds = jax.random.split(jax.random.key(seed), 7)
    return {
        "hidden": draw_hidden(jax.random.fold_in(seeds[6], 71), 0),
        "w_in": draw_w_in(jax.random.fold_in(seeds[6], 71), 0),
        "embedding": draw_embedding(jax.random.fold_in(seeds[6], 71), 0),
        "depth_gain": jnp.clip(1.0 + 0.15 * jax.random.normal(seeds[3], (STEPS, DD), jnp.float32), 0.25, 1.75),
        "w_out": draw_w_out(jax.random.fold_in(seeds[6], 71), 0),
        "codebook_ids": touch_ends(jax.random.randint(seeds[5], (STEPS, FRAMES), 0, CARD), jax.random.fold_in(seeds[5], 1), 0, CARD - 1).astype(jnp.int32),
    }


def reference(hidden, w_in, embedding, depth_gain, w_out, codebook_ids):
    hidden_f = hidden.astype(jnp.float32)
    squares = lax.optimization_barrier(jnp.sum(hidden_f * hidden_f, axis=1))
    ratio = lax.rsqrt(squares / DT + 1e-06)
    proj = jnp.einsum('fd,kde->fke', hidden_f, w_in.astype(jnp.float32))
    x_rows = ratio[:, None, None] * proj
    for step in range(1, STEPS):
        looked = jnp.take(embedding[step - 1], codebook_ids[step - 1], axis=0).astype(jnp.float32)
        x_rows = x_rows.at[:, step].add(looked)
    scale = lax.rsqrt(lax.optimization_barrier(jnp.mean(x_rows * x_rows, axis=2, keepdims=True)) + 1e-06)
    normed = (x_rows * scale * depth_gain[None]).astype(jnp.bfloat16)
    logits = jnp.einsum('fkd,dkc->fkc', normed.astype(jnp.float32), w_out.astype(jnp.float32))
    targets = codebook_ids.T
    lse = jax.nn.logsumexp(logits, axis=2)
    onehot = (targets[:, :, None] == jnp.arange(CARD, dtype=jnp.int32)[None, None, :]).astype(jnp.float32)
    loss_weight = 2.0 * CARD / FRAMES
    d_logit = ((jnp.exp(logits - lse[:, :, None]) - onehot) * loss_weight).astype(jnp.bfloat16)
    grad_out = jnp.einsum('fkd,fkc->dkc', normed.astype(jnp.float32), d_logit.astype(jnp.float32))
    d_norm = jnp.einsum('fkc,dkc->fkd', d_logit.astype(jnp.float32), w_out.astype(jnp.float32))
    gated = depth_gain[None] * d_norm
    d_x = scale * gated - x_rows * scale ** 3 * lax.optimization_barrier(jnp.mean(gated * x_rows, axis=2, keepdims=True))
    d_round = d_x.astype(jnp.bfloat16)
    d_ratio = lax.optimization_barrier(jnp.sum(d_x * proj, axis=(1, 2)))
    scaled = (ratio[:, None, None] * d_round.astype(jnp.float32)).astype(jnp.bfloat16)
    grad_in = jnp.einsum('fd,fke->kde', hidden_f, scaled.astype(jnp.float32))
    back = jnp.einsum('fke,kde->fd', d_round.astype(jnp.float32), w_in.astype(jnp.float32))
    grad_hidden = (ratio[:, None] * back - (ratio ** 3 * d_ratio / DT)[:, None] * hidden_f).astype(jnp.bfloat16)
    return (grad_hidden, grad_in, grad_out)
```

```python
import functools

import jax
import jax.numpy as jnp
from jax import lax
from jax.experimental import pallas as pl
from jax.experimental.pallas import tpu as pltpu
from jax.sharding import PartitionSpec as P

MESH = pl.DeviceIdType.MESH
BF = jnp.bfloat16
F32 = jnp.float32


def place():
    s, h = lax.axis_index("seq"), lax.axis_index("hid")
    x_lo, y, c = lax.div(s, 8), lax.rem(lax.div(s, 2), 4), lax.rem(s, 2)
    return 2 * lax.div(h, 4) + x_lo, y, lax.rem(h, 4), c


def device(x, y, z, c):
    x, y, z, c = lax.rem(x, 4), lax.rem(y, 4), lax.rem(z, 4), lax.rem(c, 2)
    return (lax.rem(x, 2) * 8 + y * 2 + c, lax.div(x, 2) * 4 + z)


def greet(peers):
    barrier = pltpu.get_barrier_semaphore()
    for peer in peers:
        pl.semaphore_signal(barrier, inc=1, device_id=peer, device_id_type=MESH)
    pl.semaphore_wait(barrier, len(peers))


class Post:
    def __init__(self, send_sem, recv_sem):
        self.send_sem, self.recv_sem, self.copies = send_sem, recv_sem, []

    def send(self, src, dst, peer):
        i = len(self.copies)
        copy = pltpu.make_async_remote_copy(
            src_ref=src,
            dst_ref=dst,
            send_sem=self.send_sem.at[i],
            recv_sem=self.recv_sem.at[i],
            device_id=peer,
            device_id_type=MESH,
        )
        copy.start()
        self.copies.append(copy)
        return copy

    def close(self):
        for copy in self.copies:
            copy.wait_send()


def forward_kernel(
    hidden, w_in, w_rows, ids, proj, sq_all, w_full, ids_all,
    part, got, w_pair, sq_mine, send_sem, recv_sem,
):
    x, y, z, c = place()
    x_lo, x_hi, step, zh = lax.rem(x, 2), lax.div(x, 2), lax.rem(z, 2), lax.div(z, 2)
    pair = device(x, y, z + 1 - 2 * step, c)
    across = device(x, y, z + 2, c)
    twin = device(x, y, z, c + 1)
    hid_peers = [(dx, dz) for dz in (2, 1, 3, 0) for dx in (2, 0) if (dx, dz) != (0, 0)]
    greet(
        [device(x + dx, y, z + dz, c) for dx, dz in hid_peers]
        + [device(x + d, y, z, c) for d in (1, 3)]
        + [device(x, y + d, z, c) for d in (1, 2, 3)]
        + [twin]
    )
    post = Post(send_sem, recv_sem)
    hid = x_hi * 4 + z

    w_swap = post.send(w_rows.at[1 - step], w_pair, pair)
    ids_swap = post.send(ids, ids_all.at[step], pair)
    ids_all[step] = ids[...]

    h = hidden[...].astype(F32)
    h2 = h * h
    top = h2.astype(BF)
    low = (h2 - top.astype(F32)).astype(BF)
    ones = jnp.ones((8, h2.shape[1]), BF)
    dims = (((1,), (1,)), ((), ()))
    sq_mine[...] = lax.dot_general(ones, top, dims, preferred_element_type=F32) + lax.dot_general(
        ones, low, dims, preferred_element_type=F32
    )
    sq_all[hid] = sq_mine[...]
    sq_copies = [
        post.send(sq_mine, sq_all.at[hid], device(x + dx, y, z + dz, c)) for dx, dz in hid_peers
    ]

    chunk_copies = []

    def chunk(dz):
        to_z = lax.rem(z + dz, 4)
        to_step, to_zh = lax.rem(to_z, 2), lax.div(to_z, 2)
        rows = [
            hidden[pl.ds(pl.multiple_of((fx * 2 + to_zh) * 128, 128), 128), :] for fx in range(2)
        ]
        product = jnp.dot(
            jnp.concatenate(rows, axis=0), w_in[to_step], preferred_element_type=F32
        ).astype(BF)
        part[dz, 0] = product[:128]
        part[dz, 1] = product[128:]
        for dx in (2, 0):
            if (dx, dz) == (0, 0):
                continue
            fx = 1 - x_hi if dx == 2 else x_hi
            slot = len(chunk_copies)
            chunk_copies.append(
                post.send(part.at[dz, fx], got.at[slot], device(x + dx, y, z + dz, c))
            )

    chunk(2)
    w_swap.wait_recv()
    mine = w_rows[step].astype(F32)
    other = w_pair[...].astype(F32)
    first = jnp.where(step == 0, mine, other)
    second = jnp.where(step == 0, other, mine)
    w_full[x_lo, y, c, x_hi, zh] = jnp.concatenate([first, second], axis=0).astype(BF)
    block = w_full.at[x_lo, y, c, x_hi, zh]
    w_across = post.send(block, block, across)
    w_x = [post.send(block, block, device(x + d, y, z, c)) for d in (1, 3, 2)]
    chunk(1)
    chunk(3)
    w_across.wait_recv()
    block = w_full.at[x_lo, y, c, x_hi, 1 - zh]
    w_x += [post.send(block, block, device(x + d, y, z, c)) for d in (1, 3, 2)]
    chunk(0)
    for copy in w_x:
        copy.wait_recv()
    line = w_full.at[:, y, c]
    w_y = [post.send(line, line, device(x, y + d, z, c)) for d in (2, 1, 3)]
    w_c = [post.send(line, line, twin)]

    for copy in chunk_copies:
        copy.wait_recv()
    total = part[0, x_hi].astype(F32)
    for slot in range(7):
        total = total + got[slot].astype(F32)
    proj[...] = total
    ids_swap.wait_recv()
    for copy in sq_copies:
        copy.wait_recv()

    for d, copy in zip((1, 3, 2), (w_y[1], w_y[2], w_y[0])):
        copy.wait_recv()
        line = w_full.at[:, lax.rem(y + 4 - d, 4), c]
        w_c.append(post.send(line, line, twin))
    for copy in w_c:
        copy.wait_recv()
    post.close()


def return_kernel(
    d_rows, small, partial, d_all, small_all, summed, c_got, y_out, y_got, send_sem, recv_sem
):
    x, y, z, c = place()
    x_hi, step, zh = lax.div(x, 2), lax.rem(z, 2), lax.div(z, 2)
    twin = device(x, y, z, c + 1)
    hid_peers = [(dx, dz) for dz in (2, 1, 3, 0) for dx in (2, 0) if (dx, dz) != (0, 0)]
    greet(
        [device(x + dx, y, z + dz, c) for dx, dz in hid_peers]
        + [device(x, y + d, z, c) for d in (1, 2, 3)]
        + [twin]
    )
    post = Post(send_sem, recv_sem)
    hid = x_hi * 4 + z
    c_swap = [
        post.send(
            partial.at[:, lax.rem(y + d, 4), 1 - c], c_got.at[:, lax.rem(y + d, 4)], twin
        )
        for d in (2, 1, 3, 0)
    ]
    rows_copies = []
    for dx, dz in hid_peers:
        peer = device(x + dx, y, z + dz, c)
        rows_copies.append(post.send(d_rows, d_all.at[step, x_hi, zh], peer))
        rows_copies.append(post.send(small, small_all.at[hid], peer))
    d_all[step, x_hi, zh] = d_rows[...]
    small_all[hid] = small[...]

    y_copies = []
    for i, d in enumerate((2, 1, 3)):
        c_swap[i].wait_recv()
        to_y = lax.rem(y + d, 4)

        @pl.loop(0, 8)
        def add(j):
            a, b, e = lax.div(j, 4), lax.rem(lax.div(j, 2), 2), lax.rem(j, 2)
            y_out[i, a, b, e] = (
                partial[a, to_y, c, b, e].astype(F32) + c_got[a, to_y, b, e].astype(F32)
            ).astype(BF)

        y_copies.append(post.send(y_out.at[i], y_got.at[i], device(x, y + d, z, c)))
    c_swap[3].wait_recv()
    for copy in rows_copies:
        copy.wait_recv()
    for copy in y_copies:
        copy.wait_recv()

    @pl.loop(0, 8)
    def total(j):
        a, b, e = lax.div(j, 4), lax.rem(lax.div(j, 2), 2), lax.rem(j, 2)
        value = partial[a, y, c, b, e].astype(F32) + c_got[a, y, b, e].astype(F32)
        for i in range(3):
            value = value + y_got[i, a, b, e].astype(F32)
        summed[a, b, e] = value.astype(BF)

    post.close()


def last_kernel(
    in_part, out_part, grad_in, grad_out,
    c_got, y_out, y_got, x_out, x_got, gx_got, z_out, z_got, rows, send_sem, recv_sem,
):
    x, y, z, c = place()
    x_lo, x_hi, step, zh = lax.rem(x, 2), lax.div(x, 2), lax.rem(z, 2), lax.div(z, 2)
    twin = device(x, y, z, c + 1)
    pair = device(x, y, z + 1 - 2 * step, c)
    across = device(x, y, z + 2, c)
    beside = device(x + 1 - 2 * x_lo, y, z, c)
    greet(
        [device(x + d, y, z, c) for d in (1, 2, 3)]
        + [device(x, y + d, z, c) for d in (1, 2, 3)]
        + [twin, pair, across]
    )
    post = Post(send_sem, recv_sem)
    c_swap = [
        post.send(
            in_part.at[:, :, lax.rem(y + d, 4), 1 - c], c_got.at[:, :, lax.rem(y + d, 4)], twin
        )
        for d in (2, 1, 3, 0)
    ]
    gx = []
    for i, d in enumerate((2, 1, 3)):
        to_x = lax.rem(x + d, 4)
        gx.append(
            post.send(
                out_part.at[lax.rem(to_x, 2), lax.div(to_x, 2)],
                gx_got.at[i],
                device(x + d, y, z, c),
            )
        )
    y_copies = []
    for i, d in enumerate((2, 1, 3)):
        c_swap[i].wait_recv()
        to_y = lax.rem(y + d, 4)

        @pl.loop(0, 4)
        def add(j):
            a, b = lax.div(j, 2), lax.rem(j, 2)
            y_out[i, a, b] = (
                in_part[a, b, to_y, c].astype(F32) + c_got[a, b, to_y].astype(F32)
            ).astype(BF)

        y_copies.append(post.send(y_out.at[i], y_got.at[i], device(x, y + d, z, c)))
    for copy in gx:
        copy.wait_recv()

    def block(e):
        value = out_part[x_lo, x_hi, e].astype(F32)
        for i in range(3):
            value = value + gx_got[i, e].astype(F32)
        return value

    z_out[...] = block(1 - zh).astype(BF)
    gz = post.send(z_out, z_got, across)
    c_swap[3].wait_recv()
    gz.wait_recv()
    rows[...] = block(zh) + z_got[...].astype(F32)
    theirs = rows.at[pl.ds(pl.multiple_of((1 - step) * 8, 8), 8), :]
    gp = post.send(theirs, grad_out.at[step], pair)
    grad_out[step] = rows[pl.ds(pl.multiple_of(step * 8, 8), 8), :]
    for copy in y_copies:
        copy.wait_recv()

    def line(a, b):
        value = in_part[a, b, y, c].astype(F32) + c_got[a, b, y].astype(F32)
        for i in range(3):
            value = value + y_got[i, a, b].astype(F32)
        return value

    for a in range(2):
        x_out[a] = line(a, 1 - x_lo).astype(BF)
    gi = post.send(x_out, x_got, beside)
    for a in range(2):
        grad_in[a] = line(a, x_lo)
    gi.wait_recv()
    for a in range(2):
        grad_in[a] = grad_in[a] + x_got[a].astype(F32)
    gp.wait_recv()
    post.close()


def call(kernel, index, outs, scratch, copies, *args):
    vmem = pl.BlockSpec(memory_space=pltpu.VMEM)
    return pl.pallas_call(
        kernel,
        out_shape=[jax.ShapeDtypeStruct(shape, dtype) for shape, dtype in outs],
        in_specs=[vmem] * len(args),
        out_specs=[vmem] * len(outs),
        scratch_shapes=[pltpu.VMEM(shape, dtype) for shape, dtype in scratch]
        + [pltpu.SemaphoreType.DMA((copies,))] * 2,
        compiler_params=pltpu.CompilerParams(
            collective_id=index, has_side_effects=True, vmem_limit_bytes=60 * 1024 * 1024
        ),
        name=kernel.__name__,
    )(*args)


def shards(hidden, w_in, embedding, depth_gain, w_out, codebook_ids):
    hid_count = lax.axis_size("hid")
    seq_count = lax.axis_size("seq")
    hid = lax.axis_index("hid")
    step = lax.rem(hid, 2)
    quarter = lax.div(hid, 2)
    width_in = hidden.shape[1] * hid_count
    depth = w_in.shape[2]
    entries = w_out.shape[2]
    frames = hidden.shape[0]
    own = codebook_ids.shape[1]
    owned = 2 * own

    ids = jnp.pad(codebook_ids, ((0, 6), (0, 128 - own)))
    proj, sq_all, w_full, ids_all = call(
        forward_kernel,
        0,
        [
            ((owned, depth), F32),
            ((8, 8, frames), F32),
            ((2, 4, 2, 2, 2, 16, entries), BF),
            ((2, 8, 128), jnp.int32),
        ],
        [
            ((4, 2, owned, depth), BF),
            ((7, owned, depth), BF),
            ((8, entries), BF),
            ((8, frames), F32),
        ],
        30,
        hidden,
        w_in,
        jnp.transpose(w_out, (1, 0, 2)),
        ids,
    )
    ids_own = jnp.concatenate([ids_all[0, :2, :own], ids_all[1, :2, :own]], axis=1)
    ratio_all = lax.rsqrt(jnp.sum(sq_all[:, 0, :], axis=0) / width_in + 1e-06)
    ratio = lax.dynamic_slice(ratio_all, (quarter * owned,), (owned,))
    looked = jnp.take(embedding[0], ids_own[0], axis=0).astype(F32)
    x_rows = ratio[:, None] * proj + jnp.where(step == 1, looked, 0.0)
    gain = lax.dynamic_slice(depth_gain, (step, 0), (1, depth))
    scale = lax.rsqrt(jnp.mean(x_rows * x_rows, axis=1, keepdims=True) + 1e-06)
    normed = (x_rows * scale * gain).astype(BF)
    head = w_full.reshape(depth, entries)
    logits = jnp.einsum("fd,dc->fc", normed, head, preferred_element_type=F32)
    targets = jnp.where(step == 1, ids_own[1], ids_own[0])
    lse = jax.nn.logsumexp(logits, axis=1)
    onehot = (targets[:, None] == jnp.arange(entries, dtype=jnp.int32)[None, :]).astype(F32)
    loss_weight = 2.0 * entries / (frames * seq_count)
    d_logit = ((jnp.exp(logits - lse[:, None]) - onehot) * loss_weight).astype(BF)
    out_part = jnp.einsum("fd,fc->dc", normed, d_logit, preferred_element_type=F32).astype(BF)
    d_norm = jnp.einsum("fc,dc->fd", d_logit, head, preferred_element_type=F32)
    gated = gain * d_norm
    d_x = scale * gated - x_rows * scale**3 * jnp.mean(gated * x_rows, axis=1, keepdims=True)
    d_ratio = jnp.sum(d_x * proj, axis=1)
    small = jnp.broadcast_to(d_ratio[None, :], (8, owned))

    d_all, small_all, out_sum = call(
        return_kernel,
        1,
        [
            ((2, 2, 2, owned, depth), BF),
            ((8, 8, owned), F32),
            ((2, 2, 2, 16, entries), BF),
        ],
        [
            ((2, 4, 2, 2, 16, entries), BF),
            ((3, 2, 2, 2, 16, entries), BF),
            ((3, 2, 2, 2, 16, entries), BF),
        ],
        24,
        d_x.astype(BF),
        small,
        out_part.reshape(2, 4, 2, 2, 2, 16, entries),
    )
    d_all = d_all.reshape(2, frames, depth)
    d_ratio_all = small_all[:, 0, :].reshape(4, 2, owned).sum(axis=1).reshape(frames)
    correction = ratio_all**3 * d_ratio_all / width_in
    scaled = (ratio_all[None, :, None] * d_all.astype(F32)).astype(BF)
    in_part = jnp.einsum("kfe,fd->ked", scaled, hidden, preferred_element_type=F32).astype(BF)
    back = jnp.einsum("kfe,kde->fd", d_all, w_in, preferred_element_type=F32)
    grad_hidden = (
        ratio_all[:, None] * back - correction[:, None] * hidden.astype(F32)
    ).astype(BF)

    units = hidden.shape[1]
    grad_in, grad_out = call(
        last_kernel,
        2,
        [((2, 64, units), F32), ((2, 8, entries), F32)],
        [
            ((2, 2, 4, 64, units), BF),
            ((3, 2, 2, 64, units), BF),
            ((3, 2, 2, 64, units), BF),
            ((2, 64, units), BF),
            ((2, 64, units), BF),
            ((3, 2, 16, entries), BF),
            ((16, entries), BF),
            ((16, entries), BF),
            ((16, entries), F32),
        ],
        16,
        in_part.reshape(2, 2, 4, 2, 64, units),
        out_sum,
    )
    return (
        grad_hidden,
        jnp.transpose(grad_in, (0, 2, 1)),
        jnp.transpose(grad_out, (1, 0, 2)),
    )


def solution(mesh):
    placed = (
        P("seq", "hid"),
        P(None, "hid", None),
        P(),
        P(),
        P(("seq", "hid"), None, None),
        P(None, ("seq", "hid")),
    )
    return jax.shard_map(
        shards,
        mesh=mesh,
        in_specs=placed,
        out_specs=(P("seq", "hid"), P(None, "hid", "seq"), P(("seq", "hid"), None, None)),
        check_vma=False,
    )
```

```python
import functools

import jax
import jax.numpy as jnp
from jax import lax
from jax.experimental import pallas as pl
from jax.experimental.pallas import tpu as pltpu
from jax.sharding import PartitionSpec as P

MESH = pl.DeviceIdType.MESH
BF = jnp.bfloat16
F32 = jnp.float32
NT = (((1,), (1,)), ((), ()))


def place():
    s, h = lax.axis_index("seq"), lax.axis_index("hid")
    x_lo, y, c = lax.div(s, 8), lax.rem(lax.div(s, 2), 4), lax.rem(s, 2)
    return 2 * lax.div(h, 4) + x_lo, y, lax.rem(h, 4), c


def device(x, y, z, c):
    x, y, z, c = lax.rem(x, 4), lax.rem(y, 4), lax.rem(z, 4), lax.rem(c, 2)
    return (lax.rem(x, 2) * 8 + y * 2 + c, lax.div(x, 2) * 4 + z)


def greet(peers):
    barrier = pltpu.get_barrier_semaphore()
    for peer in peers:
        pl.semaphore_signal(barrier, inc=1, device_id=peer, device_id_type=MESH)
    pl.semaphore_wait(barrier, len(peers))


class Post:
    def __init__(self, send_sem, recv_sem):
        self.send_sem, self.recv_sem, self.copies = send_sem, recv_sem, []

    def send(self, src, dst, peer):
        i = len(self.copies)
        copy = pltpu.make_async_remote_copy(
            src_ref=src,
            dst_ref=dst,
            send_sem=self.send_sem.at[i],
            recv_sem=self.recv_sem.at[i],
            device_id=peer,
            device_id_type=MESH,
        )
        copy.start()
        self.copies.append(copy)
        return copy

    def close(self):
        for copy in self.copies:
            copy.wait_send()


def column(row):
    return jnp.transpose(jnp.broadcast_to(row, (128, 128)))


def at128(i):
    return pl.ds(pl.multiple_of(i * 128, 128), 128)


def kernel(loss_weight, width_in, hidden_in, w_in_in, embedding_in, gain_in, w_rows, ids, *rest):
    grad_hidden, grad_in, grad_out = rest[:3]
    (
        hidden, w_in, embedding, part, z_got, x_send, x_got, w_pair, w_full, ids_all,
        sq_mine, sq_all, ratio_rows, ratio_col, scaled, looked, x_rows, proj, normed, turned, logits,
        d_logit, scale_col, d_norm, dr_col, d_turn, d_all, small, small_all, corr_col,
        gp, gp_c, gp_y, gp_yg, gp_sum, gp_xg, gp_z, gp_zg, gp_rows, gp_pair,
        ip, ip_c, ip_y, ip_yg, ip_x, ip_xg, local_sem, send_sem, recv_sem,
    ) = rest[3:]
    x, y, z, c = place()
    x_lo, x_hi, step, zh = lax.rem(x, 2), lax.div(x, 2), lax.rem(z, 2), lax.div(z, 2)
    hid = x_hi * 4 + z
    quarter = x_hi * 2 + zh
    pair = device(x, y, z + 1 - 2 * step, c)
    across = device(x, y, z + 2, c)
    far = device(x + 2, y, z, c)
    twin = device(x, y, z, c + 1)
    beside = device(x + 1 - 2 * x_lo, y, z, c)
    xs = {d: device(x + d, y, z, c) for d in (1, 2, 3)}
    ys = {d: device(x, y + d, z, c) for d in (1, 2, 3)}
    zs = {d: device(x, y, z + d, c) for d in (1, 2, 3)}
    hid_peers = [device(x + dx, y, z + dz, c) for dz in (2, 1, 3, 0) for dx in (2, 0) if dx + dz]

    loads = [
        pltpu.make_async_copy(src, dst, local_sem.at[i])
        for i, (src, dst) in enumerate(
            ((hidden_in, hidden), (w_in_in, w_in), (embedding_in, embedding))
        )
    ]
    for load in loads:
        load.start()
    greet(hid_peers + [xs[1], xs[3]] + list(ys.values()) + [twin])
    post = Post(send_sem, recv_sem)

    w_swap = post.send(w_rows.at[1 - step], w_pair, pair)
    ids_swap = post.send(ids, ids_all.at[step], pair)
    ids_all[step] = ids[...]
    loads[0].wait()
    h = hidden[...].astype(F32)
    h2 = h * h
    top = h2.astype(BF)
    low = (h2 - top.astype(F32)).astype(BF)
    ones = jnp.ones((8, h2.shape[1]), BF)
    sq_mine[...] = lax.dot_general(ones, top, NT, preferred_element_type=F32) + lax.dot_general(
        ones, low, NT, preferred_element_type=F32
    )
    sq_all[hid] = sq_mine[...]
    loads[1].wait()

    def chunk(dz):
        to_z = lax.rem(z + dz, 4)
        rows = [hidden[at128(fx * 2 + lax.div(to_z, 2)), :] for fx in range(2)]
        product = jnp.dot(
            jnp.concatenate(rows, axis=0), w_in[lax.rem(to_z, 2)], preferred_element_type=F32
        ).astype(BF)
        part[dz, 0] = product[:128]
        part[dz, 1] = product[128:]

    chunk(2)
    sq_copies = [post.send(sq_mine, sq_all.at[hid], peer) for peer in hid_peers]
    z_copies = [post.send(part.at[2], z_got.at[0], zs[2])]
    w_swap.wait_recv()
    mine = w_rows[step].astype(F32)
    other = w_pair[...].astype(F32)
    first = jnp.where(step == 0, mine, other)
    second = jnp.where(step == 0, other, mine)
    w_full[x_lo, y, c, x_hi, zh] = jnp.concatenate([first, second], axis=0).astype(BF)
    chunk(1)
    block = w_full.at[x_lo, y, c, x_hi, zh]
    w_across = post.send(block, block, across)
    wa_x = [post.send(block, block, xs[d]) for d in (1, 3, 2)]
    z_copies.append(post.send(part.at[1], z_got.at[1], zs[1]))
    chunk(3)
    z_copies.append(post.send(part.at[3], z_got.at[2], zs[3]))
    w_across.wait_recv()
    block = w_full.at[x_lo, y, c, x_hi, 1 - zh]
    wb_y = [post.send(block, block, ys[d]) for d in (1, 3, 2)]
    chunk(0)
    for copy in wa_x:
        copy.wait_recv()
    line = w_full.at[:, y, c, :, zh]
    wa_y = {d: post.send(line, line, ys[d]) for d in (2, 1, 3)}
    w_twin = [post.send(line, line, twin)]
    for copy in wb_y:
        copy.wait_recv()
    line = w_full.at[x_lo, :, c, x_hi, 1 - zh]
    wb_x = {d: post.send(line, line, xs[d]) for d in (2, 1, 3)}
    w_twin.append(post.send(line, line, twin))

    for copy in sq_copies:
        copy.wait_recv()
    squares = sq_all[0]
    for i in range(1, 8):
        squares = squares + sq_all[i]
    ratio_rows[...] = lax.rsqrt(squares / width_in + 1e-06)
    for q in range(4):
        wide = column(ratio_rows[0:1, q * 128 : (q + 1) * 128])
        scaled[q * 128 : (q + 1) * 128, :] = (
            hidden[q * 128 : (q + 1) * 128, :].astype(F32) * wide[:, :1]
        ).astype(BF)
    ratio_col[...] = column(ratio_rows[0:1, at128(quarter)])
    ids_swap.wait_recv()

    def tokens(k):
        halves = [column(ids_all[i, k : k + 1, :].astype(F32))[:64, :1] for i in range(2)]
        return jnp.concatenate(halves, axis=0).astype(jnp.int32)

    previous, current = tokens(0), tokens(1)
    target = jnp.where(step == 1, current, previous)
    entries = logits.shape[1]
    lanes = lax.broadcasted_iota(jnp.int32, (128, entries), 1)
    loads[2].wait()
    pick = jnp.where(lanes == previous, 1.0, 0.0).astype(BF)
    live = step.astype(F32)
    for n in range(2):
        cols = slice(n * 512, (n + 1) * 512)
        looked[:, cols] = jnp.dot(pick, embedding[:, cols], preferred_element_type=F32) * live

    for copy in z_copies:
        copy.wait_recv()

    def z_sum(fx, rows):
        value = part[0, fx, rows, :].astype(F32)
        for i in range(3):
            value = value + z_got[i, fx, rows, :].astype(F32)
        return value

    @pl.loop(0, 8)
    def to_far(i):
        rows = pl.ds(pl.multiple_of(i * 16, 16), 16)
        x_send[rows, :] = z_sum(1 - x_hi, rows).astype(BF)

    x_copy = post.send(x_send, x_got, far)
    for d in (1, 3, 2):
        wa_y[d].wait_recv()
        line = w_full.at[:, lax.rem(y + 4 - d, 4), c, :, zh]
        w_twin.append(post.send(line, line, twin))
    for d in (1, 3, 2):
        wb_x[d].wait_recv()
        from_x = lax.rem(x + 4 - d, 4)
        line = w_full.at[lax.rem(from_x, 2), :, c, lax.div(from_x, 2), 1 - zh]
        w_twin.append(post.send(line, line, twin))
    x_copy.wait_recv()
    gain = gain_in[pl.ds(step, 1), :]

    @pl.loop(0, 8)
    def norm(i):
        rows = pl.ds(pl.multiple_of(i * 16, 16), 16)
        p = z_sum(x_hi, rows) + x_got[rows, :].astype(F32)
        value = ratio_col[rows, :1] * p + looked[rows, :]
        scale = lax.rsqrt(jnp.mean(value * value, axis=1, keepdims=True) + 1e-06)
        proj[rows, :] = p
        x_rows[rows, :] = value
        scale_col[rows, :] = jnp.broadcast_to(scale, (16, 128))
        normed[rows, :] = (value * scale * gain).astype(BF)

    for copy in w_twin:
        copy.wait_recv()

    depth = normed.shape[1]
    for n in range(4):
        cols = slice(n * 512, (n + 1) * 512)
        head = w_full[:, :, :, :, :, :, cols].reshape(depth, 512)
        logits[:, cols] = jnp.dot(normed[...], head, preferred_element_type=F32)
    for k in range(8):
        cols = slice(k * 128, (k + 1) * 128)
        turned[cols, :] = jnp.transpose(normed[:, cols].astype(F32)).astype(BF)
    scale_t = jnp.broadcast_to(target.astype(F32), (128, 128))
    dr_col[...] = scale_t

    @pl.loop(0, 8)
    def soft(i):
        rows = pl.ds(pl.multiple_of(i * 16, 16), 16)
        value = logits[rows, :]
        value = jnp.exp(value - jnp.max(value, axis=1, keepdims=True))
        share = value * (1.0 / jnp.sum(value, axis=1, keepdims=True))
        hot = lax.broadcasted_iota(jnp.int32, (16, entries), 1) == dr_col[rows, :1].astype(
            jnp.int32
        )
        d_logit[rows, :] = ((share - jnp.where(hot, 1.0, 0.0)) * loss_weight).astype(BF)

    for k in range(4):
        a, b = k // 2, (k % 2) * 2
        head = w_full[a, b : b + 2].reshape(256, entries)
        d_norm[:, k * 256 : (k + 1) * 256] = lax.dot_general(
            d_logit[...], head, NT, preferred_element_type=F32
        )

    @pl.loop(0, 8)
    def unnorm(i):
        rows = pl.ds(pl.multiple_of(i * 16, 16), 16)
        value, scale = x_rows[rows, :], scale_col[rows, :1]
        gated = gain * d_norm[rows, :]
        inner = jnp.mean(gated * value, axis=1, keepdims=True)
        d_x = scale * gated - value * (scale * scale * scale * inner)
        d_norm[rows, :] = d_x
        total = jnp.sum(d_x * proj[rows, :], axis=1, keepdims=True)
        dr_col[rows, :] = jnp.broadcast_to(total, (16, 128))

    small[...] = jnp.transpose(dr_col[...])[:8]
    for k in range(8):
        cols = slice(k * 128, (k + 1) * 128)
        d_turn[cols, :] = jnp.transpose(d_norm[:, cols]).astype(BF)
    slab = d_all.at[step, :, at128(quarter)]
    rows_copies = []
    for peer in hid_peers:
        rows_copies.append(post.send(d_turn, slab, peer))
        rows_copies.append(post.send(small, small_all.at[hid], peer))
    d_all[step, :, at128(quarter)] = d_turn[...]
    small_all[hid] = small[...]

    order = (2, 1, 3, 0)
    gp_swap = []
    for d in order:
        to_y = lax.rem(y + d, 4)
        for a in range(2):
            rows = at128(a * 4 + to_y)
            gp[a, to_y] = (
                jnp.dot(turned[rows, :], d_logit[...], preferred_element_type=F32)
                .astype(BF)
                .reshape(2, 2, 2, 16, entries)
            )
        gp_swap.append(post.send(gp.at[:, to_y, 1 - c], gp_c.at[:, to_y], twin))
    gp_ys = []
    for i, d in enumerate(order[:3]):
        gp_swap[i].wait_recv()
        to_y = lax.rem(y + d, 4)

        @pl.loop(0, 8)
        def add(j):
            a, b, e = lax.div(j, 4), lax.rem(lax.div(j, 2), 2), lax.rem(j, 2)
            gp_y[i, a, b, e] = (
                gp[a, to_y, c, b, e].astype(F32) + gp_c[a, to_y, b, e].astype(F32)
            ).astype(BF)

        gp_ys.append(post.send(gp_y.at[i], gp_yg.at[i], ys[d]))
    gp_swap[3].wait_recv()

    for copy in rows_copies:
        copy.wait_recv()
    ip_swap = []
    for d in order:
        to_y = lax.rem(y + d, 4)
        rows = [d_all[s, at128(a * 4 + to_y), :] for s in range(2) for a in range(2)]
        product = jnp.dot(
            jnp.concatenate(rows, axis=0), scaled[...], preferred_element_type=F32
        ).astype(BF)
        for s in range(2):
            for a in range(2):
                for e in range(2):
                    start = (s * 2 + a) * 128 + e * 64
                    ip[s, a, to_y, e] = product[start : start + 64]
        ip_swap.append(post.send(ip.at[:, :, to_y, 1 - c], ip_c.at[:, :, to_y], twin))
    ip_ys = []
    for i, d in enumerate(order[:3]):
        ip_swap[i].wait_recv()
        to_y = lax.rem(y + d, 4)

        @pl.loop(0, 4)
        def add_in(j):
            a, b = lax.div(j, 2), lax.rem(j, 2)
            ip_y[i, a, b] = (
                ip[a, b, to_y, c].astype(F32) + ip_c[a, b, to_y].astype(F32)
            ).astype(BF)

        ip_ys.append(post.send(ip_y.at[i], ip_yg.at[i], ys[d]))
    ip_swap[3].wait_recv()

    for copy in gp_ys:
        copy.wait_recv()

    @pl.loop(0, 8)
    def total(j):
        a, b, e = lax.div(j, 4), lax.rem(lax.div(j, 2), 2), lax.rem(j, 2)
        value = gp[a, y, c, b, e].astype(F32) + gp_c[a, y, b, e].astype(F32)
        for i in range(3):
            value = value + gp_yg[i, a, b, e].astype(F32)
        gp_sum[a, b, e] = value.astype(BF)

    gp_xs = []
    for i, d in enumerate(order[:3]):
        to_x = lax.rem(x + d, 4)
        gp_xs.append(
            post.send(gp_sum.at[lax.rem(to_x, 2), lax.div(to_x, 2)], gp_xg.at[i], xs[d])
        )

    ratio_row = ratio_rows[0:1, :]
    for q in range(4):
        cols = slice(q * 128, (q + 1) * 128)
        r = ratio_rows[0:1, cols]
        total_dr = small_all[2 * q, 0:1, :] + small_all[2 * q + 1, 0:1, :]
        corr_col[cols, :] = column(r * r * r * total_dr * (1.0 / width_in))

    def back(k):
        cols = slice(k * 128, (k + 1) * 128)
        value = jnp.dot(w_in[0, cols, :], d_all[0], preferred_element_type=F32) + jnp.dot(
            w_in[1, cols, :], d_all[1], preferred_element_type=F32
        )
        grad_hidden[:, cols] = (
            jnp.transpose(value * ratio_row)
            - corr_col[:, :1] * hidden[:, cols].astype(F32)
        ).astype(BF)

    back(0)
    back(1)
    for copy in gp_xs:
        copy.wait_recv()

    def out_block(e):
        value = gp_sum[x_lo, x_hi, e].astype(F32)
        for i in range(3):
            value = value + gp_xg[i, e].astype(F32)
        return value

    gp_z[...] = out_block(1 - zh).astype(BF)
    gp_across = post.send(gp_z, gp_zg, across)
    back(2)
    for copy in ip_ys:
        copy.wait_recv()

    def in_block(a, b):
        value = ip[a, b, y, c].astype(F32) + ip_c[a, b, y].astype(F32)
        for i in range(3):
            value = value + ip_yg[i, a, b].astype(F32)
        return value

    for a in range(2):
        ip_x[a] = in_block(a, 1 - x_lo).astype(BF)
    ip_beside = post.send(ip_x, ip_xg, beside)
    gp_across.wait_recv()
    gp_rows[...] = out_block(zh) + gp_zg[...].astype(F32)
    theirs = gp_rows.at[pl.ds(pl.multiple_of((1 - step) * 8, 8), 8), :]
    gp_swap_rows = post.send(theirs, gp_pair, pair)
    back(3)
    own = [in_block(a, x_lo) for a in range(2)]
    ip_beside.wait_recv()
    both = jnp.concatenate([own[a] + ip_xg[a].astype(F32) for a in range(2)], axis=0)
    both = jnp.transpose(both)
    grad_in[0] = both[:, :64]
    grad_in[1] = both[:, 64:]
    gp_swap_rows.wait_recv()
    grad_out[step] = gp_rows[pl.ds(pl.multiple_of(step * 8, 8), 8), :]
    grad_out[1 - step] = gp_pair[...]
    post.close()


def shards(hidden, w_in, embedding, depth_gain, w_out, codebook_ids):
    hid_count = lax.axis_size("hid")
    seq_count = lax.axis_size("seq")
    width_in = hidden.shape[1] * hid_count
    depth = w_in.shape[2]
    entries = w_out.shape[2]
    frames, units = hidden.shape
    own = codebook_ids.shape[1]
    loss_weight = 2.0 * entries / (frames * seq_count)
    ids = jnp.pad(codebook_ids, ((0, 6), (0, 128 - own)))
    vmem = pl.BlockSpec(memory_space=pltpu.VMEM)
    anywhere = pl.BlockSpec(memory_space=pl.ANY)
    scratch = [
        ((frames, units), BF),
        ((2, units, depth), BF),
        ((entries, depth), BF),
        ((4, 2, 128, depth), BF),
        ((3, 2, 128, depth), BF),
        ((128, depth), BF),
        ((128, depth), BF),
        ((8, entries), BF),
        ((2, 4, 2, 2, 2, 16, entries), BF),
        ((2, 8, 128), jnp.int32),
        ((8, frames), F32),
        ((8, 8, frames), F32),
        ((8, frames), F32),
        ((128, 128), F32),
        ((frames, units), BF),
        ((128, depth), F32),
        ((128, depth), F32),
        ((128, depth), F32),
        ((128, depth), BF),
        ((depth, 128), BF),
        ((128, entries), F32),
        ((128, entries), BF),
        ((128, 128), F32),
        ((128, depth), F32),
        ((128, 128), F32),
        ((depth, 128), BF),
        ((2, depth, frames), BF),
        ((8, 128), F32),
        ((8, 8, 128), F32),
        ((frames, 128), F32),
        ((2, 4, 2, 2, 2, 16, entries), BF),
        ((2, 4, 2, 2, 16, entries), BF),
        ((3, 2, 2, 2, 16, entries), BF),
        ((3, 2, 2, 2, 16, entries), BF),
        ((2, 2, 2, 16, entries), BF),
        ((3, 2, 16, entries), BF),
        ((16, entries), BF),
        ((16, entries), BF),
        ((16, entries), F32),
        ((8, entries), F32),
        ((2, 2, 4, 2, 64, units), BF),
        ((2, 2, 4, 64, units), BF),
        ((3, 2, 2, 64, units), BF),
        ((3, 2, 2, 64, units), BF),
        ((2, 64, units), BF),
        ((2, 64, units), BF),
    ]
    grad_hidden, grad_in, grad_out = pl.pallas_call(
        functools.partial(kernel, loss_weight, width_in),
        out_shape=[
            jax.ShapeDtypeStruct((frames, units), BF),
            jax.ShapeDtypeStruct((2, units, 64), F32),
            jax.ShapeDtypeStruct((2, 8, entries), F32),
        ],
        in_specs=[anywhere] * 3 + [vmem] * 3,
        out_specs=[vmem] * 3,
        scratch_shapes=[pltpu.VMEM(shape, dtype) for shape, dtype in scratch]
        + [
            pltpu.SemaphoreType.DMA((3,)),
            pltpu.SemaphoreType.DMA((80,)),
            pltpu.SemaphoreType.DMA((80,)),
        ],
        compiler_params=pltpu.CompilerParams(
            collective_id=0, has_side_effects=True, vmem_limit_bytes=60 * 1024 * 1024
        ),
        name="whole",
    )(hidden, w_in, embedding[0], depth_gain, jnp.transpose(w_out, (1, 0, 2)), ids)
    return grad_hidden, grad_in, jnp.transpose(grad_out, (1, 0, 2))


def solution(mesh):
    placed = (
        P("seq", "hid"),
        P(None, "hid", None),
        P(),
        P(),
        P(("seq", "hid"), None, None),
        P(None, ("seq", "hid")),
    )
    return jax.shard_map(
        shards,
        mesh=mesh,
        in_specs=placed,
        out_specs=(P("seq", "hid"), P(None, "hid", "seq"), P(("seq", "hid"), None, None)),
        check_vma=False,
    )
```

```python
import functools

import jax
import jax.numpy as jnp
from jax import lax
from jax.experimental import pallas as pl
from jax.experimental.pallas import tpu as pltpu
from jax.sharding import PartitionSpec as P

MESH = pl.DeviceIdType.MESH
BF = jnp.bfloat16
F32 = jnp.float32
NT = (((1,), (1,)), ((), ()))


def place():
    s, h = lax.axis_index("seq"), lax.axis_index("hid")
    x_lo, y, c = lax.div(s, 8), lax.rem(lax.div(s, 2), 4), lax.rem(s, 2)
    return 2 * lax.div(h, 4) + x_lo, y, lax.rem(h, 4), c


def device(x, y, z, c):
    x, y, z, c = lax.rem(x, 4), lax.rem(y, 4), lax.rem(z, 4), lax.rem(c, 2)
    return (lax.rem(x, 2) * 8 + y * 2 + c, lax.div(x, 2) * 4 + z)


def greet(peers):
    barrier = pltpu.get_barrier_semaphore()
    for peer in peers:
        pl.semaphore_signal(barrier, inc=1, device_id=peer, device_id_type=MESH)
    pl.semaphore_wait(barrier, len(peers))


class Post:
    def __init__(self, send_sem, recv_sem):
        self.send_sem, self.recv_sem, self.copies = send_sem, recv_sem, []

    def send(self, src, dst, peer):
        i = len(self.copies)
        copy = pltpu.make_async_remote_copy(
            src_ref=src,
            dst_ref=dst,
            send_sem=self.send_sem.at[i],
            recv_sem=self.recv_sem.at[i],
            device_id=peer,
            device_id_type=MESH,
        )
        copy.start()
        self.copies.append(copy)
        return copy

    def close(self):
        for copy in self.copies:
            copy.wait_send()


def column(row):
    return jnp.transpose(jnp.broadcast_to(row, (128, 128)))


def at128(i):
    return pl.ds(pl.multiple_of(i * 128, 128), 128)


def kernel(loss_weight, width_in, hidden_in, w_in_in, embedding_in, gain_in, w_out, ids, *rest):
    grad_hidden, grad_in, grad_out = rest[:3]
    (
        hidden, w_in, embedding, part, relay, relay_sum, z_got, x_send, x_got,
        w_rows, w_got, w_full, ids_mine, ids_all,
        sq_mine, sq_all, ratio_rows, ratio_col, scaled, looked, x_rows, proj, normed, turned, logits,
        d_logit, scale_col, d_norm, dr_col, d_turn, d_all, small, small_all, corr_col,
        gp, gp_c, ga_y, ga_yg, ga_sum, ga_xg, gb_x, gb_xg, gb_sum, gb_yg, gp_z, gp_zg, gp_rows, gp_pair,
        ip, ip_c, ip_y, ip_yg, ip_x, ip_xg, local_sem, send_sem, recv_sem,
    ) = rest[3:]
    x, y, z, c = place()
    x_lo, x_hi, step, zh = lax.rem(x, 2), lax.div(x, 2), lax.rem(z, 2), lax.div(z, 2)
    hid = x_hi * 4 + z
    quarter, far_quarter = x_hi * 2 + zh, (1 - x_hi) * 2 + zh
    pair = device(x, y, z + 1 - 2 * step, c)
    far = device(x + 2, y, z, c)
    twin = device(x, y, z, c + 1)
    beside = device(x + 1 - 2 * x_lo, y, z, c)
    xs = {d: device(x + d, y, z, c) for d in (1, 2, 3)}
    ys = {d: device(x, y + d, z, c) for d in (1, 2, 3)}
    zs = {d: device(x, y, z + d, c) for d in (1, 2, 3)}
    hid_peers = [device(x + dx, y, z + dz, c) for dz in (2, 1, 3, 0) for dx in (2, 0) if dx + dz]
    order = (2, 1, 3, 0)

    loads = [
        pltpu.make_async_copy(src, dst, local_sem.at[i])
        for i, (src, dst) in enumerate(
            ((hidden_in, hidden), (w_in_in, w_in), (embedding_in, embedding))
        )
    ]
    for load in loads:
        load.start()
    w_rows[0] = w_out[:, 0, :]
    w_rows[1] = w_out[:, 1, :]
    ids_mine[...] = jnp.zeros_like(ids_mine)
    ids_mine[0:2, 0:64] = ids[...]
    greet(hid_peers + [xs[1], xs[3]] + list(ys.values()) + [twin])
    post = Post(send_sem, recv_sem)

    w_z = [post.send(w_rows.at[(step + d) % 2], w_got.at[z], zs[d]) for d in (2, 1, 3)]
    ids_swap = post.send(ids_mine, ids_all.at[step], pair)
    ids_all[step] = ids_mine[...]
    w_got[z] = w_rows[step]
    loads[0].wait()
    h = hidden[...].astype(F32)
    h2 = h * h
    top = h2.astype(BF)
    low = (h2 - top.astype(F32)).astype(BF)
    ones = jnp.ones((8, h2.shape[1]), BF)
    sq_mine[...] = lax.dot_general(ones, top, NT, preferred_element_type=F32) + lax.dot_general(
        ones, low, NT, preferred_element_type=F32
    )
    sq_all[hid] = sq_mine[...]
    loads[1].wait()

    def chunk(dz):
        to_z = lax.rem(z + dz, 4)
        rows = [hidden[at128(fx * 2 + lax.div(to_z, 2)), :] for fx in range(2)]
        product = jnp.dot(
            jnp.concatenate(rows, axis=0), w_in[lax.rem(to_z, 2)], preferred_element_type=F32
        ).astype(BF)
        part[dz, 0] = product[:128]
        part[dz, 1] = product[128:]

    halves = (pl.ds(0, 64), pl.ds(64, 64))
    relays, z_copies = [[], []], [[], []]

    def send_opposite(p):
        rows = halves[p]
        relays[p].append(post.send(part.at[2, 0, rows], relay.at[0, rows], zs[1]))
        relays[p].append(post.send(part.at[2, 1, rows], relay.at[1, rows], zs[3]))

    def send_direct(p, dz):
        rows, fx, slot = halves[p], (1 if dz == 1 else 0), (0 if dz == 1 else 1)
        z_copies[p].append(post.send(part.at[dz, fx, rows], z_got.at[slot, fx, rows], zs[dz]))

    def send_sums(p):
        for fx, dz in ((0, 1), (1, 3)):
            rows = halves[p]
            relays[p][fx].wait_recv()
            relay_sum[fx, rows, :] = (
                part[dz, fx, rows, :].astype(F32) + relay[fx, rows, :].astype(F32)
            ).astype(BF)
            z_copies[p].append(
                post.send(relay_sum.at[fx, rows], z_got.at[fx, fx, rows], zs[dz])
            )

    chunk(2)
    send_opposite(0)
    sq_copies = [post.send(sq_mine, sq_all.at[hid], peer) for peer in hid_peers]
    chunk(1)
    send_direct(0, 1)
    chunk(3)
    send_direct(0, 3)
    send_opposite(1)
    send_direct(1, 1)
    send_direct(1, 3)
    for copy in w_z:
        copy.wait_recv()
    for e in range(2):
        both = [w_got[2 * e + i].astype(F32) for i in range(2)]
        w_full[x_lo, y, c, x_hi, e] = jnp.concatenate(both, axis=0).astype(BF)
    block = w_full.at[x_lo, y, c, x_hi, zh]
    wa_x = [post.send(block, block, xs[d]) for d in (1, 3, 2)]
    block = w_full.at[x_lo, y, c, x_hi, 1 - zh]
    wb_y = [post.send(block, block, ys[d]) for d in (1, 3, 2)]
    chunk(0)
    send_sums(0)
    for copy in wa_x:
        copy.wait_recv()
    line = w_full.at[:, y, c, :, zh]
    wa_y = {d: post.send(line, line, ys[d]) for d in (2, 1, 3)}
    w_twin = [post.send(line, line, twin)]
    for copy in wb_y:
        copy.wait_recv()
    line = w_full.at[x_lo, :, c, x_hi, 1 - zh]
    wb_x = {d: post.send(line, line, xs[d]) for d in (2, 1, 3)}
    w_twin.append(post.send(line, line, twin))
    send_sums(1)

    for copy in sq_copies:
        copy.wait_recv()
    squares = sq_all[0]
    for i in range(1, 8):
        squares = squares + sq_all[i]
    ratio_rows[...] = lax.rsqrt(squares / width_in + 1e-06)
    for q in range(4):
        wide = column(ratio_rows[0:1, q * 128 : (q + 1) * 128])
        scaled[q * 128 : (q + 1) * 128, :] = (
            hidden[q * 128 : (q + 1) * 128, :].astype(F32) * wide[:, :1]
        ).astype(BF)
    ratio_col[...] = column(ratio_rows[0:1, at128(quarter)])
    ids_swap.wait_recv()

    def tokens(k):
        parts = [column(ids_all[i, k : k + 1, :].astype(F32))[:64, :1] for i in range(2)]
        return jnp.concatenate(parts, axis=0).astype(jnp.int32)

    previous, current = tokens(0), tokens(1)
    target = jnp.where(step == 1, current, previous)
    entries = logits.shape[1]
    lanes = lax.broadcasted_iota(jnp.int32, (128, entries), 1)
    loads[2].wait()
    pick = jnp.where(lanes == previous, 1.0, 0.0).astype(BF)
    live = step.astype(F32)
    for n in range(2):
        cols = slice(n * 512, (n + 1) * 512)
        looked[:, cols] = jnp.dot(pick, embedding[:, cols], preferred_element_type=F32) * live

    def z_sum(fx, rows):
        return (
            part[0, fx, rows, :].astype(F32)
            + z_got[0, fx, rows, :].astype(F32)
            + z_got[1, fx, rows, :].astype(F32)
        )

    x_copies = []
    for p in range(2):
        for copy in z_copies[p]:
            copy.wait_recv()

        @pl.loop(p * 4, p * 4 + 4, unroll=True)
        def to_far(i):
            rows = pl.ds(pl.multiple_of(i * 16, 16), 16)
            x_send[rows, :] = z_sum(1 - x_hi, rows).astype(BF)

        x_copies.append(post.send(x_send.at[halves[p]], x_got.at[halves[p]], far))
    for d in (1, 3, 2):
        wa_y[d].wait_recv()
        line = w_full.at[:, lax.rem(y + 4 - d, 4), c, :, zh]
        w_twin.append(post.send(line, line, twin))
    for d in (1, 3, 2):
        wb_x[d].wait_recv()
        from_x = lax.rem(x + 4 - d, 4)
        line = w_full.at[lax.rem(from_x, 2), :, c, lax.div(from_x, 2), 1 - zh]
        w_twin.append(post.send(line, line, twin))
    gain = gain_in[pl.ds(step, 1), :]
    for p in range(2):
        x_copies[p].wait_recv()

        @pl.loop(p * 4, p * 4 + 4, unroll=True)
        def norm(i):
            rows = pl.ds(pl.multiple_of(i * 16, 16), 16)
            value = z_sum(x_hi, rows) + x_got[rows, :].astype(F32)
            proj[rows, :] = value
            value = ratio_col[rows, :1] * value + looked[rows, :]
            scale = lax.rsqrt(jnp.mean(value * value, axis=1, keepdims=True) + 1e-06)
            x_rows[rows, :] = value
            scale_col[rows, :] = jnp.broadcast_to(scale, (16, 128))
            normed[rows, :] = (value * scale * gain).astype(BF)

    for copy in w_twin:
        copy.wait_recv()

    depth = normed.shape[1]
    for n in range(4):
        cols = slice(n * 512, (n + 1) * 512)
        head = w_full[:, :, :, :, :, :, cols].reshape(depth, 512)
        logits[:, cols] = jnp.dot(normed[...], head, preferred_element_type=F32)
    dr_col[...] = jnp.broadcast_to(target.astype(F32), (128, 128))

    @pl.loop(0, 8, unroll=2)
    def soft(i):
        rows = pl.ds(pl.multiple_of(i * 16, 16), 16)
        value = logits[rows, :]
        value = jnp.exp(value - jnp.max(value, axis=1, keepdims=True))
        share = value * (loss_weight / jnp.sum(value, axis=1, keepdims=True))
        hot = lax.broadcasted_iota(jnp.int32, (16, entries), 1) == dr_col[rows, :1].astype(
            jnp.int32
        )
        d_logit[rows, :] = (share - jnp.where(hot, loss_weight, 0.0)).astype(BF)

    for k in range(4):
        a, b = k // 2, (k % 2) * 2
        head = w_full[a, b : b + 2].reshape(256, entries)
        d_norm[:, k * 256 : (k + 1) * 256] = lax.dot_general(
            d_logit[...], head, NT, preferred_element_type=F32
        )

    @pl.loop(0, 8, unroll=4)
    def unnorm(i):
        rows = pl.ds(pl.multiple_of(i * 16, 16), 16)
        value, scale = x_rows[rows, :], scale_col[rows, :1]
        gated = gain * d_norm[rows, :]
        inner = jnp.mean(gated * value, axis=1, keepdims=True)
        d_x = scale * gated - value * (scale * scale * scale * inner)
        d_norm[rows, :] = d_x
        total = jnp.sum(d_x * proj[rows, :], axis=1, keepdims=True)
        dr_col[rows, :] = jnp.broadcast_to(total, (16, 128))

    for k in range(8):
        d_turn[k // 4, k % 4] = jnp.transpose(d_norm[:, k * 128 : (k + 1) * 128]).astype(BF)
    lane, far_lane = at128(quarter), at128(far_quarter)

    d_x_copies, d_z_copies = [], [[], [], [], []]
    for d in order:
        to_y = lax.rem(y + d, 4)
        d_x_copies.append(
            post.send(d_turn.at[:, to_y], d_all.at[step, :, to_y, :, lane], far)
        )

    def send_own(i):
        to_y = lax.rem(y + order[i], 4)
        for d in (2, 1, 3):
            d_z_copies[i].append(
                post.send(d_turn.at[:, to_y], d_all.at[step, :, to_y, :, lane], zs[d])
            )

    def send_far(i):
        to_y = lax.rem(y + order[i], 4)
        d_x_copies[i].wait_recv()
        view = d_all.at[step, :, to_y, :, far_lane]
        for d in (2, 1, 3):
            d_z_copies[i].append(post.send(view, view, zs[d]))

    send_own(0)
    send_own(1)
    small[...] = jnp.transpose(dr_col[...])[:8]
    small_copies = [post.send(small, small_all.at[hid], peer) for peer in hid_peers]
    for b in range(4):
        for a in range(2):
            d_all[step, a, b, :, lane] = d_turn[a, b]
    small_all[hid] = small[...]

    for k in range(8):
        cols = slice(k * 128, (k + 1) * 128)
        turned[cols, :] = jnp.transpose(normed[:, cols].astype(F32)).astype(BF)
    gp_swap = []

    def product_out(i):
        to_y = lax.rem(y + order[i], 4)
        for a in range(2):
            rows = at128(a * 4 + to_y)
            gp[a, to_y] = (
                jnp.dot(turned[rows, :], d_logit[...], preferred_element_type=F32)
                .astype(BF)
                .reshape(2, 2, 2, 16, entries)
            )
        gp_swap.append(post.send(gp.at[:, to_y, 1 - c], gp_c.at[:, to_y], twin))

    for i in range(4):
        product_out(i)
    send_far(0)
    send_own(2)
    send_far(1)
    send_own(3)

    def core_sum(a, b, e, f):
        return gp[a, b, c, e, f].astype(F32) + gp_c[a, b, e, f].astype(F32)

    ga_ys, gb_xs = [], []
    for i, d in enumerate(order[:3]):
        gp_swap[i].wait_recv()
        to_y = lax.rem(y + d, 4)
        for a in range(2):
            for e in range(2):
                ga_y[i, a, e] = core_sum(a, to_y, e, zh).astype(BF)
        ga_ys.append(post.send(ga_y.at[i], ga_yg.at[i], ys[d]))
    gp_swap[3].wait_recv()
    for i, d in enumerate(order[:3]):
        to_x = lax.rem(x + d, 4)
        for b in range(4):
            gb_x[i, b] = core_sum(lax.rem(to_x, 2), b, lax.div(to_x, 2), 1 - zh).astype(BF)
        gb_xs.append(post.send(gb_x.at[i], gb_xg.at[i], xs[d]))
    send_far(2)
    send_far(3)

    ip_ys = []

    def product_in(i):
        for copy in d_z_copies[i]:
            copy.wait_recv()
        to_y = lax.rem(y + order[i], 4)
        rows = [d_all[s, a, to_y] for s in range(2) for a in range(2)]
        product = jnp.dot(
            jnp.concatenate(rows, axis=0), scaled[...], preferred_element_type=F32
        ).astype(BF)
        for s in range(2):
            for a in range(2):
                for e in range(2):
                    start = (s * 2 + a) * 128 + e * 64
                    ip[s, a, to_y, e] = product[start : start + 64]
        return post.send(ip.at[:, :, to_y, 1 - c], ip_c.at[:, :, to_y], twin)

    def sum_in(i, swap):
        swap.wait_recv()
        to_y = lax.rem(y + order[i], 4)
        for s in range(2):
            for a in range(2):
                ip_y[i, s, a] = (
                    ip[s, a, to_y, c].astype(F32) + ip_c[s, a, to_y].astype(F32)
                ).astype(BF)
        ip_ys.append(post.send(ip_y.at[i], ip_yg.at[i], ys[order[i]]))

    swap = product_in(0)
    sum_in(0, swap)
    swap = product_in(1)
    sum_in(1, swap)
    for copy in ga_ys:
        copy.wait_recv()
    for a in range(2):
        for e in range(2):
            value = core_sum(a, y, e, zh)
            for i in range(3):
                value = value + ga_yg[i, a, e].astype(F32)
            ga_sum[a, e] = value.astype(BF)
    ga_xs = []
    for i, d in enumerate(order[:3]):
        to_x = lax.rem(x + d, 4)
        ga_xs.append(
            post.send(ga_sum.at[lax.rem(to_x, 2), lax.div(to_x, 2)], ga_xg.at[i], xs[d])
        )
    for copy in gb_xs:
        copy.wait_recv()
    for b in range(4):
        value = core_sum(x_lo, b, x_hi, 1 - zh)
        for i in range(3):
            value = value + gb_xg[i, b].astype(F32)
        gb_sum[b] = value.astype(BF)
    gb_ys = []
    for i, d in enumerate(order[:3]):
        gb_ys.append(post.send(gb_sum.at[lax.rem(y + d, 4)], gb_yg.at[i], ys[d]))
    swap = product_in(2)
    sum_in(2, swap)
    last_swap = product_in(3)

    for copy in gb_ys:
        copy.wait_recv()
    value = gb_sum[y].astype(F32)
    for i in range(3):
        value = value + gb_yg[i].astype(F32)
    gp_z[...] = value.astype(BF)
    gp_across = post.send(gp_z, gp_zg, zs[2])

    ratio_row = ratio_rows[0:1, :]
    for copy in small_copies:
        copy.wait_recv()
    for q in range(4):
        cols = slice(q * 128, (q + 1) * 128)
        r = ratio_rows[0:1, cols]
        total_dr = small_all[2 * q, 0:1, :] + small_all[2 * q + 1, 0:1, :]
        corr_col[cols, :] = column(r * r * r * total_dr * (1.0 / width_in))

    def back(k):
        cols = slice(k * 128, (k + 1) * 128)
        value = sum(
            jnp.dot(w_in[s, cols, :], d_all[s].reshape(depth, -1), preferred_element_type=F32)
            for s in range(2)
        )
        grad_hidden[:, cols] = (
            jnp.transpose(value * ratio_row)
            - corr_col[:, :1] * hidden[:, cols].astype(F32)
        ).astype(BF)

    back(0)
    back(1)
    for copy in ga_xs:
        copy.wait_recv()
    value = ga_sum[x_lo, x_hi].astype(F32)
    for i in range(3):
        value = value + ga_xg[i].astype(F32)
    gp_across.wait_recv()
    gp_rows[...] = value + gp_zg[...].astype(F32)
    theirs = gp_rows.at[pl.ds(pl.multiple_of((1 - step) * 8, 8), 8), :]
    gp_swap_rows = post.send(theirs, gp_pair, pair)
    last_swap.wait_recv()
    for copy in ip_ys:
        copy.wait_recv()

    def in_block(a, b):
        value = ip[a, b, y, c].astype(F32) + ip_c[a, b, y].astype(F32)
        for i in range(3):
            value = value + ip_yg[i, a, b].astype(F32)
        return value

    for a in range(2):
        ip_x[a] = in_block(a, 1 - x_lo).astype(BF)
    ip_beside = post.send(ip_x, ip_xg, beside)
    back(2)
    back(3)
    for a in range(2):
        grad_in[a] = in_block(a, x_lo)
    gp_swap_rows.wait_recv()
    grad_out[step] = gp_rows[pl.ds(pl.multiple_of(step * 8, 8), 8), :]
    grad_out[1 - step] = gp_pair[...]
    ip_beside.wait_recv()
    for a in range(2):
        grad_in[a] = grad_in[a] + ip_xg[a].astype(F32)
    post.close()


def finish(gh, gi, go, grad_hidden, grad_in, grad_out):
    grad_hidden[...] = gh[...]
    grad_in[...] = gi[...]
    grad_out[:, 0, :] = go[0]
    grad_out[:, 1, :] = go[1]


def shards(hidden, w_in, embedding, depth_gain, w_out, codebook_ids):
    hid_count = lax.axis_size("hid")
    seq_count = lax.axis_size("seq")
    width_in = hidden.shape[1] * hid_count
    depth = w_in.shape[2]
    entries = w_out.shape[2]
    frames, units = hidden.shape
    loss_weight = 2.0 * entries / (frames * seq_count)
    vmem = pl.BlockSpec(memory_space=pltpu.VMEM)
    anywhere = pl.BlockSpec(memory_space=pl.ANY)
    scratch = [
        ((frames, units), BF),
        ((2, units, depth), BF),
        ((entries, depth), BF),
        ((4, 2, 128, depth), BF),
        ((2, 128, depth), BF),
        ((2, 128, depth), BF),
        ((2, 2, 128, depth), BF),
        ((128, depth), BF),
        ((128, depth), BF),
        ((2, 8, entries), BF),
        ((4, 8, entries), BF),
        ((2, 4, 2, 2, 2, 16, entries), BF),
        ((8, 128), jnp.int32),
        ((2, 8, 128), jnp.int32),
        ((8, frames), F32),
        ((8, 8, frames), F32),
        ((8, frames), F32),
        ((128, 128), F32),
        ((frames, units), BF),
        ((128, depth), F32),
        ((128, depth), F32),
        ((128, depth), F32),
        ((128, depth), BF),
        ((depth, 128), BF),
        ((128, entries), F32),
        ((128, entries), BF),
        ((128, 128), F32),
        ((128, depth), F32),
        ((128, 128), F32),
        ((2, 4, 128, 128), BF),
        ((2, 2, 4, 128, frames), BF),
        ((8, 128), F32),
        ((8, 8, 128), F32),
        ((frames, 128), F32),
        ((2, 4, 2, 2, 2, 16, entries), BF),
        ((2, 4, 2, 2, 16, entries), BF),
        ((3, 2, 2, 16, entries), BF),
        ((3, 2, 2, 16, entries), BF),
        ((2, 2, 16, entries), BF),
        ((3, 16, entries), BF),
        ((3, 4, 16, entries), BF),
        ((3, 4, 16, entries), BF),
        ((4, 16, entries), BF),
        ((3, 16, entries), BF),
        ((16, entries), BF),
        ((16, entries), BF),
        ((16, entries), F32),
        ((8, entries), F32),
        ((2, 2, 4, 2, 64, units), BF),
        ((2, 2, 4, 64, units), BF),
        ((3, 2, 2, 64, units), BF),
        ((3, 2, 2, 64, units), BF),
        ((2, 64, units), BF),
        ((2, 64, units), BF),
    ]
    grad_hidden, grad_in, grad_out = pl.pallas_call(
        functools.partial(kernel, loss_weight, width_in),
        out_shape=[
            jax.ShapeDtypeStruct((frames, units), BF),
            jax.ShapeDtypeStruct((2, 64, units), F32),
            jax.ShapeDtypeStruct((2, 8, entries), F32),
        ],
        in_specs=[anywhere] * 3 + [vmem] * 3,
        out_specs=[vmem] * 3,
        scratch_shapes=[pltpu.VMEM(shape, dtype) for shape, dtype in scratch]
        + [
            pltpu.SemaphoreType.DMA((3,)),
            pltpu.SemaphoreType.DMA((112,)),
            pltpu.SemaphoreType.DMA((112,)),
        ],
        compiler_params=pltpu.CompilerParams(
            collective_id=0, has_side_effects=True, vmem_limit_bytes=60 * 1024 * 1024
        ),
        name="whole",
    )(hidden, w_in, embedding[0], depth_gain, w_out, codebook_ids)
    grad_hidden, grad_in, grad_out = pl.pallas_call(
        finish,
        out_shape=[
            jax.ShapeDtypeStruct((frames, units), BF),
            jax.ShapeDtypeStruct((2, 64, units), F32),
            jax.ShapeDtypeStruct((8, 2, entries), F32),
        ],
        in_specs=[vmem] * 3,
        out_specs=[vmem] * 3,
        name="finish",
    )(grad_hidden, grad_in, grad_out)
    return grad_hidden, jnp.transpose(grad_in, (0, 2, 1)), grad_out


def solution(mesh):
    placed = (
        P("seq", "hid"),
        P(None, "hid", None),
        P(),
        P(),
        P(("seq", "hid"), None, None),
        P(None, ("seq", "hid")),
    )
    return jax.shard_map(
        shards,
        mesh=mesh,
        in_specs=placed,
        out_specs=(P("seq", "hid"), P(None, "hid", "seq"), P(("seq", "hid"), None, None)),
        check_vma=False,
    )
```

```python
import functools

import jax
import jax.numpy as jnp
from jax import lax
from jax.experimental import pallas as pl
from jax.experimental.pallas import tpu as pltpu
from jax.sharding import PartitionSpec as P

MESH = pl.DeviceIdType.MESH
BF = jnp.bfloat16
F32 = jnp.float32
NT = (((1,), (1,)), ((), ()))


def place():
    s, h = lax.axis_index("seq"), lax.axis_index("hid")
    x_lo, y, c = lax.div(s, 8), lax.rem(lax.div(s, 2), 4), lax.rem(s, 2)
    return 2 * lax.div(h, 4) + x_lo, y, lax.rem(h, 4), c


def device(x, y, z, c):
    x, y, z, c = lax.rem(x, 4), lax.rem(y, 4), lax.rem(z, 4), lax.rem(c, 2)
    return (lax.rem(x, 2) * 8 + y * 2 + c, lax.div(x, 2) * 4 + z)


def greet(peers):
    barrier = pltpu.get_barrier_semaphore()
    for peer in peers:
        pl.semaphore_signal(barrier, inc=1, device_id=peer, device_id_type=MESH)
    return lambda: pl.semaphore_wait(barrier, len(peers))


class Post:
    def __init__(self, send_sem, recv_sem):
        self.send_sem, self.recv_sem, self.copies = send_sem, recv_sem, []

    def send(self, src, dst, peer):
        i = len(self.copies)
        copy = pltpu.make_async_remote_copy(
            src_ref=src,
            dst_ref=dst,
            send_sem=self.send_sem.at[i],
            recv_sem=self.recv_sem.at[i],
            device_id=peer,
            device_id_type=MESH,
        )
        copy.start()
        self.copies.append(copy)
        return copy

    def close(self):
        for copy in self.copies:
            copy.wait_send()


def column(row):
    return jnp.transpose(jnp.broadcast_to(row, (128, 128)))


def at128(i):
    return pl.ds(pl.multiple_of(i * 128, 128), 128)


def kernel(loss_weight, width_in, hidden_in, w_in_in, embedding_in, gain_in, w_out, ids, *rest):
    grad_hidden, grad_in, grad_out = rest[:3]
    (
        hidden, w_in, embedding, part, relay, relay_sum, z_got, x_send, x_got,
        w_rows, w_got, w_full, ids_mine, ids_all,
        sq_mine, sq_all, ratio_rows, ratio_col, scaled, looked, x_rows, proj, normed, turned, logits,
        d_logit, scale_col, d_norm, dr_col, d_turn, d_all, small, small_all, corr_col,
        gp, gp_c, ga_y, ga_rel, ga_yg, ga_sum, ga_xg, gb_x, gb_rel, gb_xg, gb_sum, gb_yg,
        gp_z, gp_zg, gp_rows, gp_pair, ip, ip_c, ip_y, ip_rel, ip_yg, ip_x, ip_xg, local_sem, send_sem, recv_sem,
    ) = rest[3:]
    x, y, z, c = place()
    x_lo, x_hi, step, zh = lax.rem(x, 2), lax.div(x, 2), lax.rem(z, 2), lax.div(z, 2)
    hid = x_hi * 4 + z
    quarter = x_hi * 2 + zh
    pair = device(x, y, z + 1 - 2 * step, c)
    far = device(x + 2, y, z, c)
    twin = device(x, y, z, c + 1)
    beside = device(x + 1 - 2 * x_lo, y, z, c)
    xs = {d: device(x + d, y, z, c) for d in (1, 2, 3)}
    ys = {d: device(x, y + d, z, c) for d in (1, 2, 3)}
    zs = {d: device(x, y, z + d, c) for d in (1, 2, 3)}
    hid_peers = [device(x + dx, y, z + dz, c) for dz in (2, 1, 3, 0) for dx in (2, 0) if dx + dz]
    order = (2, 1, 3, 0)

    sources = (
        (hidden_in, hidden),
        (w_in_in.at[step], w_in.at[step]),
        (w_in_in.at[1 - step], w_in.at[1 - step]),
        (embedding_in, embedding),
    )
    loads = [
        pltpu.make_async_copy(src, dst, local_sem.at[i]) for i, (src, dst) in enumerate(sources)
    ]
    for load in loads:
        load.start()
    everyone_here = greet(hid_peers + [xs[1], xs[3]] + list(ys.values()) + [twin])
    w_rows[0] = w_out[:, 0, :]
    w_rows[1] = w_out[:, 1, :]
    ids_mine[...] = jnp.zeros_like(ids_mine)
    ids_mine[0:2, 0:64] = ids[...]
    ids_all[step] = ids_mine[...]
    w_got[z] = w_rows[step]

    def chunk(dz):
        to_z = lax.rem(z + dz, 4)
        rows = [hidden[at128(fx * 2 + lax.div(to_z, 2)), :] for fx in range(2)]
        product = jnp.dot(
            jnp.concatenate(rows, axis=0), w_in[lax.rem(to_z, 2)], preferred_element_type=F32
        ).astype(BF)
        part[dz, 0] = product[:128]
        part[dz, 1] = product[128:]

    loads[0].wait()
    loads[1].wait()
    chunk(2)
    everyone_here()
    post = Post(send_sem, recv_sem)

    bounds = ((0, 64), (64, 96), (96, 128))
    pieces = [pl.ds(a, b - a) for a, b in bounds]
    relays, z_copies = [[] for _ in pieces], [[] for _ in pieces]

    def send_opposite(p):
        rows = pieces[p]
        relays[p].append(post.send(part.at[2, 0, rows], relay.at[0, rows], zs[1]))
        relays[p].append(post.send(part.at[2, 1, rows], relay.at[1, rows], zs[3]))

    def send_direct(p, dz):
        rows, fx, slot = pieces[p], (1 if dz == 1 else 0), (0 if dz == 1 else 1)
        z_copies[p].append(post.send(part.at[dz, fx, rows], z_got.at[slot, fx, rows], zs[dz]))

    def send_sums(p):
        for fx, dz in ((0, 1), (1, 3)):
            rows = pieces[p]
            relays[p][fx].wait_recv()
            relay_sum[fx, rows, :] = (
                part[dz, fx, rows, :].astype(F32) + relay[fx, rows, :].astype(F32)
            ).astype(BF)
            z_copies[p].append(
                post.send(relay_sum.at[fx, rows], z_got.at[fx, fx, rows], zs[dz])
            )

    w_z = [post.send(w_rows.at[(step + d) % 2], w_got.at[z], zs[d]) for d in (2, 1, 3)]
    ids_swap = post.send(ids_mine, ids_all.at[step], pair)
    send_opposite(0)
    h = hidden[...].astype(F32)
    h2 = h * h
    top = h2.astype(BF)
    low = (h2 - top.astype(F32)).astype(BF)
    ones = jnp.ones((8, h2.shape[1]), BF)
    sq_mine[...] = lax.dot_general(ones, top, NT, preferred_element_type=F32) + lax.dot_general(
        ones, low, NT, preferred_element_type=F32
    )
    sq_all[hid] = sq_mine[...]
    loads[2].wait()
    chunk(1)
    send_direct(0, 1)
    sq_copies = [post.send(sq_mine, sq_all.at[hid], peer) for peer in hid_peers]
    chunk(3)
    send_direct(0, 3)
    for p in (1, 2):
        send_opposite(p)
        send_direct(p, 1)
        send_direct(p, 3)
    for copy in w_z:
        copy.wait_recv()
    for e in range(2):
        both = [w_got[2 * e + i].astype(F32) for i in range(2)]
        w_full[x_lo, y, c, x_hi, e] = jnp.concatenate(both, axis=0).astype(BF)
    block = w_full.at[x_lo, y, c, x_hi, zh]
    wa_x = [post.send(block, block, xs[d]) for d in (1, 3, 2)]
    block = w_full.at[x_lo, y, c, x_hi, 1 - zh]
    wb_y = [post.send(block, block, ys[d]) for d in (1, 3, 2)]
    chunk(0)
    send_sums(0)
    for copy in wa_x:
        copy.wait_recv()
    line = w_full.at[:, y, c, :, zh]
    wa_y = {d: post.send(line, line, ys[d]) for d in (2, 1, 3)}
    w_twin = [post.send(line, line, twin)]
    for copy in wb_y:
        copy.wait_recv()
    line = w_full.at[x_lo, :, c, x_hi, 1 - zh]
    wb_x = {d: post.send(line, line, xs[d]) for d in (2, 1, 3)}
    w_twin.append(post.send(line, line, twin))
    send_sums(1)
    send_sums(2)

    for copy in sq_copies:
        copy.wait_recv()
    squares = sq_all[0]
    for i in range(1, 8):
        squares = squares + sq_all[i]
    ratio_rows[...] = lax.rsqrt(squares / width_in + 1e-06)
    for q in range(4):
        wide = column(ratio_rows[0:1, q * 128 : (q + 1) * 128])
        scaled[q * 128 : (q + 1) * 128, :] = (
            hidden[q * 128 : (q + 1) * 128, :].astype(F32) * wide[:, :1]
        ).astype(BF)
    ratio_col[...] = column(ratio_rows[0:1, at128(quarter)])
    ids_swap.wait_recv()

    def tokens(k):
        parts = [column(ids_all[i, k : k + 1, :].astype(F32))[:64, :1] for i in range(2)]
        return jnp.concatenate(parts, axis=0).astype(jnp.int32)

    previous, current = tokens(0), tokens(1)
    target = jnp.where(step == 1, current, previous)
    entries = logits.shape[1]
    lanes = lax.broadcasted_iota(jnp.int32, (128, entries), 1)
    loads[3].wait()
    pick = jnp.where(lanes == previous, 1.0, 0.0).astype(BF)
    live = step.astype(F32)
    for n in range(2):
        cols = slice(n * 512, (n + 1) * 512)
        looked[:, cols] = jnp.dot(pick, embedding[:, cols], preferred_element_type=F32) * live

    def z_sum(fx, rows):
        return (
            part[0, fx, rows, :].astype(F32)
            + z_got[0, fx, rows, :].astype(F32)
            + z_got[1, fx, rows, :].astype(F32)
        )

    x_copies = []
    for p in range(3):
        for copy in z_copies[p]:
            copy.wait_recv()

        @pl.loop(bounds[p][0] // 16, bounds[p][1] // 16, unroll=True)
        def to_far(i):
            rows = pl.ds(pl.multiple_of(i * 16, 16), 16)
            x_send[rows, :] = z_sum(1 - x_hi, rows).astype(BF)

        x_copies.append(post.send(x_send.at[pieces[p]], x_got.at[pieces[p]], far))
    for d in (1, 3, 2):
        wa_y[d].wait_recv()
        line = w_full.at[:, lax.rem(y + 4 - d, 4), c, :, zh]
        w_twin.append(post.send(line, line, twin))
    for d in (1, 3, 2):
        wb_x[d].wait_recv()
        from_x = lax.rem(x + 4 - d, 4)
        line = w_full.at[lax.rem(from_x, 2), :, c, lax.div(from_x, 2), 1 - zh]
        w_twin.append(post.send(line, line, twin))
    gain = gain_in[pl.ds(step, 1), :]
    for p in range(3):
        x_copies[p].wait_recv()

        @pl.loop(bounds[p][0] // 16, bounds[p][1] // 16, unroll=True)
        def norm(i):
            rows = pl.ds(pl.multiple_of(i * 16, 16), 16)
            value = z_sum(x_hi, rows) + x_got[rows, :].astype(F32)
            proj[rows, :] = value
            value = ratio_col[rows, :1] * value + looked[rows, :]
            scale = lax.rsqrt(jnp.mean(value * value, axis=1, keepdims=True) + 1e-06)
            x_rows[rows, :] = value
            scale_col[rows, :] = jnp.broadcast_to(scale, (16, 128))
            normed[rows, :] = (value * scale * gain).astype(BF)

    for copy in w_twin:
        copy.wait_recv()

    depth = normed.shape[1]
    for n in range(4):
        cols = slice(n * 512, (n + 1) * 512)
        head = w_full[:, :, :, :, :, :, cols].reshape(depth, 512)
        logits[:, cols] = jnp.dot(normed[...], head, preferred_element_type=F32)
    dr_col[...] = jnp.broadcast_to(target.astype(F32), (128, 128))

    @pl.loop(0, 8, unroll=2)
    def soft(i):
        rows = pl.ds(pl.multiple_of(i * 16, 16), 16)
        value = logits[rows, :]
        value = jnp.exp(value - jnp.max(value, axis=1, keepdims=True))
        share = value * (loss_weight / jnp.sum(value, axis=1, keepdims=True))
        hot = lax.broadcasted_iota(jnp.int32, (16, entries), 1) == dr_col[rows, :1].astype(
            jnp.int32
        )
        d_logit[rows, :] = (share - jnp.where(hot, loss_weight, 0.0)).astype(BF)

    for k in range(4):
        a, b = k // 2, (k % 2) * 2
        head = w_full[a, b : b + 2].reshape(256, entries)
        d_norm[:, k * 256 : (k + 1) * 256] = lax.dot_general(
            d_logit[...], head, NT, preferred_element_type=F32
        )

    @pl.loop(0, 8, unroll=4)
    def unnorm(i):
        rows = pl.ds(pl.multiple_of(i * 16, 16), 16)
        value, scale = x_rows[rows, :], scale_col[rows, :1]
        gated = gain * d_norm[rows, :]
        inner = jnp.mean(gated * value, axis=1, keepdims=True)
        d_x = scale * gated - value * (scale * scale * scale * inner)
        d_norm[rows, :] = d_x
        total = jnp.sum(d_x * proj[rows, :], axis=1, keepdims=True)
        dr_col[rows, :] = jnp.broadcast_to(total, (16, 128))

    for k in range(8):
        d_turn[k // 4, k % 4] = jnp.transpose(d_norm[:, k * 128 : (k + 1) * 128]).astype(BF)
    lane = at128(quarter)

    def lane_of(fx, dz):
        return at128(fx * 2 + lax.div(lax.rem(z + dz, 4), 2))

    d_x_copies = []
    for d in order:
        to_y = lax.rem(y + d, 4)
        d_x_copies.append(
            post.send(d_turn.at[:, to_y], d_all.at[step, :, to_y, :, lane], far)
        )
    first_hop, second_hop = {}, [[], [], [], []]

    def send_own(i):
        to_y = lax.rem(y + order[i], 4)
        view = d_all.at[step, :, to_y, :, lane]
        first_hop[i, 0] = [post.send(d_turn.at[:, to_y], view, zs[d]) for d in (1, 3)]

    def send_far(i):
        to_y = lax.rem(y + order[i], 4)
        d_x_copies[i].wait_recv()
        view = d_all.at[step, :, to_y, :, lane_of(1 - x_hi, 0)]
        first_hop[i, 1] = [post.send(view, view, zs[d]) for d in (1, 3)]

    def forward(i, other):
        to_y = lax.rem(y + order[i], 4)
        fx = 1 - x_hi if other else x_hi
        for a, (dz, copy) in enumerate(zip((3, 1), first_hop[i, other])):
            copy.wait_recv()
            view = d_all.at[1 - step, a, to_y, :, lane_of(fx, dz)]
            second_hop[i].append(post.send(view, view, zs[4 - dz]))

    send_own(0)
    send_own(1)
    send_own(2)
    small[...] = jnp.transpose(dr_col[...])[:8]
    small_copies = [post.send(small, small_all.at[hid], peer) for peer in hid_peers]
    for b in range(4):
        for a in range(2):
            d_all[step, a, b, :, lane] = d_turn[a, b]
    small_all[hid] = small[...]

    for k in range(8):
        cols = slice(k * 128, (k + 1) * 128)
        turned[cols, :] = jnp.transpose(normed[:, cols].astype(F32)).astype(BF)
    gp_swap = []

    def product_out(i):
        to_y = lax.rem(y + order[i], 4)
        for a in range(2):
            rows = at128(a * 4 + to_y)
            gp[a, to_y] = (
                jnp.dot(turned[rows, :], d_logit[...], preferred_element_type=F32)
                .astype(BF)
                .reshape(2, 2, 2, 16, entries)
            )
        gp_swap.append(post.send(gp.at[:, to_y, 1 - c], gp_c.at[:, to_y], twin))

    for i in range(4):
        product_out(i)
    def core_sum(a, b, e, f):
        return gp[a, b, c, e, f].astype(F32) + gp_c[a, b, e, f].astype(F32)

    def ga_part(i, a, more=None):
        to_y = lax.rem(y + order[i], 4)
        for e in range(2):
            value = core_sum(a, to_y, e, zh)
            if more is not None:
                value = value + ga_rel[more, e].astype(F32)
            ga_y[i, a, e] = value.astype(BF)
        return ga_y.at[i, a]

    def gb_part(i, k, more=None):
        to_x = lax.rem(x + order[i], 4)
        for b in range(2):
            value = core_sum(lax.rem(to_x, 2), 2 * k + b, lax.div(to_x, 2), 1 - zh)
            if more is not None:
                value = value + gb_rel[more, b].astype(F32)
            gb_x[i, k, b] = value.astype(BF)
        return gb_x.at[i, k]

    gp_swap[0].wait_recv()
    ga_relay = [post.send(ga_part(0, a), ga_rel.at[a], ys[d]) for a, d in ((0, 1), (1, 3))]
    gp_swap[1].wait_recv()
    ga_ys = [post.send(ga_part(1, 1), ga_yg.at[0, 1], ys[1])]
    gp_swap[2].wait_recv()
    ga_ys.append(post.send(ga_part(2, 0), ga_yg.at[1, 0], ys[3]))
    gp_swap[3].wait_recv()
    gb_relay = [post.send(gb_part(0, k), gb_rel.at[k], xs[d]) for k, d in ((0, 1), (1, 3))]
    gb_xs = [
        post.send(gb_part(1, 1), gb_xg.at[0, 1], xs[1]),
        post.send(gb_part(2, 0), gb_xg.at[1, 0], xs[3]),
    ]
    forward(0, 0)
    send_far(0)
    forward(1, 0)
    send_own(3)
    send_far(1)
    forward(2, 0)
    ga_relay[0].wait_recv()
    ga_ys.append(post.send(ga_part(1, 0, 0), ga_yg.at[0, 0], ys[1]))
    ga_relay[1].wait_recv()
    ga_ys.append(post.send(ga_part(2, 1, 1), ga_yg.at[1, 1], ys[3]))
    send_far(2)
    forward(0, 1)
    gb_relay[0].wait_recv()
    gb_xs.append(post.send(gb_part(1, 0, 0), gb_xg.at[0, 0], xs[1]))
    gb_relay[1].wait_recv()
    gb_xs.append(post.send(gb_part(2, 1, 1), gb_xg.at[1, 1], xs[3]))
    forward(3, 0)
    send_far(3)
    forward(1, 1)

    ip_ys, ip_relay = [], []

    def product_in(i):
        for copy in second_hop[i]:
            copy.wait_recv()
        to_y = lax.rem(y + order[i], 4)
        rows = [d_all[s, a, to_y] for s in range(2) for a in range(2)]
        product = jnp.dot(
            jnp.concatenate(rows, axis=0), scaled[...], preferred_element_type=F32
        ).astype(BF)
        for s in range(2):
            for a in range(2):
                for e in range(2):
                    start = (s * 2 + a) * 128 + e * 64
                    ip[s, a, to_y, e] = product[start : start + 64]
        return post.send(ip.at[:, :, to_y, 1 - c], ip_c.at[:, :, to_y], twin)

    def sum_in(i, swap):
        swap.wait_recv()
        to_y = lax.rem(y + order[i], 4)
        if i:
            ip_relay[i - 1].wait_recv()
        for s in range(2):
            for a in range(2):
                value = ip[s, a, to_y, c].astype(F32) + ip_c[s, a, to_y].astype(F32)
                if s == i - 1:
                    value = value + ip_rel[s, a].astype(F32)
                ip_y[i, s, a] = value.astype(BF)
        if i:
            ip_ys.append(post.send(ip_y.at[i], ip_yg.at[i - 1], ys[order[i]]))
        else:
            for s, d in ((0, 1), (1, 3)):
                ip_relay.append(post.send(ip_y.at[0, s], ip_rel.at[s], ys[d]))

    swap = product_in(0)
    sum_in(0, swap)
    forward(2, 1)
    swap = product_in(1)
    sum_in(1, swap)
    forward(3, 1)
    for copy in ga_ys:
        copy.wait_recv()
    for a in range(2):
        for e in range(2):
            value = core_sum(a, y, e, zh)
            for i in range(2):
                value = value + ga_yg[i, a, e].astype(F32)
            ga_sum[a, e] = value.astype(BF)
    ga_xs = []
    for i, d in enumerate(order[:3]):
        to_x = lax.rem(x + d, 4)
        ga_xs.append(
            post.send(ga_sum.at[lax.rem(to_x, 2), lax.div(to_x, 2)], ga_xg.at[i], xs[d])
        )
    for copy in gb_xs:
        copy.wait_recv()
    for b in range(4):
        value = core_sum(x_lo, b, x_hi, 1 - zh)
        for i in range(2):
            value = value + gb_xg[i, b // 2, b % 2].astype(F32)
        gb_sum[b] = value.astype(BF)
    gb_ys = []
    for i, d in enumerate(order[:3]):
        gb_ys.append(post.send(gb_sum.at[lax.rem(y + d, 4)], gb_yg.at[i], ys[d]))
    swap = product_in(2)
    sum_in(2, swap)
    last_swap = product_in(3)

    for copy in gb_ys:
        copy.wait_recv()
    value = gb_sum[y].astype(F32)
    for i in range(3):
        value = value + gb_yg[i].astype(F32)
    gp_z[...] = value.astype(BF)
    gp_across = post.send(gp_z, gp_zg, zs[2])

    ratio_row = ratio_rows[0:1, :]
    for copy in small_copies:
        copy.wait_recv()
    for q in range(4):
        cols = slice(q * 128, (q + 1) * 128)
        r = ratio_rows[0:1, cols]
        total_dr = small_all[2 * q, 0:1, :] + small_all[2 * q + 1, 0:1, :]
        corr_col[cols, :] = column(r * r * r * total_dr * (1.0 / width_in))

    def back(k):
        cols = slice(k * 128, (k + 1) * 128)
        value = sum(
            jnp.dot(w_in[s, cols, :], d_all[s].reshape(depth, -1), preferred_element_type=F32)
            for s in range(2)
        )
        grad_hidden[:, cols] = (
            jnp.transpose(value * ratio_row)
            - corr_col[:, :1] * hidden[:, cols].astype(F32)
        ).astype(BF)

    back(0)
    back(1)
    for copy in ga_xs:
        copy.wait_recv()
    value = ga_sum[x_lo, x_hi].astype(F32)
    for i in range(3):
        value = value + ga_xg[i].astype(F32)
    gp_across.wait_recv()
    gp_rows[...] = value + gp_zg[...].astype(F32)
    theirs = gp_rows.at[pl.ds(pl.multiple_of((1 - step) * 8, 8), 8), :]
    gp_swap_rows = post.send(theirs, gp_pair, pair)
    last_swap.wait_recv()
    for copy in ip_ys:
        copy.wait_recv()

    def in_block(a, b):
        value = ip[a, b, y, c].astype(F32) + ip_c[a, b, y].astype(F32)
        for i in range(2):
            value = value + ip_yg[i, a, b].astype(F32)
        return value

    for a in range(2):
        ip_x[a] = in_block(a, 1 - x_lo).astype(BF)
    ip_beside = post.send(ip_x, ip_xg, beside)
    back(2)
    back(3)
    for a in range(2):
        grad_in[a] = in_block(a, x_lo)
    gp_swap_rows.wait_recv()
    grad_out[step] = gp_rows[pl.ds(pl.multiple_of(step * 8, 8), 8), :]
    grad_out[1 - step] = gp_pair[...]
    ip_beside.wait_recv()
    for a in range(2):
        grad_in[a] = grad_in[a] + ip_xg[a].astype(F32)
    post.close()


def finish(gh, gi, go, grad_hidden, grad_in, grad_out):
    grad_hidden[...] = gh[...]
    grad_in[...] = gi[...]
    grad_out[:, 0, :] = go[0]
    grad_out[:, 1, :] = go[1]


def shards(hidden, w_in, embedding, depth_gain, w_out, codebook_ids):
    hid_count = lax.axis_size("hid")
    seq_count = lax.axis_size("seq")
    width_in = hidden.shape[1] * hid_count
    depth = w_in.shape[2]
    entries = w_out.shape[2]
    frames, units = hidden.shape
    loss_weight = 2.0 * entries / (frames * seq_count)
    vmem = pl.BlockSpec(memory_space=pltpu.VMEM)
    anywhere = pl.BlockSpec(memory_space=pl.ANY)
    scratch = [
        ((frames, units), BF),
        ((2, units, depth), BF),
        ((entries, depth), BF),
        ((4, 2, 128, depth), BF),
        ((2, 128, depth), BF),
        ((2, 128, depth), BF),
        ((2, 2, 128, depth), BF),
        ((128, depth), BF),
        ((128, depth), BF),
        ((2, 8, entries), BF),
        ((4, 8, entries), BF),
        ((2, 4, 2, 2, 2, 16, entries), BF),
        ((8, 128), jnp.int32),
        ((2, 8, 128), jnp.int32),
        ((8, frames), F32),
        ((8, 8, frames), F32),
        ((8, frames), F32),
        ((128, 128), F32),
        ((frames, units), BF),
        ((128, depth), F32),
        ((128, depth), F32),
        ((128, depth), F32),
        ((128, depth), BF),
        ((depth, 128), BF),
        ((128, entries), F32),
        ((128, entries), BF),
        ((128, 128), F32),
        ((128, depth), F32),
        ((128, 128), F32),
        ((2, 4, 128, 128), BF),
        ((2, 2, 4, 128, frames), BF),
        ((8, 128), F32),
        ((8, 8, 128), F32),
        ((frames, 128), F32),
        ((2, 4, 2, 2, 2, 16, entries), BF),
        ((2, 4, 2, 2, 16, entries), BF),
        ((3, 2, 2, 16, entries), BF),
        ((2, 2, 16, entries), BF),
        ((2, 2, 2, 16, entries), BF),
        ((2, 2, 16, entries), BF),
        ((3, 16, entries), BF),
        ((3, 2, 2, 16, entries), BF),
        ((2, 2, 16, entries), BF),
        ((2, 2, 2, 16, entries), BF),
        ((4, 16, entries), BF),
        ((3, 16, entries), BF),
        ((16, entries), BF),
        ((16, entries), BF),
        ((16, entries), F32),
        ((8, entries), F32),
        ((2, 2, 4, 2, 64, units), BF),
        ((2, 2, 4, 64, units), BF),
        ((3, 2, 2, 64, units), BF),
        ((2, 2, 64, units), BF),
        ((2, 2, 2, 64, units), BF),
        ((2, 64, units), BF),
        ((2, 64, units), BF),
    ]
    grad_hidden, grad_in, grad_out = pl.pallas_call(
        functools.partial(kernel, loss_weight, width_in),
        out_shape=[
            jax.ShapeDtypeStruct((frames, units), BF),
            jax.ShapeDtypeStruct((2, 64, units), F32),
            jax.ShapeDtypeStruct((2, 8, entries), F32),
        ],
        in_specs=[anywhere] * 3 + [vmem] * 3,
        out_specs=[vmem] * 3,
        scratch_shapes=[pltpu.VMEM(shape, dtype) for shape, dtype in scratch]
        + [
            pltpu.SemaphoreType.DMA((4,)),
            pltpu.SemaphoreType.DMA((144,)),
            pltpu.SemaphoreType.DMA((144,)),
        ],
        compiler_params=pltpu.CompilerParams(
            collective_id=0, has_side_effects=True, vmem_limit_bytes=60 * 1024 * 1024
        ),
        name="whole",
    )(hidden, w_in, embedding[0], depth_gain, w_out, codebook_ids)
    grad_hidden, grad_in, grad_out = pl.pallas_call(
        finish,
        out_shape=[
            jax.ShapeDtypeStruct((frames, units), BF),
            jax.ShapeDtypeStruct((2, 64, units), F32),
            jax.ShapeDtypeStruct((8, 2, entries), F32),
        ],
        in_specs=[vmem] * 3,
        out_specs=[vmem] * 3,
        name="finish",
    )(grad_hidden, grad_in, grad_out)
    return grad_hidden, jnp.transpose(grad_in, (0, 2, 1)), grad_out


def solution(mesh):
    placed = (
        P("seq", "hid"),
        P(None, "hid", None),
        P(),
        P(),
        P(("seq", "hid"), None, None),
        P(None, ("seq", "hid")),
    )
    return jax.shard_map(
        shards,
        mesh=mesh,
        in_specs=placed,
        out_specs=(P("seq", "hid"), P(None, "hid", "seq"), P(("seq", "hid"), None, None)),
        check_vma=False,
    )
```

```python
import functools

import jax
import jax.numpy as jnp
from jax import lax
from jax.experimental import pallas as pl
from jax.experimental.pallas import tpu as pltpu
from jax.sharding import PartitionSpec as P

MESH = pl.DeviceIdType.MESH
BF = jnp.bfloat16
F32 = jnp.float32
NT = (((1,), (1,)), ((), ()))


def place():
    s, h = lax.axis_index("seq"), lax.axis_index("hid")
    x_lo, y, c = lax.div(s, 8), lax.rem(lax.div(s, 2), 4), lax.rem(s, 2)
    return 2 * lax.div(h, 4) + x_lo, y, lax.rem(h, 4), c


def device(x, y, z, c):
    x, y, z, c = lax.rem(x, 4), lax.rem(y, 4), lax.rem(z, 4), lax.rem(c, 2)
    return (lax.rem(x, 2) * 8 + y * 2 + c, lax.div(x, 2) * 4 + z)


def greet(peers):
    barrier = pltpu.get_barrier_semaphore()
    for peer in peers:
        pl.semaphore_signal(barrier, inc=1, device_id=peer, device_id_type=MESH)
    return lambda: pl.semaphore_wait(barrier, len(peers))


class Post:
    def __init__(self, send_sem, recv_sem):
        self.send_sem, self.recv_sem, self.copies = send_sem, recv_sem, []

    def send(self, src, dst, peer):
        i = len(self.copies)
        copy = pltpu.make_async_remote_copy(
            src_ref=src,
            dst_ref=dst,
            send_sem=self.send_sem.at[i],
            recv_sem=self.recv_sem.at[i],
            device_id=peer,
            device_id_type=MESH,
        )
        copy.start()
        self.copies.append(copy)
        return copy

    def close(self):
        for copy in self.copies:
            copy.wait_send()


def column(row):
    return jnp.transpose(jnp.broadcast_to(row, (128, 128)))


def at128(i):
    return pl.ds(pl.multiple_of(i * 128, 128), 128)


def kernel(loss_weight, width_in, hidden_in, w_in_in, embedding_in, gain_in, w_out, ids, *rest):
    grad_hidden, grad_in, grad_out = rest[:3]
    (
        hidden, w_in, embedding, part, relay, relay_sum, z_got, x_send, x_got,
        w_rows, w_got, w_full, ids_mine, ids_all,
        sq_mine, sq_all, ratio_rows, ratio_col, scaled, looked, x_rows, proj, normed, turned, logits,
        d_logit, scale_col, d_norm, dr_col, d_turn, d_all, small, small_all, corr_col,
        gp, gp_c, ga_y, ga_rel, ga_yg, ga_sum, ga_xg, gb_x, gb_rel, gb_xg, gb_sum, gb_yg,
        gp_z, gp_zg, gp_rows, gp_pair, ip, ip_c, ip_y, ip_rel, ip_yg, ip_x, ip_xg, local_sem, send_sem, recv_sem,
    ) = rest[3:]
    x, y, z, c = place()
    x_lo, x_hi, step, zh = lax.rem(x, 2), lax.div(x, 2), lax.rem(z, 2), lax.div(z, 2)
    hid = x_hi * 4 + z
    quarter = x_hi * 2 + zh
    pair = device(x, y, z + 1 - 2 * step, c)
    far = device(x + 2, y, z, c)
    twin = device(x, y, z, c + 1)
    beside = device(x + 1 - 2 * x_lo, y, z, c)
    xs = {d: device(x + d, y, z, c) for d in (1, 2, 3)}
    ys = {d: device(x, y + d, z, c) for d in (1, 2, 3)}
    zs = {d: device(x, y, z + d, c) for d in (1, 2, 3)}
    hid_peers = [device(x + dx, y, z + dz, c) for dz in (2, 1, 3, 0) for dx in (2, 0) if dx + dz]
    order = (2, 1, 3, 0)

    sources = (
        (hidden_in, hidden),
        (w_in_in.at[step], w_in.at[step]),
        (w_in_in.at[1 - step], w_in.at[1 - step]),
        (embedding_in, embedding),
    )
    loads = [
        pltpu.make_async_copy(src, dst, local_sem.at[i]) for i, (src, dst) in enumerate(sources)
    ]
    for load in loads:
        load.start()
    everyone_here = greet(hid_peers + [xs[1], xs[3]] + list(ys.values()) + [twin])
    w_rows[0] = w_out[:, 0, :]
    w_rows[1] = w_out[:, 1, :]
    ids_mine[...] = jnp.zeros_like(ids_mine)
    ids_mine[0:2, 0:64] = ids[...]
    ids_all[step] = ids_mine[...]
    w_got[z] = w_rows[step]

    def chunk(dz):
        to_z = lax.rem(z + dz, 4)
        rows = [hidden[at128(fx * 2 + lax.div(to_z, 2)), :] for fx in range(2)]
        product = jnp.dot(
            jnp.concatenate(rows, axis=0), w_in[lax.rem(to_z, 2)], preferred_element_type=F32
        ).astype(BF)
        part[dz, 0] = product[:128]
        part[dz, 1] = product[128:]

    loads[0].wait()
    loads[1].wait()
    chunk(2)
    everyone_here()
    post = Post(send_sem, recv_sem)

    bounds = ((0, 64), (64, 96), (96, 128))
    pieces = [pl.ds(a, b - a) for a, b in bounds]
    relays, z_copies = [[] for _ in pieces], [[] for _ in pieces]

    def send_opposite(p):
        rows = pieces[p]
        relays[p].append(post.send(part.at[2, 0, rows], relay.at[0, rows], zs[1]))
        relays[p].append(post.send(part.at[2, 1, rows], relay.at[1, rows], zs[3]))

    def send_direct(p, dz):
        rows, fx, slot = pieces[p], (1 if dz == 1 else 0), (0 if dz == 1 else 1)
        z_copies[p].append(post.send(part.at[dz, fx, rows], z_got.at[slot, fx, rows], zs[dz]))

    def send_sums(p):
        for fx, dz in ((0, 1), (1, 3)):
            rows = pieces[p]
            relays[p][fx].wait_recv()
            relay_sum[fx, rows, :] = (
                part[dz, fx, rows, :].astype(F32) + relay[fx, rows, :].astype(F32)
            ).astype(BF)
            z_copies[p].append(
                post.send(relay_sum.at[fx, rows], z_got.at[fx, fx, rows], zs[dz])
            )

    w_z = [post.send(w_rows.at[(step + d) % 2], w_got.at[z], zs[d]) for d in (2, 1, 3)]
    ids_swap = post.send(ids_mine, ids_all.at[step], pair)
    send_opposite(0)
    h = hidden[...].astype(F32)
    h2 = h * h
    top = h2.astype(BF)
    low = (h2 - top.astype(F32)).astype(BF)
    ones = jnp.ones((8, h2.shape[1]), BF)
    sq_mine[...] = lax.dot_general(ones, top, NT, preferred_element_type=F32) + lax.dot_general(
        ones, low, NT, preferred_element_type=F32
    )
    sq_all[hid] = sq_mine[...]
    loads[2].wait()
    chunk(1)
    send_direct(0, 1)
    sq_copies = [post.send(sq_mine, sq_all.at[hid], peer) for peer in hid_peers]
    chunk(3)
    send_direct(0, 3)
    for p in (1, 2):
        send_opposite(p)
        send_direct(p, 1)
        send_direct(p, 3)
    for copy in w_z:
        copy.wait_recv()
    for e in range(2):
        both = [w_got[2 * e + i].astype(F32) for i in range(2)]
        w_full[x_lo, y, c, x_hi, e] = jnp.concatenate(both, axis=0).astype(BF)
    block = w_full.at[x_lo, y, c, x_hi, zh]
    wa_x = [post.send(block, block, xs[d]) for d in (1, 3, 2)]
    block = w_full.at[x_lo, y, c, x_hi, 1 - zh]
    wb_y = [post.send(block, block, ys[d]) for d in (1, 3, 2)]
    chunk(0)
    send_sums(0)
    for copy in wa_x:
        copy.wait_recv()
    line = w_full.at[:, y, c, :, zh]
    wa_y = {d: post.send(line, line, ys[d]) for d in (2, 1, 3)}
    w_twin = [post.send(line, line, twin)]
    for copy in wb_y:
        copy.wait_recv()
    line = w_full.at[x_lo, :, c, x_hi, 1 - zh]
    wb_x = {d: post.send(line, line, xs[d]) for d in (2, 1, 3)}
    w_twin.append(post.send(line, line, twin))
    send_sums(1)
    send_sums(2)

    for copy in sq_copies:
        copy.wait_recv()
    squares = sq_all[0]
    for i in range(1, 8):
        squares = squares + sq_all[i]
    ratio_rows[...] = lax.rsqrt(squares / width_in + 1e-06)
    for q in range(4):
        wide = column(ratio_rows[0:1, q * 128 : (q + 1) * 128])
        scaled[q * 128 : (q + 1) * 128, :] = (
            hidden[q * 128 : (q + 1) * 128, :].astype(F32) * wide[:, :1]
        ).astype(BF)
    ratio_col[...] = column(ratio_rows[0:1, at128(quarter)])
    ids_swap.wait_recv()

    def tokens(k):
        parts = [column(ids_all[i, k : k + 1, :].astype(F32))[:64, :1] for i in range(2)]
        return jnp.concatenate(parts, axis=0).astype(jnp.int32)

    previous, current = tokens(0), tokens(1)
    target = jnp.where(step == 1, current, previous)
    entries = logits.shape[1]
    lanes = lax.broadcasted_iota(jnp.int32, (128, entries), 1)
    loads[3].wait()
    pick = jnp.where(lanes == previous, 1.0, 0.0).astype(BF)
    live = step.astype(F32)
    for n in range(2):
        cols = slice(n * 512, (n + 1) * 512)
        looked[:, cols] = jnp.dot(pick, embedding[:, cols], preferred_element_type=F32) * live

    def z_sum(fx, rows):
        return (
            part[0, fx, rows, :].astype(F32)
            + z_got[0, fx, rows, :].astype(F32)
            + z_got[1, fx, rows, :].astype(F32)
        )

    x_copies = []
    for p in range(3):
        for copy in z_copies[p]:
            copy.wait_recv()

        @pl.loop(bounds[p][0] // 16, bounds[p][1] // 16, unroll=True)
        def to_far(i):
            rows = pl.ds(pl.multiple_of(i * 16, 16), 16)
            x_send[rows, :] = z_sum(1 - x_hi, rows).astype(BF)

        x_copies.append(post.send(x_send.at[pieces[p]], x_got.at[pieces[p]], far))
    for d in (1, 3, 2):
        wa_y[d].wait_recv()
        line = w_full.at[:, lax.rem(y + 4 - d, 4), c, :, zh]
        w_twin.append(post.send(line, line, twin))
    for d in (1, 3, 2):
        wb_x[d].wait_recv()
        from_x = lax.rem(x + 4 - d, 4)
        line = w_full.at[lax.rem(from_x, 2), :, c, lax.div(from_x, 2), 1 - zh]
        w_twin.append(post.send(line, line, twin))
    gain = gain_in[pl.ds(step, 1), :]
    for p in range(3):
        x_copies[p].wait_recv()

        @pl.loop(bounds[p][0] // 16, bounds[p][1] // 16, unroll=True)
        def norm(i):
            rows = pl.ds(pl.multiple_of(i * 16, 16), 16)
            value = z_sum(x_hi, rows) + x_got[rows, :].astype(F32)
            proj[rows, :] = value
            value = ratio_col[rows, :1] * value + looked[rows, :]
            scale = lax.rsqrt(jnp.mean(value * value, axis=1, keepdims=True) + 1e-06)
            x_rows[rows, :] = value
            scale_col[rows, :] = jnp.broadcast_to(scale, (16, 128))
            normed[rows, :] = (value * scale * gain).astype(BF)

    for copy in w_twin:
        copy.wait_recv()

    depth = normed.shape[1]
    for n in range(4):
        cols = slice(n * 512, (n + 1) * 512)
        head = w_full[:, :, :, :, :, :, cols].reshape(depth, 512)
        logits[:, cols] = jnp.dot(normed[...], head, preferred_element_type=F32)
    dr_col[...] = jnp.broadcast_to(target.astype(F32), (128, 128))

    @pl.loop(0, 8, unroll=2)
    def soft(i):
        rows = pl.ds(pl.multiple_of(i * 16, 16), 16)
        value = logits[rows, :]
        value = jnp.exp(value - jnp.max(value, axis=1, keepdims=True))
        share = value * (loss_weight / jnp.sum(value, axis=1, keepdims=True))
        hot = lax.broadcasted_iota(jnp.int32, (16, entries), 1) == dr_col[rows, :1].astype(
            jnp.int32
        )
        d_logit[rows, :] = (share - jnp.where(hot, loss_weight, 0.0)).astype(BF)

    for k in range(4):
        a, b = k // 2, (k % 2) * 2
        head = w_full[a, b : b + 2].reshape(256, entries)
        d_norm[:, k * 256 : (k + 1) * 256] = lax.dot_general(
            d_logit[...], head, NT, preferred_element_type=F32
        )

    @pl.loop(0, 8, unroll=4)
    def unnorm(i):
        rows = pl.ds(pl.multiple_of(i * 16, 16), 16)
        value, scale = x_rows[rows, :], scale_col[rows, :1]
        gated = gain * d_norm[rows, :]
        inner = jnp.mean(gated * value, axis=1, keepdims=True)
        d_x = scale * gated - value * (scale * scale * scale * inner)
        d_norm[rows, :] = d_x
        total = jnp.sum(d_x * proj[rows, :], axis=1, keepdims=True)
        dr_col[rows, :] = jnp.broadcast_to(total, (16, 128))

    for k in range(8):
        d_turn[k // 4, k % 4] = jnp.transpose(d_norm[:, k * 128 : (k + 1) * 128]).astype(BF)
    lane, far_lane = at128(quarter), at128((1 - x_hi) * 2 + zh)

    def piece(k):
        return (1 - x_lo if k < 4 else x_lo), lax.rem(y + order[k % 4], 4)

    d_x_copies, d_z_copies = [], [[] for _ in range(8)]
    for k in range(8):
        b, to_y = piece(k)
        d_x_copies.append(post.send(d_turn.at[b, to_y], d_all.at[step, b, to_y, :, lane], far))

    def send_own(k):
        b, to_y = piece(k)
        view = d_all.at[step, b, to_y, :, lane]
        d_z_copies[k] += [post.send(d_turn.at[b, to_y], view, zs[d]) for d in (2, 1, 3)]

    def send_far(k):
        b, to_y = piece(k)
        d_x_copies[k].wait_recv()
        view = d_all.at[step, b, to_y, :, far_lane]
        d_z_copies[k] += [post.send(view, view, zs[d]) for d in (2, 1, 3)]

    for k in range(3):
        send_own(k)
    small[...] = jnp.transpose(dr_col[...])[:8]
    small_copies = [post.send(small, small_all.at[hid], peer) for peer in hid_peers]
    for b in range(4):
        for a in range(2):
            d_all[step, a, b, :, lane] = d_turn[a, b]
    small_all[hid] = small[...]

    for k in range(8):
        cols = slice(k * 128, (k + 1) * 128)
        turned[cols, :] = jnp.transpose(normed[:, cols].astype(F32)).astype(BF)
    gp_swap = []

    def product_out(i):
        to_y = lax.rem(y + order[i], 4)
        for a in range(2):
            rows = at128(a * 4 + to_y)
            gp[a, to_y] = (
                jnp.dot(turned[rows, :], d_logit[...], preferred_element_type=F32)
                .astype(BF)
                .reshape(2, 2, 2, 16, entries)
            )
        gp_swap.append(post.send(gp.at[:, to_y, 1 - c], gp_c.at[:, to_y], twin))

    for i in range(4):
        product_out(i)
    def core_sum(a, b, e, f):
        return gp[a, b, c, e, f].astype(F32) + gp_c[a, b, e, f].astype(F32)

    def ga_part(i, a, more=None):
        to_y = lax.rem(y + order[i], 4)
        for e in range(2):
            value = core_sum(a, to_y, e, zh)
            if more is not None:
                value = value + ga_rel[more, e].astype(F32)
            ga_y[i, a, e] = value.astype(BF)
        return ga_y.at[i, a]

    def gb_part(i, k, more=None):
        to_x = lax.rem(x + order[i], 4)
        for b in range(2):
            value = core_sum(lax.rem(to_x, 2), 2 * k + b, lax.div(to_x, 2), 1 - zh)
            if more is not None:
                value = value + gb_rel[more, b].astype(F32)
            gb_x[i, k, b] = value.astype(BF)
        return gb_x.at[i, k]

    gp_swap[0].wait_recv()
    ga_relay = [post.send(ga_part(0, a), ga_rel.at[a], ys[d]) for a, d in ((0, 1), (1, 3))]
    gp_swap[1].wait_recv()
    ga_ys = [post.send(ga_part(1, 1), ga_yg.at[0, 1], ys[1])]
    gp_swap[2].wait_recv()
    ga_ys.append(post.send(ga_part(2, 0), ga_yg.at[1, 0], ys[3]))
    gp_swap[3].wait_recv()
    gb_relay = [post.send(gb_part(0, k), gb_rel.at[k], xs[d]) for k, d in ((0, 1), (1, 3))]
    gb_xs = [
        post.send(gb_part(1, 1), gb_xg.at[0, 1], xs[1]),
        post.send(gb_part(2, 0), gb_xg.at[1, 0], xs[3]),
    ]
    for k in range(8):
        send_far(k)
        if k < 5:
            send_own(k + 3)
    ga_relay[0].wait_recv()
    ga_ys.append(post.send(ga_part(1, 0, 0), ga_yg.at[0, 0], ys[1]))
    ga_relay[1].wait_recv()
    ga_ys.append(post.send(ga_part(2, 1, 1), ga_yg.at[1, 1], ys[3]))

    ip_ys, ip_relay = [[], []], [[], []]

    def grad_in_piece(k):
        for copy in d_z_copies[k]:
            copy.wait_recv()
        b, to_y = piece(k)
        late, i = k // 4, k % 4
        rows = [d_all[s, b, to_y] for s in range(2)]
        product = jnp.dot(
            jnp.concatenate(rows, axis=0), scaled[...], preferred_element_type=F32
        ).astype(BF)
        for s in range(2):
            for e in range(2):
                start = s * 128 + e * 64
                ip[late, to_y, e, s] = product[start : start + 64]
        swap = post.send(ip.at[late, to_y, 1 - c], ip_c.at[late, to_y], twin)
        swap.wait_recv()
        if i == 3:
            return
        if i:
            ip_relay[late][i - 1].wait_recv()
        for s in range(2):
            value = ip[late, to_y, c, s].astype(F32) + ip_c[late, to_y, s].astype(F32)
            if s == i - 1:
                value = value + ip_rel[late, s].astype(F32)
            ip_y[late, i, s] = value.astype(BF)
        if i:
            ip_ys[late].append(
                post.send(ip_y.at[late, i], ip_yg.at[late, i - 1], ys[order[i]])
            )
        else:
            for s, d in ((0, 1), (1, 3)):
                ip_relay[late].append(post.send(ip_y.at[late, 0, s], ip_rel.at[late, s], ys[d]))

    def in_block(late, s):
        value = ip[late, y, c, s].astype(F32) + ip_c[late, y, s].astype(F32)
        for i in range(2):
            value = value + ip_yg[late, i, s].astype(F32)
        return value

    grad_in_piece(0)
    gb_relay[0].wait_recv()
    gb_xs.append(post.send(gb_part(1, 0, 0), gb_xg.at[0, 0], xs[1]))
    gb_relay[1].wait_recv()
    gb_xs.append(post.send(gb_part(2, 1, 1), gb_xg.at[1, 1], xs[3]))
    grad_in_piece(1)
    grad_in_piece(2)
    for copy in ga_ys:
        copy.wait_recv()
    for a in range(2):
        for e in range(2):
            value = core_sum(a, y, e, zh)
            for i in range(2):
                value = value + ga_yg[i, a, e].astype(F32)
            ga_sum[a, e] = value.astype(BF)
    ga_xs = []
    for i, d in enumerate(order[:3]):
        to_x = lax.rem(x + d, 4)
        ga_xs.append(
            post.send(ga_sum.at[lax.rem(to_x, 2), lax.div(to_x, 2)], ga_xg.at[i], xs[d])
        )
    for copy in gb_xs:
        copy.wait_recv()
    for b in range(4):
        value = core_sum(x_lo, b, x_hi, 1 - zh)
        for i in range(2):
            value = value + gb_xg[i, b // 2, b % 2].astype(F32)
        gb_sum[b] = value.astype(BF)
    gb_ys = []
    for i, d in enumerate(order[:3]):
        gb_ys.append(post.send(gb_sum.at[lax.rem(y + d, 4)], gb_yg.at[i], ys[d]))
    grad_in_piece(3)
    grad_in_piece(4)
    for copy in ip_ys[0]:
        copy.wait_recv()
    for s in range(2):
        ip_x[s] = in_block(0, s).astype(BF)
    ip_beside = post.send(ip_x, ip_xg, beside)
    grad_in_piece(5)
    for copy in gb_ys:
        copy.wait_recv()
    value = gb_sum[y].astype(F32)
    for i in range(3):
        value = value + gb_yg[i].astype(F32)
    gp_z[...] = value.astype(BF)
    gp_across = post.send(gp_z, gp_zg, zs[2])
    grad_in_piece(6)
    for copy in ga_xs:
        copy.wait_recv()
    value = ga_sum[x_lo, x_hi].astype(F32)
    for i in range(3):
        value = value + ga_xg[i].astype(F32)
    gp_rows[...] = value
    grad_in_piece(7)

    ratio_row = ratio_rows[0:1, :]
    for copy in small_copies:
        copy.wait_recv()
    for q in range(4):
        cols = slice(q * 128, (q + 1) * 128)
        r = ratio_rows[0:1, cols]
        total_dr = small_all[2 * q, 0:1, :] + small_all[2 * q + 1, 0:1, :]
        corr_col[cols, :] = column(r * r * r * total_dr * (1.0 / width_in))

    def back(k):
        cols = slice(k * 128, (k + 1) * 128)
        value = sum(
            jnp.dot(w_in[s, cols, :], d_all[s].reshape(depth, -1), preferred_element_type=F32)
            for s in range(2)
        )
        grad_hidden[:, cols] = (
            jnp.transpose(value * ratio_row)
            - corr_col[:, :1] * hidden[:, cols].astype(F32)
        ).astype(BF)

    back(0)
    back(1)
    gp_across.wait_recv()
    gp_rows[...] = gp_rows[...] + gp_zg[...].astype(F32)
    theirs = gp_rows.at[pl.ds(pl.multiple_of((1 - step) * 8, 8), 8), :]
    gp_swap_rows = post.send(theirs, gp_pair, pair)
    back(2)
    back(3)
    ip_beside.wait_recv()
    for copy in ip_ys[1]:
        copy.wait_recv()
    for s in range(2):
        grad_in[s] = in_block(1, s) + ip_xg[s].astype(F32)
    gp_swap_rows.wait_recv()
    grad_out[step] = gp_rows[pl.ds(pl.multiple_of(step * 8, 8), 8), :]
    grad_out[1 - step] = gp_pair[...]
    post.close()


def finish(gh, gi, go, grad_hidden, grad_in, grad_out):
    grad_hidden[...] = gh[...]
    grad_in[...] = gi[...]
    grad_out[:, 0, :] = go[0]
    grad_out[:, 1, :] = go[1]


def shards(hidden, w_in, embedding, depth_gain, w_out, codebook_ids):
    hid_count = lax.axis_size("hid")
    seq_count = lax.axis_size("seq")
    width_in = hidden.shape[1] * hid_count
    depth = w_in.shape[2]
    entries = w_out.shape[2]
    frames, units = hidden.shape
    loss_weight = 2.0 * entries / (frames * seq_count)
    vmem = pl.BlockSpec(memory_space=pltpu.VMEM)
    anywhere = pl.BlockSpec(memory_space=pl.ANY)
    scratch = [
        ((frames, units), BF),
        ((2, units, depth), BF),
        ((entries, depth), BF),
        ((4, 2, 128, depth), BF),
        ((2, 128, depth), BF),
        ((2, 128, depth), BF),
        ((2, 2, 128, depth), BF),
        ((128, depth), BF),
        ((128, depth), BF),
        ((2, 8, entries), BF),
        ((4, 8, entries), BF),
        ((2, 4, 2, 2, 2, 16, entries), BF),
        ((8, 128), jnp.int32),
        ((2, 8, 128), jnp.int32),
        ((8, frames), F32),
        ((8, 8, frames), F32),
        ((8, frames), F32),
        ((128, 128), F32),
        ((frames, units), BF),
        ((128, depth), F32),
        ((128, depth), F32),
        ((128, depth), F32),
        ((128, depth), BF),
        ((depth, 128), BF),
        ((128, entries), F32),
        ((128, entries), BF),
        ((128, 128), F32),
        ((128, depth), F32),
        ((128, 128), F32),
        ((2, 4, 128, 128), BF),
        ((2, 2, 4, 128, frames), BF),
        ((8, 128), F32),
        ((8, 8, 128), F32),
        ((frames, 128), F32),
        ((2, 4, 2, 2, 2, 16, entries), BF),
        ((2, 4, 2, 2, 16, entries), BF),
        ((3, 2, 2, 16, entries), BF),
        ((2, 2, 16, entries), BF),
        ((2, 2, 2, 16, entries), BF),
        ((2, 2, 16, entries), BF),
        ((3, 16, entries), BF),
        ((3, 2, 2, 16, entries), BF),
        ((2, 2, 16, entries), BF),
        ((2, 2, 2, 16, entries), BF),
        ((4, 16, entries), BF),
        ((3, 16, entries), BF),
        ((16, entries), BF),
        ((16, entries), BF),
        ((16, entries), F32),
        ((8, entries), F32),
        ((2, 4, 2, 2, 64, units), BF),
        ((2, 4, 2, 64, units), BF),
        ((2, 3, 2, 64, units), BF),
        ((2, 2, 64, units), BF),
        ((2, 2, 2, 64, units), BF),
        ((2, 64, units), BF),
        ((2, 64, units), BF),
    ]
    grad_hidden, grad_in, grad_out = pl.pallas_call(
        functools.partial(kernel, loss_weight, width_in),
        out_shape=[
            jax.ShapeDtypeStruct((frames, units), BF),
            jax.ShapeDtypeStruct((2, 64, units), F32),
            jax.ShapeDtypeStruct((2, 8, entries), F32),
        ],
        in_specs=[anywhere] * 3 + [vmem] * 3,
        out_specs=[vmem] * 3,
        scratch_shapes=[pltpu.VMEM(shape, dtype) for shape, dtype in scratch]
        + [
            pltpu.SemaphoreType.DMA((4,)),
            pltpu.SemaphoreType.DMA((176,)),
            pltpu.SemaphoreType.DMA((176,)),
        ],
        compiler_params=pltpu.CompilerParams(
            collective_id=0, has_side_effects=True, vmem_limit_bytes=62 * 1024 * 1024
        ),
        name="whole",
    )(hidden, w_in, embedding[0], depth_gain, w_out, codebook_ids)
    grad_hidden, grad_in, grad_out = pl.pallas_call(
        finish,
        out_shape=[
            jax.ShapeDtypeStruct((frames, units), BF),
            jax.ShapeDtypeStruct((2, 64, units), F32),
            jax.ShapeDtypeStruct((8, 2, entries), F32),
        ],
        in_specs=[vmem] * 3,
        out_specs=[vmem] * 3,
        compiler_params=pltpu.CompilerParams(vmem_limit_bytes=4 * 1024 * 1024),
        name="finish",
    )(grad_hidden, grad_in, grad_out)
    return grad_hidden, jnp.transpose(grad_in, (0, 2, 1)), grad_out


def solution(mesh):
    placed = (
        P("seq", "hid"),
        P(None, "hid", None),
        P(),
        P(),
        P(("seq", "hid"), None, None),
        P(None, ("seq", "hid")),
    )
    return jax.shard_map(
        shards,
        mesh=mesh,
        in_specs=placed,
        out_specs=(P("seq", "hid"), P(None, "hid", "seq"), P(("seq", "hid"), None, None)),
        check_vma=False,
    )
```

```python
import functools

import jax
import jax.numpy as jnp
from jax import lax
from jax.experimental import pallas as pl
from jax.experimental.pallas import tpu as pltpu
from jax.sharding import PartitionSpec as P

MESH = pl.DeviceIdType.MESH
BF = jnp.bfloat16
F32 = jnp.float32
NT = (((1,), (1,)), ((), ()))


def place():
    s, h = lax.axis_index("seq"), lax.axis_index("hid")
    x_lo, y, c = lax.div(s, 8), lax.rem(lax.div(s, 2), 4), lax.rem(s, 2)
    return 2 * lax.div(h, 4) + x_lo, y, lax.rem(h, 4), c


def device(x, y, z, c):
    x, y, z, c = lax.rem(x, 4), lax.rem(y, 4), lax.rem(z, 4), lax.rem(c, 2)
    return (lax.rem(x, 2) * 8 + y * 2 + c, lax.div(x, 2) * 4 + z)


def greet(peers):
    barrier = pltpu.get_barrier_semaphore()
    for peer in peers:
        pl.semaphore_signal(barrier, inc=1, device_id=peer, device_id_type=MESH)
    return lambda: pl.semaphore_wait(barrier, len(peers))


class Post:
    def __init__(self, send_sem, recv_sem):
        self.send_sem, self.recv_sem, self.copies = send_sem, recv_sem, []

    def send(self, src, dst, peer):
        i = len(self.copies)
        copy = pltpu.make_async_remote_copy(
            src_ref=src,
            dst_ref=dst,
            send_sem=self.send_sem.at[i],
            recv_sem=self.recv_sem.at[i],
            device_id=peer,
            device_id_type=MESH,
        )
        copy.start()
        self.copies.append(copy)
        return copy

    def close(self):
        for copy in self.copies:
            copy.wait_send()


def column(row):
    return jnp.transpose(jnp.broadcast_to(row, (128, 128)))


def at128(i):
    return pl.ds(pl.multiple_of(i * 128, 128), 128)


def kernel(loss_weight, width_in, hidden_in, w_in_in, embedding_in, gain_in, w_out, ids, *rest):
    grad_hidden, grad_in, grad_out = rest[:3]
    (
        hidden, w_in, embedding, part, relay, relay_sum, z_got, x_send, x_got,
        w_rows, w_got, w_full, ids_mine, ids_all,
        sq_mine, sq_all, ratio_rows, ratio_col, scaled, looked, x_rows, proj, normed, turned, logits,
        d_logit, scale_col, d_norm, dr_col, d_turn, d_all, small, small_all, corr_col,
        gp, gp_c, ga_y, ga_rel, ga_yg, ga_sum, ga_xg, gb_x, gb_rel, gb_xg, gb_sum, gb_yg,
        gp_z, gp_zg, gp_rows, gp_pair, ip, ip_c, ip_y, ip_rel, ip_yg, ip_x, ip_xg, local_sem, send_sem, recv_sem,
    ) = rest[3:]
    x, y, z, c = place()
    x_lo, x_hi, step, zh = lax.rem(x, 2), lax.div(x, 2), lax.rem(z, 2), lax.div(z, 2)
    hid = x_hi * 4 + z
    quarter = x_hi * 2 + zh
    pair = device(x, y, z + 1 - 2 * step, c)
    far = device(x + 2, y, z, c)
    twin = device(x, y, z, c + 1)
    beside = device(x + 1 - 2 * x_lo, y, z, c)
    xs = {d: device(x + d, y, z, c) for d in (1, 2, 3)}
    ys = {d: device(x, y + d, z, c) for d in (1, 2, 3)}
    zs = {d: device(x, y, z + d, c) for d in (1, 2, 3)}
    hid_peers = [device(x + dx, y, z + dz, c) for dz in (2, 1, 3, 0) for dx in (2, 0) if dx + dz]
    order = (2, 1, 3, 0)

    sources = (
        (hidden_in, hidden),
        (w_in_in.at[step], w_in.at[step]),
        (w_in_in.at[1 - step], w_in.at[1 - step]),
        (embedding_in, embedding),
    )
    loads = [
        pltpu.make_async_copy(src, dst, local_sem.at[i]) for i, (src, dst) in enumerate(sources)
    ]
    for load in loads:
        load.start()
    everyone_here = greet(hid_peers + [xs[1], xs[3]] + list(ys.values()) + [twin])
    w_rows[0] = w_out[:, 0, :]
    w_rows[1] = w_out[:, 1, :]
    ids_mine[...] = jnp.zeros_like(ids_mine)
    ids_mine[0:2, 0:64] = ids[...]
    ids_all[step] = ids_mine[...]
    w_got[z] = w_rows[step]

    def chunk(dz):
        to_z = lax.rem(z + dz, 4)
        rows = [hidden[at128(fx * 2 + lax.div(to_z, 2)), :] for fx in range(2)]
        product = jnp.dot(
            jnp.concatenate(rows, axis=0), w_in[lax.rem(to_z, 2)], preferred_element_type=F32
        ).astype(BF)
        part[dz, 0] = product[:128]
        part[dz, 1] = product[128:]

    loads[0].wait()
    loads[1].wait()
    chunk(2)
    everyone_here()
    post = Post(send_sem, recv_sem)

    bounds = ((0, 64), (64, 96), (96, 128))
    pieces = [pl.ds(a, b - a) for a, b in bounds]
    relays, z_copies = [[] for _ in pieces], [[] for _ in pieces]

    def send_opposite(p):
        rows = pieces[p]
        relays[p].append(post.send(part.at[2, 0, rows], relay.at[0, rows], zs[1]))
        relays[p].append(post.send(part.at[2, 1, rows], relay.at[1, rows], zs[3]))

    def send_direct(p, dz):
        rows, fx, slot = pieces[p], (1 if dz == 1 else 0), (0 if dz == 1 else 1)
        z_copies[p].append(post.send(part.at[dz, fx, rows], z_got.at[slot, fx, rows], zs[dz]))

    def send_sums(p):
        for fx, dz in ((0, 1), (1, 3)):
            rows = pieces[p]
            relays[p][fx].wait_recv()
            relay_sum[fx, rows, :] = (
                part[dz, fx, rows, :].astype(F32) + relay[fx, rows, :].astype(F32)
            ).astype(BF)
            z_copies[p].append(
                post.send(relay_sum.at[fx, rows], z_got.at[fx, fx, rows], zs[dz])
            )

    w_z = [post.send(w_rows.at[(step + d) % 2], w_got.at[z], zs[d]) for d in (2, 1, 3)]
    ids_swap = post.send(ids_mine, ids_all.at[step], pair)
    send_opposite(0)
    h = hidden[...].astype(F32)
    h2 = h * h
    top = h2.astype(BF)
    low = (h2 - top.astype(F32)).astype(BF)
    ones = jnp.ones((8, h2.shape[1]), BF)
    sq_mine[...] = lax.dot_general(ones, top, NT, preferred_element_type=F32) + lax.dot_general(
        ones, low, NT, preferred_element_type=F32
    )
    sq_all[hid] = sq_mine[...]
    loads[2].wait()
    chunk(1)
    send_direct(0, 1)
    sq_copies = [post.send(sq_mine, sq_all.at[hid], peer) for peer in hid_peers]
    chunk(3)
    send_direct(0, 3)
    for p in (1, 2):
        send_opposite(p)
        send_direct(p, 1)
        send_direct(p, 3)
    for copy in w_z:
        copy.wait_recv()
    for e in range(2):
        both = [w_got[2 * e + i].astype(F32) for i in range(2)]
        w_full[x_lo, y, c, x_hi, e] = jnp.concatenate(both, axis=0).astype(BF)
    block = w_full.at[x_lo, y, c, x_hi, zh]
    wa_x = [post.send(block, block, xs[d]) for d in (1, 3, 2)]
    block = w_full.at[x_lo, y, c, x_hi, 1 - zh]
    wb_y = [post.send(block, block, ys[d]) for d in (1, 3, 2)]
    chunk(0)
    send_sums(0)
    for copy in wa_x:
        copy.wait_recv()
    line = w_full.at[:, y, c, :, zh]
    wa_y = {d: post.send(line, line, ys[d]) for d in (2, 1, 3)}
    w_twin = [post.send(line, line, twin)]
    for copy in wb_y:
        copy.wait_recv()
    line = w_full.at[x_lo, :, c, x_hi, 1 - zh]
    wb_x = {d: post.send(line, line, xs[d]) for d in (2, 1, 3)}
    w_twin.append(post.send(line, line, twin))
    send_sums(1)
    send_sums(2)

    for copy in sq_copies:
        copy.wait_recv()
    squares = sq_all[0]
    for i in range(1, 8):
        squares = squares + sq_all[i]
    ratio_rows[...] = lax.rsqrt(squares / width_in + 1e-06)
    for q in range(4):
        wide = column(ratio_rows[0:1, q * 128 : (q + 1) * 128])
        scaled[q * 128 : (q + 1) * 128, :] = (
            hidden[q * 128 : (q + 1) * 128, :].astype(F32) * wide[:, :1]
        ).astype(BF)
    ratio_col[...] = column(ratio_rows[0:1, at128(quarter)])
    ids_swap.wait_recv()

    def tokens(k):
        parts = [column(ids_all[i, k : k + 1, :].astype(F32))[:64, :1] for i in range(2)]
        return jnp.concatenate(parts, axis=0).astype(jnp.int32)

    previous, current = tokens(0), tokens(1)
    target = jnp.where(step == 1, current, previous)
    entries = logits.shape[1]
    lanes = lax.broadcasted_iota(jnp.int32, (128, entries), 1)
    loads[3].wait()
    pick = jnp.where(lanes == previous, 1.0, 0.0).astype(BF)
    live = step.astype(F32)
    for n in range(2):
        cols = slice(n * 512, (n + 1) * 512)
        looked[:, cols] = jnp.dot(pick, embedding[:, cols], preferred_element_type=F32) * live

    def z_sum(fx, rows):
        return (
            part[0, fx, rows, :].astype(F32)
            + z_got[0, fx, rows, :].astype(F32)
            + z_got[1, fx, rows, :].astype(F32)
        )

    x_copies = []
    for p in range(3):
        for copy in z_copies[p]:
            copy.wait_recv()

        @pl.loop(bounds[p][0] // 16, bounds[p][1] // 16, unroll=True)
        def to_far(i):
            rows = pl.ds(pl.multiple_of(i * 16, 16), 16)
            x_send[rows, :] = z_sum(1 - x_hi, rows).astype(BF)

        x_copies.append(post.send(x_send.at[pieces[p]], x_got.at[pieces[p]], far))
    for d in (1, 3, 2):
        wa_y[d].wait_recv()
        line = w_full.at[:, lax.rem(y + 4 - d, 4), c, :, zh]
        w_twin.append(post.send(line, line, twin))
    for d in (1, 3, 2):
        wb_x[d].wait_recv()
        from_x = lax.rem(x + 4 - d, 4)
        line = w_full.at[lax.rem(from_x, 2), :, c, lax.div(from_x, 2), 1 - zh]
        w_twin.append(post.send(line, line, twin))
    gain = gain_in[pl.ds(step, 1), :]
    for p in range(3):
        x_copies[p].wait_recv()

        @pl.loop(bounds[p][0] // 16, bounds[p][1] // 16, unroll=True)
        def norm(i):
            rows = pl.ds(pl.multiple_of(i * 16, 16), 16)
            value = z_sum(x_hi, rows) + x_got[rows, :].astype(F32)
            proj[rows, :] = value
            value = ratio_col[rows, :1] * value + looked[rows, :]
            scale = lax.rsqrt(jnp.mean(value * value, axis=1, keepdims=True) + 1e-06)
            x_rows[rows, :] = value
            scale_col[rows, :] = jnp.broadcast_to(scale, (16, 128))
            normed[rows, :] = (value * scale * gain).astype(BF)

    for copy in w_twin:
        copy.wait_recv()

    depth = normed.shape[1]
    for n in range(4):
        cols = slice(n * 512, (n + 1) * 512)
        head = w_full[:, :, :, :, :, :, cols].reshape(depth, 512)
        logits[:, cols] = jnp.dot(normed[...], head, preferred_element_type=F32)
    dr_col[...] = jnp.broadcast_to(target.astype(F32), (128, 128))

    @pl.loop(0, 8, unroll=4)
    def soft(i):
        rows = pl.ds(pl.multiple_of(i * 16, 16), 16)
        value = logits[rows, :]
        value = jnp.exp(value - jnp.max(value, axis=1, keepdims=True))
        share = value * (loss_weight / jnp.sum(value, axis=1, keepdims=True))
        hot = lax.broadcasted_iota(jnp.int32, (16, entries), 1) == dr_col[rows, :1].astype(
            jnp.int32
        )
        d_logit[rows, :] = (share - jnp.where(hot, loss_weight, 0.0)).astype(BF)

    for k in range(4):
        a, b = k // 2, (k % 2) * 2
        head = w_full[a, b : b + 2].reshape(256, entries)
        d_norm[:, k * 256 : (k + 1) * 256] = lax.dot_general(
            d_logit[...], head, NT, preferred_element_type=F32
        )

    @pl.loop(0, 8, unroll=8)
    def unnorm(i):
        rows = pl.ds(pl.multiple_of(i * 16, 16), 16)
        value, scale = x_rows[rows, :], scale_col[rows, :1]
        gated = gain * d_norm[rows, :]
        inner = jnp.mean(gated * value, axis=1, keepdims=True)
        d_x = scale * gated - value * (scale * scale * scale * inner)
        d_norm[rows, :] = d_x
        total = jnp.sum(d_x * proj[rows, :], axis=1, keepdims=True)
        dr_col[rows, :] = jnp.broadcast_to(total, (16, 128))

    for k in range(8):
        d_turn[k // 4, k % 4] = jnp.transpose(d_norm[:, k * 128 : (k + 1) * 128]).astype(BF)
    lane, far_lane = at128(quarter), at128((1 - x_hi) * 2 + zh)

    def piece(k):
        return (1 - x_lo if k < 4 else x_lo), lax.rem(y + order[k % 4], 4)

    d_x_copies, d_z_copies = [], [[] for _ in range(8)]
    for k in range(8):
        b, to_y = piece(k)
        d_x_copies.append(post.send(d_turn.at[b, to_y], d_all.at[step, b, to_y, :, lane], far))

    def send_own(k):
        b, to_y = piece(k)
        view = d_all.at[step, b, to_y, :, lane]
        d_z_copies[k] += [post.send(d_turn.at[b, to_y], view, zs[d]) for d in (2, 1, 3)]

    def send_far(k):
        b, to_y = piece(k)
        d_x_copies[k].wait_recv()
        view = d_all.at[step, b, to_y, :, far_lane]
        d_z_copies[k] += [post.send(view, view, zs[d]) for d in (2, 1, 3)]

    for k in range(3):
        send_own(k)
    small[...] = jnp.transpose(dr_col[...])[:8]
    small_copies = [post.send(small, small_all.at[hid], peer) for peer in hid_peers]
    for b in range(4):
        for a in range(2):
            d_all[step, a, b, :, lane] = d_turn[a, b]
    small_all[hid] = small[...]

    for k in range(8):
        cols = slice(k * 128, (k + 1) * 128)
        turned[cols, :] = jnp.transpose(normed[:, cols].astype(F32)).astype(BF)
    gp_swap = []

    def product_out(i):
        to_y = lax.rem(y + order[i], 4)
        for a in range(2):
            rows = at128(a * 4 + to_y)
            gp[a, to_y] = (
                jnp.dot(turned[rows, :], d_logit[...], preferred_element_type=F32)
                .astype(BF)
                .reshape(2, 2, 2, 16, entries)
            )
        gp_swap.append(post.send(gp.at[:, to_y, 1 - c], gp_c.at[:, to_y], twin))

    for i in range(4):
        product_out(i)
    def core_sum(a, b, e, f):
        return gp[a, b, c, e, f].astype(F32) + gp_c[a, b, e, f].astype(F32)

    def ga_part(i, a, more=None):
        to_y = lax.rem(y + order[i], 4)
        for e in range(2):
            value = core_sum(a, to_y, e, zh)
            if more is not None:
                value = value + ga_rel[more, e].astype(F32)
            ga_y[i, a, e] = value.astype(BF)
        return ga_y.at[i, a]

    def gb_part(i, k, more=None):
        to_x = lax.rem(x + order[i], 4)
        for b in range(2):
            value = core_sum(lax.rem(to_x, 2), 2 * k + b, lax.div(to_x, 2), 1 - zh)
            if more is not None:
                value = value + gb_rel[more, b].astype(F32)
            gb_x[i, k, b] = value.astype(BF)
        return gb_x.at[i, k]

    gp_swap[0].wait_recv()
    ga_relay = [post.send(ga_part(0, a), ga_rel.at[a], ys[d]) for a, d in ((0, 1), (1, 3))]
    gp_swap[1].wait_recv()
    ga_ys = [post.send(ga_part(1, 1), ga_yg.at[0, 1], ys[1])]
    gp_swap[2].wait_recv()
    ga_ys.append(post.send(ga_part(2, 0), ga_yg.at[1, 0], ys[3]))
    gp_swap[3].wait_recv()
    gb_relay = [post.send(gb_part(0, k), gb_rel.at[k], xs[d]) for k, d in ((0, 1), (1, 3))]
    gb_xs = [
        post.send(gb_part(1, 1), gb_xg.at[0, 1], xs[1]),
        post.send(gb_part(2, 0), gb_xg.at[1, 0], xs[3]),
    ]
    for k in range(8):
        send_far(k)
        if k < 5:
            send_own(k + 3)
    ga_relay[0].wait_recv()
    ga_ys.append(post.send(ga_part(1, 0, 0), ga_yg.at[0, 0], ys[1]))
    ga_relay[1].wait_recv()
    ga_ys.append(post.send(ga_part(2, 1, 1), ga_yg.at[1, 1], ys[3]))

    ip_ys, ip_relay = [[], []], [[], []]

    def grad_in_piece(k):
        for copy in d_z_copies[k]:
            copy.wait_recv()
        b, to_y = piece(k)
        late, i = k // 4, k % 4
        rows = [d_all[s, b, to_y] for s in range(2)]
        product = jnp.dot(
            jnp.concatenate(rows, axis=0), scaled[...], preferred_element_type=F32
        ).astype(BF)
        for s in range(2):
            for e in range(2):
                start = s * 128 + e * 64
                ip[late, to_y, e, s] = product[start : start + 64]
        swap = post.send(ip.at[late, to_y, 1 - c], ip_c.at[late, to_y], twin)
        swap.wait_recv()
        if i == 3:
            return
        if i:
            ip_relay[late][i - 1].wait_recv()
        for s in range(2):
            value = ip[late, to_y, c, s].astype(F32) + ip_c[late, to_y, s].astype(F32)
            if s == i - 1:
                value = value + ip_rel[late, s].astype(F32)
            ip_y[late, i, s] = value.astype(BF)
        if i:
            ip_ys[late].append(
                post.send(ip_y.at[late, i], ip_yg.at[late, i - 1], ys[order[i]])
            )
        else:
            for s, d in ((0, 1), (1, 3)):
                ip_relay[late].append(post.send(ip_y.at[late, 0, s], ip_rel.at[late, s], ys[d]))

    def in_block(late, s):
        value = ip[late, y, c, s].astype(F32) + ip_c[late, y, s].astype(F32)
        for i in range(2):
            value = value + ip_yg[late, i, s].astype(F32)
        return value

    grad_in_piece(0)
    gb_relay[0].wait_recv()
    gb_xs.append(post.send(gb_part(1, 0, 0), gb_xg.at[0, 0], xs[1]))
    gb_relay[1].wait_recv()
    gb_xs.append(post.send(gb_part(2, 1, 1), gb_xg.at[1, 1], xs[3]))
    grad_in_piece(1)
    grad_in_piece(2)
    for copy in ga_ys:
        copy.wait_recv()
    for a in range(2):
        for e in range(2):
            value = core_sum(a, y, e, zh)
            for i in range(2):
                value = value + ga_yg[i, a, e].astype(F32)
            ga_sum[a, e] = value.astype(BF)
    ga_xs = []
    for i, d in enumerate(order[:3]):
        to_x = lax.rem(x + d, 4)
        ga_xs.append(
            post.send(ga_sum.at[lax.rem(to_x, 2), lax.div(to_x, 2)], ga_xg.at[i], xs[d])
        )
    for copy in gb_xs:
        copy.wait_recv()
    for b in range(4):
        value = core_sum(x_lo, b, x_hi, 1 - zh)
        for i in range(2):
            value = value + gb_xg[i, b // 2, b % 2].astype(F32)
        gb_sum[b] = value.astype(BF)
    gb_ys = []
    for i, d in enumerate(order[:3]):
        gb_ys.append(post.send(gb_sum.at[lax.rem(y + d, 4)], gb_yg.at[i], ys[d]))
    grad_in_piece(3)
    grad_in_piece(4)
    for copy in ip_ys[0]:
        copy.wait_recv()
    for s in range(2):
        ip_x[s] = in_block(0, s).astype(BF)
    ip_beside = post.send(ip_x, ip_xg, beside)
    for copy in gb_ys:
        copy.wait_recv()
    value = gb_sum[y].astype(F32)
    for i in range(3):
        value = value + gb_yg[i].astype(F32)
    gp_z[...] = value.astype(BF)
    gp_across = post.send(gp_z, gp_zg, zs[2])
    grad_in_piece(5)
    grad_in_piece(6)
    for copy in ga_xs:
        copy.wait_recv()
    value = ga_sum[x_lo, x_hi].astype(F32)
    for i in range(3):
        value = value + ga_xg[i].astype(F32)
    gp_across.wait_recv()
    gp_rows[...] = value + gp_zg[...].astype(F32)
    theirs = gp_rows.at[pl.ds(pl.multiple_of((1 - step) * 8, 8), 8), :]
    gp_swap_rows = post.send(theirs, gp_pair, pair)
    grad_in_piece(7)

    ratio_row = ratio_rows[0:1, :]
    for copy in small_copies:
        copy.wait_recv()
    for q in range(4):
        cols = slice(q * 128, (q + 1) * 128)
        r = ratio_rows[0:1, cols]
        total_dr = small_all[2 * q, 0:1, :] + small_all[2 * q + 1, 0:1, :]
        corr_col[cols, :] = column(r * r * r * total_dr * (1.0 / width_in))

    def back(k):
        cols = slice(k * 128, (k + 1) * 128)
        value = sum(
            jnp.dot(w_in[s, cols, :], d_all[s].reshape(depth, -1), preferred_element_type=F32)
            for s in range(2)
        )
        grad_hidden[:, cols] = (
            jnp.transpose(value * ratio_row)
            - corr_col[:, :1] * hidden[:, cols].astype(F32)
        ).astype(BF)

    back(0)
    back(1)
    back(2)
    back(3)
    ip_beside.wait_recv()
    for copy in ip_ys[1]:
        copy.wait_recv()
    for s in range(2):
        grad_in[s] = in_block(1, s) + ip_xg[s].astype(F32)
    gp_swap_rows.wait_recv()
    grad_out[step] = gp_rows[pl.ds(pl.multiple_of(step * 8, 8), 8), :]
    grad_out[1 - step] = gp_pair[...]
    post.close()


def finish(gh, gi, go, grad_hidden, grad_in, grad_out):
    grad_hidden[...] = gh[...]
    grad_in[...] = gi[...]
    grad_out[:, 0, :] = go[0]
    grad_out[:, 1, :] = go[1]


def shards(hidden, w_in, embedding, depth_gain, w_out, codebook_ids):
    hid_count = lax.axis_size("hid")
    seq_count = lax.axis_size("seq")
    width_in = hidden.shape[1] * hid_count
    depth = w_in.shape[2]
    entries = w_out.shape[2]
    frames, units = hidden.shape
    loss_weight = 2.0 * entries / (frames * seq_count)
    vmem = pl.BlockSpec(memory_space=pltpu.VMEM)
    anywhere = pl.BlockSpec(memory_space=pl.ANY)
    scratch = [
        ((frames, units), BF),
        ((2, units, depth), BF),
        ((entries, depth), BF),
        ((4, 2, 128, depth), BF),
        ((2, 128, depth), BF),
        ((2, 128, depth), BF),
        ((2, 2, 128, depth), BF),
        ((128, depth), BF),
        ((128, depth), BF),
        ((2, 8, entries), BF),
        ((4, 8, entries), BF),
        ((2, 4, 2, 2, 2, 16, entries), BF),
        ((8, 128), jnp.int32),
        ((2, 8, 128), jnp.int32),
        ((8, frames), F32),
        ((8, 8, frames), F32),
        ((8, frames), F32),
        ((128, 128), F32),
        ((frames, units), BF),
        ((128, depth), F32),
        ((128, depth), F32),
        ((128, depth), F32),
        ((128, depth), BF),
        ((depth, 128), BF),
        ((128, entries), F32),
        ((128, entries), BF),
        ((128, 128), F32),
        ((128, depth), F32),
        ((128, 128), F32),
        ((2, 4, 128, 128), BF),
        ((2, 2, 4, 128, frames), BF),
        ((8, 128), F32),
        ((8, 8, 128), F32),
        ((frames, 128), F32),
        ((2, 4, 2, 2, 2, 16, entries), BF),
        ((2, 4, 2, 2, 16, entries), BF),
        ((3, 2, 2, 16, entries), BF),
        ((2, 2, 16, entries), BF),
        ((2, 2, 2, 16, entries), BF),
        ((2, 2, 16, entries), BF),
        ((3, 16, entries), BF),
        ((3, 2, 2, 16, entries), BF),
        ((2, 2, 16, entries), BF),
        ((2, 2, 2, 16, entries), BF),
        ((4, 16, entries), BF),
        ((3, 16, entries), BF),
        ((16, entries), BF),
        ((16, entries), BF),
        ((16, entries), F32),
        ((8, entries), F32),
        ((2, 4, 2, 2, 64, units), BF),
        ((2, 4, 2, 64, units), BF),
        ((2, 3, 2, 64, units), BF),
        ((2, 2, 64, units), BF),
        ((2, 2, 2, 64, units), BF),
        ((2, 64, units), BF),
        ((2, 64, units), BF),
    ]
    grad_hidden, grad_in, grad_out = pl.pallas_call(
        functools.partial(kernel, loss_weight, width_in),
        out_shape=[
            jax.ShapeDtypeStruct((frames, units), BF),
            jax.ShapeDtypeStruct((2, 64, units), F32),
            jax.ShapeDtypeStruct((2, 8, entries), F32),
        ],
        in_specs=[anywhere] * 3 + [vmem] * 3,
        out_specs=[vmem] * 3,
        scratch_shapes=[pltpu.VMEM(shape, dtype) for shape, dtype in scratch]
        + [
            pltpu.SemaphoreType.DMA((4,)),
            pltpu.SemaphoreType.DMA((176,)),
            pltpu.SemaphoreType.DMA((176,)),
        ],
        compiler_params=pltpu.CompilerParams(
            collective_id=0, has_side_effects=True, vmem_limit_bytes=62 * 1024 * 1024
        ),
        name="whole",
    )(hidden, w_in, embedding[0], depth_gain, w_out, codebook_ids)
    grad_hidden, grad_in, grad_out = pl.pallas_call(
        finish,
        out_shape=[
            jax.ShapeDtypeStruct((frames, units), BF),
            jax.ShapeDtypeStruct((2, 64, units), F32),
            jax.ShapeDtypeStruct((8, 2, entries), F32),
        ],
        in_specs=[vmem] * 3,
        out_specs=[vmem] * 3,
        name="finish",
    )(grad_hidden, grad_in, grad_out)
    return grad_hidden, jnp.transpose(grad_in, (0, 2, 1)), grad_out


def solution(mesh):
    placed = (
        P("seq", "hid"),
        P(None, "hid", None),
        P(),
        P(),
        P(("seq", "hid"), None, None),
        P(None, ("seq", "hid")),
    )
    return jax.shard_map(
        shards,
        mesh=mesh,
        in_specs=placed,
        out_specs=(P("seq", "hid"), P(None, "hid", "seq"), P(("seq", "hid"), None, None)),
        check_vma=False,
    )
```

```python
import functools

import jax
import jax.numpy as jnp
from jax import lax
from jax.experimental import pallas as pl
from jax.experimental.pallas import tpu as pltpu
from jax.sharding import PartitionSpec as P

MESH = pl.DeviceIdType.MESH
BF = jnp.bfloat16
F32 = jnp.float32
NT = (((1,), (1,)), ((), ()))


def place():
    s, h = lax.axis_index("seq"), lax.axis_index("hid")
    x_lo, y, c = lax.div(s, 8), lax.rem(lax.div(s, 2), 4), lax.rem(s, 2)
    return 2 * lax.div(h, 4) + x_lo, y, lax.rem(h, 4), c


def device(x, y, z, c):
    x, y, z, c = lax.rem(x, 4), lax.rem(y, 4), lax.rem(z, 4), lax.rem(c, 2)
    return (lax.rem(x, 2) * 8 + y * 2 + c, lax.div(x, 2) * 4 + z)


def greet(peers):
    barrier = pltpu.get_barrier_semaphore()
    for peer in peers:
        pl.semaphore_signal(barrier, inc=1, device_id=peer, device_id_type=MESH)
    return lambda: pl.semaphore_wait(barrier, len(peers))


class Post:
    def __init__(self, send_sem, recv_sem):
        self.send_sem, self.recv_sem, self.copies = send_sem, recv_sem, []

    def send(self, src, dst, peer):
        i = len(self.copies)
        copy = pltpu.make_async_remote_copy(
            src_ref=src,
            dst_ref=dst,
            send_sem=self.send_sem.at[i],
            recv_sem=self.recv_sem.at[i],
            device_id=peer,
            device_id_type=MESH,
        )
        copy.start()
        self.copies.append(copy)
        return copy

    def close(self):
        for copy in self.copies:
            copy.wait_send()


def column(row):
    return jnp.transpose(jnp.broadcast_to(row, (128, 128)))


def at128(i):
    return pl.ds(pl.multiple_of(i * 128, 128), 128)


def kernel(loss_weight, width_in, hidden_in, w_in_in, embedding_in, gain_in, w_out, ids, *rest):
    grad_hidden, grad_in, grad_out = rest[:3]
    (
        hidden, w_in, embedding, part, relay, relay_sum, z_got, x_send, x_got,
        w_rows, w_got, w_full, ids_mine, ids_all,
        sq_mine, sq_all, ratio_rows, ratio_col, scaled, looked, x_rows, proj, normed, turned, logits,
        d_logit, scale_col, d_norm, dr_col, d_turn, d_all, small, small_all, corr_col,
        gp, gp_c, ga_y, ga_rel, ga_yg, ga_sum, ga_xg, gb_x, gb_rel, gb_xg, gb_sum, gb_yg,
        gp_z, gp_zg, gp_rows, gp_pair, ip, ip_c, ip_y, ip_rel, ip_yg, ip_x, ip_xg, local_sem, send_sem, recv_sem,
    ) = rest[3:]
    x, y, z, c = place()
    x_lo, x_hi, step, zh = lax.rem(x, 2), lax.div(x, 2), lax.rem(z, 2), lax.div(z, 2)
    hid = x_hi * 4 + z
    quarter = x_hi * 2 + zh
    pair = device(x, y, z + 1 - 2 * step, c)
    far = device(x + 2, y, z, c)
    twin = device(x, y, z, c + 1)
    beside = device(x + 1 - 2 * x_lo, y, z, c)
    xs = {d: device(x + d, y, z, c) for d in (1, 2, 3)}
    ys = {d: device(x, y + d, z, c) for d in (1, 2, 3)}
    zs = {d: device(x, y, z + d, c) for d in (1, 2, 3)}
    hid_peers = [device(x + dx, y, z + dz, c) for dz in (2, 1, 3, 0) for dx in (2, 0) if dx + dz]
    order = (2, 1, 3, 0)

    sources = (
        (hidden_in, hidden),
        (w_in_in.at[step], w_in.at[step]),
        (w_in_in.at[1 - step], w_in.at[1 - step]),
        (embedding_in, embedding),
    )
    loads = [
        pltpu.make_async_copy(src, dst, local_sem.at[i]) for i, (src, dst) in enumerate(sources)
    ]
    for load in loads:
        load.start()
    everyone_here = greet(hid_peers + [xs[1], xs[3]] + list(ys.values()) + [twin])
    w_rows[0] = w_out[:, 0, :]
    w_rows[1] = w_out[:, 1, :]
    ids_mine[...] = jnp.zeros_like(ids_mine)
    ids_mine[0:2, 0:64] = ids[...]
    ids_all[step] = ids_mine[...]
    w_got[z] = w_rows[step]

    def chunk(dz):
        to_z = lax.rem(z + dz, 4)
        rows = [hidden[at128(fx * 2 + lax.div(to_z, 2)), :] for fx in range(2)]
        product = jnp.dot(
            jnp.concatenate(rows, axis=0), w_in[lax.rem(to_z, 2)], preferred_element_type=F32
        ).astype(BF)
        part[dz, 0] = product[:128]
        part[dz, 1] = product[128:]

    loads[0].wait()
    loads[1].wait()
    chunk(2)
    everyone_here()
    post = Post(send_sem, recv_sem)

    bounds = ((0, 64), (64, 96), (96, 128))
    pieces = [pl.ds(a, b - a) for a, b in bounds]
    relays, z_copies = [[] for _ in pieces], [[] for _ in pieces]

    def send_opposite(p):
        rows = pieces[p]
        relays[p].append(post.send(part.at[2, 0, rows], relay.at[0, rows], zs[1]))
        relays[p].append(post.send(part.at[2, 1, rows], relay.at[1, rows], zs[3]))

    def send_direct(p, dz):
        rows, fx, slot = pieces[p], (1 if dz == 1 else 0), (0 if dz == 1 else 1)
        z_copies[p].append(post.send(part.at[dz, fx, rows], z_got.at[slot, fx, rows], zs[dz]))

    def send_sums(p):
        for fx, dz in ((0, 1), (1, 3)):
            rows = pieces[p]
            relays[p][fx].wait_recv()
            relay_sum[fx, rows, :] = (
                part[dz, fx, rows, :].astype(F32) + relay[fx, rows, :].astype(F32)
            ).astype(BF)
            z_copies[p].append(
                post.send(relay_sum.at[fx, rows], z_got.at[fx, fx, rows], zs[dz])
            )

    w_z = [post.send(w_rows.at[(step + d) % 2], w_got.at[z], zs[d]) for d in (2, 1, 3)]
    ids_swap = post.send(ids_mine, ids_all.at[step], pair)
    send_opposite(0)
    h = hidden[...].astype(F32)
    h2 = h * h
    top = h2.astype(BF)
    low = (h2 - top.astype(F32)).astype(BF)
    ones = jnp.ones((8, h2.shape[1]), BF)
    sq_mine[...] = lax.dot_general(ones, top, NT, preferred_element_type=F32) + lax.dot_general(
        ones, low, NT, preferred_element_type=F32
    )
    sq_all[hid] = sq_mine[...]
    loads[2].wait()
    chunk(1)
    send_direct(0, 1)
    sq_copies = [post.send(sq_mine, sq_all.at[hid], peer) for peer in hid_peers]
    chunk(3)
    send_direct(0, 3)
    for p in (1, 2):
        send_opposite(p)
        send_direct(p, 1)
        send_direct(p, 3)
    for copy in w_z:
        copy.wait_recv()
    for e in range(2):
        both = [w_got[2 * e + i].astype(F32) for i in range(2)]
        w_full[x_lo, y, c, x_hi, e] = jnp.concatenate(both, axis=0).astype(BF)
    block = w_full.at[x_lo, y, c, x_hi, zh]
    wa_x = [post.send(block, block, xs[d]) for d in (1, 3, 2)]
    block = w_full.at[x_lo, y, c, x_hi, 1 - zh]
    wb_y = [post.send(block, block, ys[d]) for d in (1, 3, 2)]
    chunk(0)
    send_sums(0)
    for copy in wa_x:
        copy.wait_recv()
    line = w_full.at[:, y, c, :, zh]
    wa_y = {d: post.send(line, line, ys[d]) for d in (2, 1, 3)}
    w_twin = [post.send(line, line, twin)]
    for copy in wb_y:
        copy.wait_recv()
    line = w_full.at[x_lo, :, c, x_hi, 1 - zh]
    wb_x = {d: post.send(line, line, xs[d]) for d in (2, 1, 3)}
    w_twin.append(post.send(line, line, twin))
    send_sums(1)
    send_sums(2)

    for copy in sq_copies:
        copy.wait_recv()
    squares = sq_all[0]
    for i in range(1, 8):
        squares = squares + sq_all[i]
    ratio_rows[...] = lax.rsqrt(squares / width_in + 1e-06)
    for q in range(4):
        wide = column(ratio_rows[0:1, q * 128 : (q + 1) * 128])
        scaled[q * 128 : (q + 1) * 128, :] = (
            hidden[q * 128 : (q + 1) * 128, :].astype(F32) * wide[:, :1]
        ).astype(BF)
    ratio_col[...] = column(ratio_rows[0:1, at128(quarter)])
    ids_swap.wait_recv()

    def tokens(k):
        parts = [column(ids_all[i, k : k + 1, :].astype(F32))[:64, :1] for i in range(2)]
        return jnp.concatenate(parts, axis=0).astype(jnp.int32)

    previous, current = tokens(0), tokens(1)
    target = jnp.where(step == 1, current, previous)
    entries = logits.shape[1]
    lanes = lax.broadcasted_iota(jnp.int32, (128, entries), 1)
    loads[3].wait()
    pick = jnp.where(lanes == previous, 1.0, 0.0).astype(BF)
    live = step.astype(F32)
    for n in range(2):
        cols = slice(n * 512, (n + 1) * 512)
        looked[:, cols] = jnp.dot(pick, embedding[:, cols], preferred_element_type=F32) * live

    def z_sum(fx, rows):
        return (
            part[0, fx, rows, :].astype(F32)
            + z_got[0, fx, rows, :].astype(F32)
            + z_got[1, fx, rows, :].astype(F32)
        )

    x_copies = []
    for p in range(3):
        for copy in z_copies[p]:
            copy.wait_recv()

        @pl.loop(bounds[p][0] // 16, bounds[p][1] // 16, unroll=True)
        def to_far(i):
            rows = pl.ds(pl.multiple_of(i * 16, 16), 16)
            x_send[rows, :] = z_sum(1 - x_hi, rows).astype(BF)

        x_copies.append(post.send(x_send.at[pieces[p]], x_got.at[pieces[p]], far))
    for d in (1, 3, 2):
        wa_y[d].wait_recv()
        line = w_full.at[:, lax.rem(y + 4 - d, 4), c, :, zh]
        w_twin.append(post.send(line, line, twin))
    for d in (1, 3, 2):
        wb_x[d].wait_recv()
        from_x = lax.rem(x + 4 - d, 4)
        line = w_full.at[lax.rem(from_x, 2), :, c, lax.div(from_x, 2), 1 - zh]
        w_twin.append(post.send(line, line, twin))
    gain = gain_in[pl.ds(step, 1), :]
    for p in range(3):
        x_copies[p].wait_recv()

        @pl.loop(bounds[p][0] // 16, bounds[p][1] // 16, unroll=True)
        def norm(i):
            rows = pl.ds(pl.multiple_of(i * 16, 16), 16)
            value = z_sum(x_hi, rows) + x_got[rows, :].astype(F32)
            proj[rows, :] = value
            value = ratio_col[rows, :1] * value + looked[rows, :]
            scale = lax.rsqrt(jnp.mean(value * value, axis=1, keepdims=True) + 1e-06)
            x_rows[rows, :] = value
            scale_col[rows, :] = jnp.broadcast_to(scale, (16, 128))
            normed[rows, :] = (value * scale * gain).astype(BF)

    for copy in w_twin:
        copy.wait_recv()

    depth = normed.shape[1]
    for n in range(4):
        cols = slice(n * 512, (n + 1) * 512)
        head = w_full[:, :, :, :, :, :, cols].reshape(depth, 512)
        logits[:, cols] = jnp.dot(normed[...], head, preferred_element_type=F32)
    dr_col[...] = jnp.broadcast_to(target.astype(F32), (128, 128))

    @pl.loop(0, 8, unroll=4)
    def soft(i):
        rows = pl.ds(pl.multiple_of(i * 16, 16), 16)
        value = logits[rows, :]
        value = jnp.exp(value - jnp.max(value, axis=1, keepdims=True))
        share = value * (loss_weight / jnp.sum(value, axis=1, keepdims=True))
        hot = lax.broadcasted_iota(jnp.int32, (16, entries), 1) == dr_col[rows, :1].astype(
            jnp.int32
        )
        d_logit[rows, :] = (share - jnp.where(hot, loss_weight, 0.0)).astype(BF)

    for k in range(4):
        a, b = k // 2, (k % 2) * 2
        head = w_full[a, b : b + 2].reshape(256, entries)
        d_norm[:, k * 256 : (k + 1) * 256] = lax.dot_general(
            d_logit[...], head, NT, preferred_element_type=F32
        )

    @pl.loop(0, 8, unroll=8)
    def unnorm(i):
        rows = pl.ds(pl.multiple_of(i * 16, 16), 16)
        value, scale = x_rows[rows, :], scale_col[rows, :1]
        gated = gain * d_norm[rows, :]
        inner = jnp.mean(gated * value, axis=1, keepdims=True)
        d_x = scale * gated - value * (scale * scale * scale * inner)
        d_norm[rows, :] = d_x
        total = jnp.sum(d_x * proj[rows, :], axis=1, keepdims=True)
        dr_col[rows, :] = jnp.broadcast_to(total, (16, 128))

    for k in range(8):
        d_turn[k // 4, k % 4] = jnp.transpose(d_norm[:, k * 128 : (k + 1) * 128]).astype(BF)
    lane, far_lane = at128(quarter), at128((1 - x_hi) * 2 + zh)

    def piece(k):
        return (1 - x_lo if k < 4 else x_lo), lax.rem(y + order[k % 4], 4)

    d_x_copies, d_z_copies = [], [[] for _ in range(8)]
    for k in range(8):
        b, to_y = piece(k)
        d_x_copies.append(post.send(d_turn.at[b, to_y], d_all.at[step, b, to_y, :, lane], far))

    def send_own(k):
        b, to_y = piece(k)
        view = d_all.at[step, b, to_y, :, lane]
        d_z_copies[k] += [post.send(d_turn.at[b, to_y], view, zs[d]) for d in (2, 1, 3)]

    def send_far(k):
        b, to_y = piece(k)
        d_x_copies[k].wait_recv()
        view = d_all.at[step, b, to_y, :, far_lane]
        d_z_copies[k] += [post.send(view, view, zs[d]) for d in (2, 1, 3)]

    for k in range(3):
        send_own(k)
    small[...] = jnp.transpose(dr_col[...])[:8]
    small_copies = [post.send(small, small_all.at[hid], peer) for peer in hid_peers]
    for b in range(4):
        for a in range(2):
            d_all[step, a, b, :, lane] = d_turn[a, b]
    small_all[hid] = small[...]

    for k in range(8):
        cols = slice(k * 128, (k + 1) * 128)
        turned[cols, :] = jnp.transpose(normed[:, cols].astype(F32)).astype(BF)
    gp_swap = []

    def product_out(i):
        to_y = lax.rem(y + order[i], 4)
        for a in range(2):
            rows = at128(a * 4 + to_y)
            gp[a, to_y] = (
                jnp.dot(turned[rows, :], d_logit[...], preferred_element_type=F32)
                .astype(BF)
                .reshape(2, 2, 2, 16, entries)
            )
        gp_swap.append(post.send(gp.at[:, to_y, 1 - c], gp_c.at[:, to_y], twin))

    for i in range(4):
        product_out(i)
    def core_sum(a, b, e, f):
        return gp[a, b, c, e, f].astype(F32) + gp_c[a, b, e, f].astype(F32)

    def ga_part(i, a, more=None):
        to_y = lax.rem(y + order[i], 4)
        for e in range(2):
            value = core_sum(a, to_y, e, zh)
            if more is not None:
                value = value + ga_rel[more, e].astype(F32)
            ga_y[i, a, e] = value.astype(BF)
        return ga_y.at[i, a]

    def gb_part(i, k, more=None):
        to_x = lax.rem(x + order[i], 4)
        for b in range(2):
            value = core_sum(lax.rem(to_x, 2), 2 * k + b, lax.div(to_x, 2), 1 - zh)
            if more is not None:
                value = value + gb_rel[more, b].astype(F32)
            gb_x[i, k, b] = value.astype(BF)
        return gb_x.at[i, k]

    gp_swap[0].wait_recv()
    ga_relay = [post.send(ga_part(0, a), ga_rel.at[a], ys[d]) for a, d in ((0, 1), (1, 3))]
    gp_swap[1].wait_recv()
    ga_ys = [post.send(ga_part(1, 1), ga_yg.at[0, 1], ys[1])]
    gp_swap[2].wait_recv()
    ga_ys.append(post.send(ga_part(2, 0), ga_yg.at[1, 0], ys[3]))
    gp_swap[3].wait_recv()
    gb_relay = [post.send(gb_part(0, k), gb_rel.at[k], xs[d]) for k, d in ((0, 1), (1, 3))]
    gb_xs = [
        post.send(gb_part(1, 1), gb_xg.at[0, 1], xs[1]),
        post.send(gb_part(2, 0), gb_xg.at[1, 0], xs[3]),
    ]
    for k in range(8):
        send_far(k)
        if k < 5:
            send_own(k + 3)
    ga_relay[0].wait_recv()
    ga_ys.append(post.send(ga_part(1, 0, 0), ga_yg.at[0, 0], ys[1]))
    ga_relay[1].wait_recv()
    ga_ys.append(post.send(ga_part(2, 1, 1), ga_yg.at[1, 1], ys[3]))

    ip_ys, ip_relay = [[], []], [[], []]

    swaps = {}

    def grad_in_product(k):
        for copy in d_z_copies[k]:
            copy.wait_recv()
        b, to_y = piece(k)
        late = k // 4
        rows = [d_all[s, b, to_y] for s in range(2)]
        product = jnp.dot(
            jnp.concatenate(rows, axis=0), scaled[...], preferred_element_type=F32
        ).astype(BF)
        for s in range(2):
            for e in range(2):
                start = s * 128 + e * 64
                ip[late, to_y, e, s] = product[start : start + 64]
        swaps[k] = post.send(ip.at[late, to_y, 1 - c], ip_c.at[late, to_y], twin)

    def grad_in_sum(k):
        b, to_y = piece(k)
        late, i = k // 4, k % 4
        swaps[k].wait_recv()
        if i == 3:
            return
        if i:
            ip_relay[late][i - 1].wait_recv()
        for s in range(2):
            value = ip[late, to_y, c, s].astype(F32) + ip_c[late, to_y, s].astype(F32)
            if s == i - 1:
                value = value + ip_rel[late, s].astype(F32)
            ip_y[late, i, s] = value.astype(BF)
        if i:
            ip_ys[late].append(
                post.send(ip_y.at[late, i], ip_yg.at[late, i - 1], ys[order[i]])
            )
        else:
            for s, d in ((0, 1), (1, 3)):
                ip_relay[late].append(post.send(ip_y.at[late, 0, s], ip_rel.at[late, s], ys[d]))

    def grad_in_piece(k):
        grad_in_product(k)
        grad_in_sum(k)

    def in_block(late, s):
        value = ip[late, y, c, s].astype(F32) + ip_c[late, y, s].astype(F32)
        for i in range(2):
            value = value + ip_yg[late, i, s].astype(F32)
        return value

    grad_in_piece(0)
    gb_relay[0].wait_recv()
    gb_xs.append(post.send(gb_part(1, 0, 0), gb_xg.at[0, 0], xs[1]))
    gb_relay[1].wait_recv()
    gb_xs.append(post.send(gb_part(2, 1, 1), gb_xg.at[1, 1], xs[3]))
    grad_in_piece(1)
    grad_in_piece(2)
    for copy in ga_ys:
        copy.wait_recv()
    for a in range(2):
        for e in range(2):
            value = core_sum(a, y, e, zh)
            for i in range(2):
                value = value + ga_yg[i, a, e].astype(F32)
            ga_sum[a, e] = value.astype(BF)
    ga_xs = []
    for i, d in enumerate(order[:3]):
        to_x = lax.rem(x + d, 4)
        ga_xs.append(
            post.send(ga_sum.at[lax.rem(to_x, 2), lax.div(to_x, 2)], ga_xg.at[i], xs[d])
        )
    for copy in gb_xs:
        copy.wait_recv()
    for b in range(4):
        value = core_sum(x_lo, b, x_hi, 1 - zh)
        for i in range(2):
            value = value + gb_xg[i, b // 2, b % 2].astype(F32)
        gb_sum[b] = value.astype(BF)
    gb_ys = []
    for i, d in enumerate(order[:3]):
        gb_ys.append(post.send(gb_sum.at[lax.rem(y + d, 4)], gb_yg.at[i], ys[d]))
    grad_in_piece(3)
    grad_in_piece(4)
    for copy in ip_ys[0]:
        copy.wait_recv()
    for s in range(2):
        ip_x[s] = in_block(0, s).astype(BF)
    ip_beside = post.send(ip_x, ip_xg, beside)
    for copy in gb_ys:
        copy.wait_recv()
    value = gb_sum[y].astype(F32)
    for i in range(3):
        value = value + gb_yg[i].astype(F32)
    gp_z[...] = value.astype(BF)
    gp_across = post.send(gp_z, gp_zg, zs[2])
    grad_in_product(5)
    grad_in_product(6)
    grad_in_sum(5)
    for copy in ga_xs:
        copy.wait_recv()
    value = ga_sum[x_lo, x_hi].astype(F32)
    for i in range(3):
        value = value + ga_xg[i].astype(F32)
    gp_across.wait_recv()
    gp_rows[...] = value + gp_zg[...].astype(F32)
    theirs = gp_rows.at[pl.ds(pl.multiple_of((1 - step) * 8, 8), 8), :]
    gp_swap_rows = post.send(theirs, gp_pair, pair)
    grad_in_product(7)
    grad_in_sum(6)

    ratio_row = ratio_rows[0:1, :]
    for copy in small_copies:
        copy.wait_recv()
    for q in range(4):
        cols = slice(q * 128, (q + 1) * 128)
        r = ratio_rows[0:1, cols]
        total_dr = small_all[2 * q, 0:1, :] + small_all[2 * q + 1, 0:1, :]
        corr_col[cols, :] = column(r * r * r * total_dr * (1.0 / width_in))

    def back(k):
        cols = slice(k * 128, (k + 1) * 128)
        value = sum(
            jnp.dot(w_in[s, cols, :], d_all[s].reshape(depth, -1), preferred_element_type=F32)
            for s in range(2)
        )
        grad_hidden[:, cols] = (
            jnp.transpose(value * ratio_row)
            - corr_col[:, :1] * hidden[:, cols].astype(F32)
        ).astype(BF)

    back(0)
    back(1)
    back(2)
    back(3)
    ip_beside.wait_recv()
    grad_in_sum(7)
    for copy in ip_ys[1]:
        copy.wait_recv()
    for s in range(2):
        grad_in[s] = in_block(1, s) + ip_xg[s].astype(F32)
    gp_swap_rows.wait_recv()
    grad_out[step] = gp_rows[pl.ds(pl.multiple_of(step * 8, 8), 8), :]
    grad_out[1 - step] = gp_pair[...]
    post.close()


def finish(gh, gi, go, grad_hidden, grad_in, grad_out):
    grad_hidden[...] = gh[...]
    grad_in[...] = gi[...]
    grad_out[:, 0, :] = go[0]
    grad_out[:, 1, :] = go[1]


def shards(hidden, w_in, embedding, depth_gain, w_out, codebook_ids):
    hid_count = lax.axis_size("hid")
    seq_count = lax.axis_size("seq")
    width_in = hidden.shape[1] * hid_count
    depth = w_in.shape[2]
    entries = w_out.shape[2]
    frames, units = hidden.shape
    loss_weight = 2.0 * entries / (frames * seq_count)
    vmem = pl.BlockSpec(memory_space=pltpu.VMEM)
    anywhere = pl.BlockSpec(memory_space=pl.ANY)
    scratch = [
        ((frames, units), BF),
        ((2, units, depth), BF),
        ((entries, depth), BF),
        ((4, 2, 128, depth), BF),
        ((2, 128, depth), BF),
        ((2, 128, depth), BF),
        ((2, 2, 128, depth), BF),
        ((128, depth), BF),
        ((128, depth), BF),
        ((2, 8, entries), BF),
        ((4, 8, entries), BF),
        ((2, 4, 2, 2, 2, 16, entries), BF),
        ((8, 128), jnp.int32),
        ((2, 8, 128), jnp.int32),
        ((8, frames), F32),
        ((8, 8, frames), F32),
        ((8, frames), F32),
        ((128, 128), F32),
        ((frames, units), BF),
        ((128, depth), F32),
        ((128, depth), F32),
        ((128, depth), F32),
        ((128, depth), BF),
        ((depth, 128), BF),
        ((128, entries), F32),
        ((128, entries), BF),
        ((128, 128), F32),
        ((128, depth), F32),
        ((128, 128), F32),
        ((2, 4, 128, 128), BF),
        ((2, 2, 4, 128, frames), BF),
        ((8, 128), F32),
        ((8, 8, 128), F32),
        ((frames, 128), F32),
        ((2, 4, 2, 2, 2, 16, entries), BF),
        ((2, 4, 2, 2, 16, entries), BF),
        ((3, 2, 2, 16, entries), BF),
        ((2, 2, 16, entries), BF),
        ((2, 2, 2, 16, entries), BF),
        ((2, 2, 16, entries), BF),
        ((3, 16, entries), BF),
        ((3, 2, 2, 16, entries), BF),
        ((2, 2, 16, entries), BF),
        ((2, 2, 2, 16, entries), BF),
        ((4, 16, entries), BF),
        ((3, 16, entries), BF),
        ((16, entries), BF),
        ((16, entries), BF),
        ((16, entries), F32),
        ((8, entries), F32),
        ((2, 4, 2, 2, 64, units), BF),
        ((2, 4, 2, 64, units), BF),
        ((2, 3, 2, 64, units), BF),
        ((2, 2, 64, units), BF),
        ((2, 2, 2, 64, units), BF),
        ((2, 64, units), BF),
        ((2, 64, units), BF),
    ]
    grad_hidden, grad_in, grad_out = pl.pallas_call(
        functools.partial(kernel, loss_weight, width_in),
        out_shape=[
            jax.ShapeDtypeStruct((frames, units), BF),
            jax.ShapeDtypeStruct((2, 64, units), F32),
            jax.ShapeDtypeStruct((2, 8, entries), F32),
        ],
        in_specs=[anywhere] * 3 + [vmem] * 3,
        out_specs=[vmem] * 3,
        scratch_shapes=[pltpu.VMEM(shape, dtype) for shape, dtype in scratch]
        + [
            pltpu.SemaphoreType.DMA((4,)),
            pltpu.SemaphoreType.DMA((176,)),
            pltpu.SemaphoreType.DMA((176,)),
        ],
        compiler_params=pltpu.CompilerParams(
            collective_id=0, has_side_effects=True, vmem_limit_bytes=62 * 1024 * 1024
        ),
        name="whole",
    )(hidden, w_in, embedding[0], depth_gain, w_out, codebook_ids)
    grad_hidden, grad_in, grad_out = pl.pallas_call(
        finish,
        out_shape=[
            jax.ShapeDtypeStruct((frames, units), BF),
            jax.ShapeDtypeStruct((2, 64, units), F32),
            jax.ShapeDtypeStruct((8, 2, entries), F32),
        ],
        in_specs=[vmem] * 3,
        out_specs=[vmem] * 3,
        name="finish",
    )(grad_hidden, grad_in, grad_out)
    return grad_hidden, jnp.transpose(grad_in, (0, 2, 1)), grad_out


def solution(mesh):
    placed = (
        P("seq", "hid"),
        P(None, "hid", None),
        P(),
        P(),
        P(("seq", "hid"), None, None),
        P(None, ("seq", "hid")),
    )
    return jax.shard_map(
        shards,
        mesh=mesh,
        in_specs=placed,
        out_specs=(P("seq", "hid"), P(None, "hid", "seq"), P(("seq", "hid"), None, None)),
        check_vma=False,
    )
```

```python
import functools

import jax
import jax.numpy as jnp
from jax import lax
from jax.experimental import pallas as pl
from jax.experimental.pallas import tpu as pltpu
from jax.sharding import PartitionSpec as P

MESH = pl.DeviceIdType.MESH
BF = jnp.bfloat16
F32 = jnp.float32
NT = (((1,), (1,)), ((), ()))


def place():
    s, h = lax.axis_index("seq"), lax.axis_index("hid")
    x_lo, y, c = lax.div(s, 8), lax.rem(lax.div(s, 2), 4), lax.rem(s, 2)
    return 2 * lax.div(h, 4) + x_lo, y, lax.rem(h, 4), c


def device(x, y, z, c):
    x, y, z, c = lax.rem(x, 4), lax.rem(y, 4), lax.rem(z, 4), lax.rem(c, 2)
    return (lax.rem(x, 2) * 8 + y * 2 + c, lax.div(x, 2) * 4 + z)


def greet(peers):
    barrier = pltpu.get_barrier_semaphore()
    for peer in peers:
        pl.semaphore_signal(barrier, inc=1, device_id=peer, device_id_type=MESH)
    return lambda: pl.semaphore_wait(barrier, len(peers))


class Post:
    def __init__(self, send_sem, recv_sem):
        self.send_sem, self.recv_sem, self.copies = send_sem, recv_sem, []

    def send(self, src, dst, peer):
        i = len(self.copies)
        copy = pltpu.make_async_remote_copy(
            src_ref=src,
            dst_ref=dst,
            send_sem=self.send_sem.at[i],
            recv_sem=self.recv_sem.at[i],
            device_id=peer,
            device_id_type=MESH,
        )
        copy.start()
        self.copies.append(copy)
        return copy

    def close(self):
        for copy in self.copies:
            copy.wait_send()


def column(row):
    return jnp.transpose(jnp.broadcast_to(row, (128, 128)))


def at128(i):
    return pl.ds(pl.multiple_of(i * 128, 128), 128)


def kernel(loss_weight, width_in, hidden_in, w_in_in, embedding_in, gain_in, w_out, ids, *rest):
    grad_hidden, grad_in, grad_out = rest[:3]
    (
        hidden, w_in, embedding, part, relay, relay_sum, z_got, x_send, x_got,
        w_rows, w_got, w_full, ids_mine, ids_all,
        sq_mine, sq_all, ratio_rows, ratio_col, scaled, looked, x_rows, proj, normed, turned, logits,
        d_logit, scale_col, d_norm, dr_col, d_turn, d_all, small, small_all, corr_col,
        gp, gp_c, ga_y, ga_rel, ga_yg, ga_sum, ga_xg, gb_x, gb_rel, gb_xg, gb_sum, gb_yg,
        gp_z, gp_zg, gp_rows, gp_pair, ip, ip_c, ip_y, ip_rel, ip_yg, ip_x, ip_xg, local_sem, send_sem, recv_sem,
    ) = rest[3:]
    x, y, z, c = place()
    x_lo, x_hi, step, zh = lax.rem(x, 2), lax.div(x, 2), lax.rem(z, 2), lax.div(z, 2)
    hid = x_hi * 4 + z
    quarter = x_hi * 2 + zh
    pair = device(x, y, z + 1 - 2 * step, c)
    far = device(x + 2, y, z, c)
    twin = device(x, y, z, c + 1)
    beside = device(x + 1 - 2 * x_lo, y, z, c)
    xs = {d: device(x + d, y, z, c) for d in (1, 2, 3)}
    ys = {d: device(x, y + d, z, c) for d in (1, 2, 3)}
    zs = {d: device(x, y, z + d, c) for d in (1, 2, 3)}
    hid_peers = [device(x + dx, y, z + dz, c) for dz in (2, 1, 3, 0) for dx in (2, 0) if dx + dz]
    order = (2, 1, 3, 0)

    sources = (
        (hidden_in, hidden),
        (w_in_in.at[step], w_in.at[step]),
        (w_in_in.at[1 - step], w_in.at[1 - step]),
        (embedding_in, embedding),
    )
    loads = [
        pltpu.make_async_copy(src, dst, local_sem.at[i]) for i, (src, dst) in enumerate(sources)
    ]
    for load in loads:
        load.start()
    everyone_here = greet(hid_peers + [xs[1], xs[3]] + list(ys.values()) + [twin])
    w_rows[0] = w_out[:, 0, :]
    w_rows[1] = w_out[:, 1, :]
    ids_mine[...] = jnp.zeros_like(ids_mine)
    ids_mine[0:2, 0:64] = ids[...]
    ids_all[step] = ids_mine[...]
    w_got[z] = w_rows[step]

    def chunk(dz):
        to_z = lax.rem(z + dz, 4)
        rows = [hidden[at128(fx * 2 + lax.div(to_z, 2)), :] for fx in range(2)]
        product = jnp.dot(
            jnp.concatenate(rows, axis=0), w_in[lax.rem(to_z, 2)], preferred_element_type=F32
        ).astype(BF)
        part[dz, 0] = product[:128]
        part[dz, 1] = product[128:]

    loads[0].wait()
    loads[1].wait()
    chunk(2)
    everyone_here()
    post = Post(send_sem, recv_sem)

    bounds = ((0, 64), (64, 96), (96, 128))
    pieces = [pl.ds(a, b - a) for a, b in bounds]
    relays, z_copies = [[] for _ in pieces], [[] for _ in pieces]

    def send_opposite(p):
        rows = pieces[p]
        relays[p].append(post.send(part.at[2, 0, rows], relay.at[0, rows], zs[1]))
        relays[p].append(post.send(part.at[2, 1, rows], relay.at[1, rows], zs[3]))

    def send_direct(p, dz):
        rows, fx, slot = pieces[p], (1 if dz == 1 else 0), (0 if dz == 1 else 1)
        z_copies[p].append(post.send(part.at[dz, fx, rows], z_got.at[slot, fx, rows], zs[dz]))

    def send_sums(p):
        for fx, dz in ((0, 1), (1, 3)):
            rows = pieces[p]
            relays[p][fx].wait_recv()
            relay_sum[fx, rows, :] = (
                part[dz, fx, rows, :].astype(F32) + relay[fx, rows, :].astype(F32)
            ).astype(BF)
            z_copies[p].append(
                post.send(relay_sum.at[fx, rows], z_got.at[fx, fx, rows], zs[dz])
            )

    w_z = [post.send(w_rows.at[(step + d) % 2], w_got.at[z], zs[d]) for d in (2, 1, 3)]
    ids_swap = post.send(ids_mine, ids_all.at[step], pair)
    send_opposite(0)
    h = hidden[...].astype(F32)
    h2 = h * h
    top = h2.astype(BF)
    low = (h2 - top.astype(F32)).astype(BF)
    ones = jnp.ones((8, h2.shape[1]), BF)
    sq_mine[...] = lax.dot_general(ones, top, NT, preferred_element_type=F32) + lax.dot_general(
        ones, low, NT, preferred_element_type=F32
    )
    sq_all[hid] = sq_mine[...]
    loads[2].wait()
    chunk(1)
    send_direct(0, 1)
    sq_copies = [post.send(sq_mine, sq_all.at[hid], peer) for peer in hid_peers]
    chunk(3)
    send_direct(0, 3)
    for p in (1, 2):
        send_opposite(p)
        send_direct(p, 1)
        send_direct(p, 3)
    for copy in w_z:
        copy.wait_recv()
    for e in range(2):
        both = [w_got[2 * e + i].astype(F32) for i in range(2)]
        w_full[x_lo, y, c, x_hi, e] = jnp.concatenate(both, axis=0).astype(BF)
    block = w_full.at[x_lo, y, c, x_hi, zh]
    wa_x = [post.send(block, block, xs[d]) for d in (1, 3, 2)]
    block = w_full.at[x_lo, y, c, x_hi, 1 - zh]
    wb_y = [post.send(block, block, ys[d]) for d in (1, 3, 2)]
    chunk(0)
    send_sums(0)
    for copy in wa_x:
        copy.wait_recv()
    line = w_full.at[:, y, c, :, zh]
    wa_y = {d: post.send(line, line, ys[d]) for d in (2, 1, 3)}
    w_twin = [post.send(line, line, twin)]
    for copy in wb_y:
        copy.wait_recv()
    line = w_full.at[x_lo, :, c, x_hi, 1 - zh]
    wb_x = {d: post.send(line, line, xs[d]) for d in (2, 1, 3)}
    w_twin.append(post.send(line, line, twin))
    send_sums(1)
    send_sums(2)

    for copy in sq_copies:
        copy.wait_recv()
    squares = sq_all[0]
    for i in range(1, 8):
        squares = squares + sq_all[i]
    ratio_rows[...] = lax.rsqrt(squares / width_in + 1e-06)
    for q in range(4):
        wide = column(ratio_rows[0:1, q * 128 : (q + 1) * 128])
        scaled[q * 128 : (q + 1) * 128, :] = (
            hidden[q * 128 : (q + 1) * 128, :].astype(F32) * wide[:, :1]
        ).astype(BF)
    ratio_col[...] = column(ratio_rows[0:1, at128(quarter)])
    ids_swap.wait_recv()

    def tokens(k):
        parts = [column(ids_all[i, k : k + 1, :].astype(F32))[:64, :1] for i in range(2)]
        return jnp.concatenate(parts, axis=0).astype(jnp.int32)

    previous, current = tokens(0), tokens(1)
    target = jnp.where(step == 1, current, previous)
    entries = logits.shape[1]
    lanes = lax.broadcasted_iota(jnp.int32, (128, entries), 1)
    loads[3].wait()
    pick = jnp.where(lanes == previous, 1.0, 0.0).astype(BF)
    live = step.astype(F32)
    for n in range(2):
        cols = slice(n * 512, (n + 1) * 512)
        looked[:, cols] = jnp.dot(pick, embedding[:, cols], preferred_element_type=F32) * live

    def z_sum(fx, rows):
        return (
            part[0, fx, rows, :].astype(F32)
            + z_got[0, fx, rows, :].astype(F32)
            + z_got[1, fx, rows, :].astype(F32)
        )

    x_copies = []
    for p in range(3):
        for copy in z_copies[p]:
            copy.wait_recv()

        @pl.loop(bounds[p][0] // 16, bounds[p][1] // 16, unroll=True)
        def to_far(i):
            rows = pl.ds(pl.multiple_of(i * 16, 16), 16)
            x_send[rows, :] = z_sum(1 - x_hi, rows).astype(BF)

        x_copies.append(post.send(x_send.at[pieces[p]], x_got.at[pieces[p]], far))
    for d in (1, 3, 2):
        wa_y[d].wait_recv()
        line = w_full.at[:, lax.rem(y + 4 - d, 4), c, :, zh]
        w_twin.append(post.send(line, line, twin))
    for d in (1, 3, 2):
        wb_x[d].wait_recv()
        from_x = lax.rem(x + 4 - d, 4)
        line = w_full.at[lax.rem(from_x, 2), :, c, lax.div(from_x, 2), 1 - zh]
        w_twin.append(post.send(line, line, twin))
    gain = gain_in[pl.ds(step, 1), :]
    for p in range(3):
        x_copies[p].wait_recv()

        @pl.loop(bounds[p][0] // 16, bounds[p][1] // 16, unroll=True)
        def norm(i):
            rows = pl.ds(pl.multiple_of(i * 16, 16), 16)
            value = z_sum(x_hi, rows) + x_got[rows, :].astype(F32)
            proj[rows, :] = value
            value = ratio_col[rows, :1] * value + looked[rows, :]
            scale = lax.rsqrt(jnp.mean(value * value, axis=1, keepdims=True) + 1e-06)
            x_rows[rows, :] = value
            scale_col[rows, :] = jnp.broadcast_to(scale, (16, 128))
            normed[rows, :] = (value * scale * gain).astype(BF)

    for copy in w_twin:
        copy.wait_recv()

    depth = normed.shape[1]
    for n in range(4):
        cols = slice(n * 512, (n + 1) * 512)
        head = w_full[:, :, :, :, :, :, cols].reshape(depth, 512)
        logits[:, cols] = jnp.dot(normed[...], head, preferred_element_type=F32)
    dr_col[...] = jnp.broadcast_to(target.astype(F32), (128, 128))

    @pl.loop(0, 8, unroll=4)
    def soft(i):
        rows = pl.ds(pl.multiple_of(i * 16, 16), 16)
        value = logits[rows, :]
        value = jnp.exp(value - jnp.max(value, axis=1, keepdims=True))
        share = value * (loss_weight / jnp.sum(value, axis=1, keepdims=True))
        hot = lax.broadcasted_iota(jnp.int32, (16, entries), 1) == dr_col[rows, :1].astype(
            jnp.int32
        )
        d_logit[rows, :] = (share - jnp.where(hot, loss_weight, 0.0)).astype(BF)

    for k in range(4):
        a, b = k // 2, (k % 2) * 2
        head = w_full[a, b : b + 2].reshape(256, entries)
        d_norm[:, k * 256 : (k + 1) * 256] = lax.dot_general(
            d_logit[...], head, NT, preferred_element_type=F32
        )

    @pl.loop(0, 8, unroll=8)
    def unnorm(i):
        rows = pl.ds(pl.multiple_of(i * 16, 16), 16)
        value, scale = x_rows[rows, :], scale_col[rows, :1]
        gated = gain * d_norm[rows, :]
        inner = jnp.mean(gated * value, axis=1, keepdims=True)
        d_x = scale * gated - value * (scale * scale * scale * inner)
        d_norm[rows, :] = d_x
        total = jnp.sum(d_x * proj[rows, :], axis=1, keepdims=True)
        dr_col[rows, :] = jnp.broadcast_to(total, (16, 128))

    for k in range(8):
        d_turn[k // 4, k % 4] = jnp.transpose(d_norm[:, k * 128 : (k + 1) * 128]).astype(BF)
    lane, far_lane = at128(quarter), at128((1 - x_hi) * 2 + zh)

    def piece(k):
        return (1 - x_lo if k < 4 else x_lo), lax.rem(y + order[k % 4], 4)

    d_x_copies, d_z_copies = {}, [[] for _ in range(8)]
    for k in (0, 1, 2, 4, 5, 6, 7):
        b, to_y = piece(k)
        d_x_copies[k] = post.send(d_turn.at[b, to_y], d_all.at[step, b, to_y, :, lane], far)

    def send_across():
        b, to_y = piece(3)
        for copy in d_z_copies[3]:
            copy.wait_recv()
        d_z_copies[3] = [
            post.send(d_turn.at[b, to_y], d_all.at[step, b, to_y, :, lane], far)
        ]
        for dz in (1, 2, 3):
            to_z = lax.rem(z + dz, 4)
            view = d_all.at[
                lax.rem(to_z, 2), b, to_y, :, at128(x_hi * 2 + lax.div(to_z, 2))
            ]
            d_z_copies[3].append(post.send(view, view, far))

    def send_own(k):
        b, to_y = piece(k)
        view = d_all.at[step, b, to_y, :, lane]
        d_z_copies[k] += [post.send(d_turn.at[b, to_y], view, zs[d]) for d in (2, 1, 3)]

    def send_far(k):
        b, to_y = piece(k)
        d_x_copies[k].wait_recv()
        view = d_all.at[step, b, to_y, :, far_lane]
        d_z_copies[k] += [post.send(view, view, zs[d]) for d in (2, 1, 3)]

    for k in range(3):
        send_own(k)
    small[...] = jnp.transpose(dr_col[...])[:8]
    small_copies = [post.send(small, small_all.at[hid], peer) for peer in hid_peers]
    for b in range(4):
        for a in range(2):
            d_all[step, a, b, :, lane] = d_turn[a, b]
    small_all[hid] = small[...]

    for k in range(8):
        cols = slice(k * 128, (k + 1) * 128)
        turned[cols, :] = jnp.transpose(normed[:, cols].astype(F32)).astype(BF)
    gp_swap = []

    def product_out(i):
        to_y = lax.rem(y + order[i], 4)
        for a in range(2):
            rows = at128(a * 4 + to_y)
            gp[a, to_y] = (
                jnp.dot(turned[rows, :], d_logit[...], preferred_element_type=F32)
                .astype(BF)
                .reshape(2, 2, 2, 16, entries)
            )
        gp_swap.append(post.send(gp.at[:, to_y, 1 - c], gp_c.at[:, to_y], twin))

    for i in range(4):
        product_out(i)
    def core_sum(a, b, e, f):
        return gp[a, b, c, e, f].astype(F32) + gp_c[a, b, e, f].astype(F32)

    def ga_part(i, a, more=None):
        to_y = lax.rem(y + order[i], 4)
        for e in range(2):
            value = core_sum(a, to_y, e, zh)
            if more is not None:
                value = value + ga_rel[more, e].astype(F32)
            ga_y[i, a, e] = value.astype(BF)
        return ga_y.at[i, a]

    def gb_part(i, k, more=None):
        to_x = lax.rem(x + order[i], 4)
        for b in range(2):
            value = core_sum(lax.rem(to_x, 2), 2 * k + b, lax.div(to_x, 2), 1 - zh)
            if more is not None:
                value = value + gb_rel[more, b].astype(F32)
            gb_x[i, k, b] = value.astype(BF)
        return gb_x.at[i, k]

    gp_swap[0].wait_recv()
    ga_relay = [post.send(ga_part(0, a), ga_rel.at[a], ys[d]) for a, d in ((0, 1), (1, 3))]
    gp_swap[1].wait_recv()
    ga_ys = [post.send(ga_part(1, 1), ga_yg.at[0, 1], ys[1])]
    gp_swap[2].wait_recv()
    ga_ys.append(post.send(ga_part(2, 0), ga_yg.at[1, 0], ys[3]))
    gp_swap[3].wait_recv()
    gb_relay = [post.send(gb_part(0, k), gb_rel.at[k], xs[d]) for k, d in ((0, 1), (1, 3))]
    gb_xs = [
        post.send(gb_part(1, 1), gb_xg.at[0, 1], xs[1]),
        post.send(gb_part(2, 0), gb_xg.at[1, 0], xs[3]),
    ]
    for k in range(8):
        if k != 3:
            send_far(k)
        if k < 5:
            send_own(k + 3)
    ga_relay[0].wait_recv()
    ga_ys.append(post.send(ga_part(1, 0, 0), ga_yg.at[0, 0], ys[1]))
    ga_relay[1].wait_recv()
    ga_ys.append(post.send(ga_part(2, 1, 1), ga_yg.at[1, 1], ys[3]))

    ip_ys, ip_relay = [[], []], [[], []]

    def grad_in_piece(k):
        for copy in d_z_copies[k]:
            copy.wait_recv()
        b, to_y = piece(k)
        late, i = k // 4, k % 4
        rows = [d_all[s, b, to_y] for s in range(2)]
        product = jnp.dot(
            jnp.concatenate(rows, axis=0), scaled[...], preferred_element_type=F32
        ).astype(BF)
        for s in range(2):
            for e in range(2):
                start = s * 128 + e * 64
                ip[late, to_y, e, s] = product[start : start + 64]
        swap = post.send(ip.at[late, to_y, 1 - c], ip_c.at[late, to_y], twin)
        swap.wait_recv()
        if i == 3:
            return
        if i:
            ip_relay[late][i - 1].wait_recv()
        for s in range(2):
            value = ip[late, to_y, c, s].astype(F32) + ip_c[late, to_y, s].astype(F32)
            if s == i - 1:
                value = value + ip_rel[late, s].astype(F32)
            ip_y[late, i, s] = value.astype(BF)
        if i:
            ip_ys[late].append(
                post.send(ip_y.at[late, i], ip_yg.at[late, i - 1], ys[order[i]])
            )
        else:
            for s, d in ((0, 1), (1, 3)):
                ip_relay[late].append(post.send(ip_y.at[late, 0, s], ip_rel.at[late, s], ys[d]))

    def in_block(late, s):
        value = ip[late, y, c, s].astype(F32) + ip_c[late, y, s].astype(F32)
        for i in range(2):
            value = value + ip_yg[late, i, s].astype(F32)
        return value

    grad_in_piece(0)
    gb_relay[0].wait_recv()
    gb_xs.append(post.send(gb_part(1, 0, 0), gb_xg.at[0, 0], xs[1]))
    gb_relay[1].wait_recv()
    gb_xs.append(post.send(gb_part(2, 1, 1), gb_xg.at[1, 1], xs[3]))
    send_across()
    grad_in_piece(1)
    grad_in_piece(2)
    for copy in ga_ys:
        copy.wait_recv()
    for a in range(2):
        for e in range(2):
            value = core_sum(a, y, e, zh)
            for i in range(2):
                value = value + ga_yg[i, a, e].astype(F32)
            ga_sum[a, e] = value.astype(BF)
    ga_xs = []
    for i, d in enumerate(order[:3]):
        to_x = lax.rem(x + d, 4)
        ga_xs.append(
            post.send(ga_sum.at[lax.rem(to_x, 2), lax.div(to_x, 2)], ga_xg.at[i], xs[d])
        )
    for copy in gb_xs:
        copy.wait_recv()
    for b in range(4):
        value = core_sum(x_lo, b, x_hi, 1 - zh)
        for i in range(2):
            value = value + gb_xg[i, b // 2, b % 2].astype(F32)
        gb_sum[b] = value.astype(BF)
    gb_ys = []
    for i, d in enumerate(order[:3]):
        gb_ys.append(post.send(gb_sum.at[lax.rem(y + d, 4)], gb_yg.at[i], ys[d]))
    grad_in_piece(3)
    grad_in_piece(4)
    for copy in ip_ys[0]:
        copy.wait_recv()
    for s in range(2):
        ip_x[s] = in_block(0, s).astype(BF)
    ip_beside = post.send(ip_x, ip_xg, beside)
    for copy in gb_ys:
        copy.wait_recv()
    value = gb_sum[y].astype(F32)
    for i in range(3):
        value = value + gb_yg[i].astype(F32)
    gp_z[...] = value.astype(BF)
    gp_across = post.send(gp_z, gp_zg, zs[2])
    grad_in_piece(5)
    grad_in_piece(6)
    for copy in ga_xs:
        copy.wait_recv()
    value = ga_sum[x_lo, x_hi].astype(F32)
    for i in range(3):
        value = value + ga_xg[i].astype(F32)
    gp_across.wait_recv()
    gp_rows[...] = value + gp_zg[...].astype(F32)
    theirs = gp_rows.at[pl.ds(pl.multiple_of((1 - step) * 8, 8), 8), :]
    gp_swap_rows = post.send(theirs, gp_pair, pair)
    grad_in_piece(7)

    ratio_row = ratio_rows[0:1, :]
    for copy in small_copies:
        copy.wait_recv()
    for q in range(4):
        cols = slice(q * 128, (q + 1) * 128)
        r = ratio_rows[0:1, cols]
        total_dr = small_all[2 * q, 0:1, :] + small_all[2 * q + 1, 0:1, :]
        corr_col[cols, :] = column(r * r * r * total_dr * (1.0 / width_in))

    def back(k):
        cols = slice(k * 128, (k + 1) * 128)
        value = sum(
            jnp.dot(w_in[s, cols, :], d_all[s].reshape(depth, -1), preferred_element_type=F32)
            for s in range(2)
        )
        grad_hidden[:, cols] = (
            jnp.transpose(value * ratio_row)
            - corr_col[:, :1] * hidden[:, cols].astype(F32)
        ).astype(BF)

    back(0)
    back(1)
    back(2)
    back(3)
    ip_beside.wait_recv()
    for copy in ip_ys[1]:
        copy.wait_recv()
    for s in range(2):
        grad_in[s] = in_block(1, s) + ip_xg[s].astype(F32)
    gp_swap_rows.wait_recv()
    grad_out[step] = gp_rows[pl.ds(pl.multiple_of(step * 8, 8), 8), :]
    grad_out[1 - step] = gp_pair[...]
    post.close()


def finish(gh, gi, go, grad_hidden, grad_in, grad_out):
    grad_hidden[...] = gh[...]
    grad_in[...] = gi[...]
    grad_out[:, 0, :] = go[0]
    grad_out[:, 1, :] = go[1]


def shards(hidden, w_in, embedding, depth_gain, w_out, codebook_ids):
    hid_count = lax.axis_size("hid")
    seq_count = lax.axis_size("seq")
    width_in = hidden.shape[1] * hid_count
    depth = w_in.shape[2]
    entries = w_out.shape[2]
    frames, units = hidden.shape
    loss_weight = 2.0 * entries / (frames * seq_count)
    vmem = pl.BlockSpec(memory_space=pltpu.VMEM)
    anywhere = pl.BlockSpec(memory_space=pl.ANY)
    scratch = [
        ((frames, units), BF),
        ((2, units, depth), BF),
        ((entries, depth), BF),
        ((4, 2, 128, depth), BF),
        ((2, 128, depth), BF),
        ((2, 128, depth), BF),
        ((2, 2, 128, depth), BF),
        ((128, depth), BF),
        ((128, depth), BF),
        ((2, 8, entries), BF),
        ((4, 8, entries), BF),
        ((2, 4, 2, 2, 2, 16, entries), BF),
        ((8, 128), jnp.int32),
        ((2, 8, 128), jnp.int32),
        ((8, frames), F32),
        ((8, 8, frames), F32),
        ((8, frames), F32),
        ((128, 128), F32),
        ((frames, units), BF),
        ((128, depth), F32),
        ((128, depth), F32),
        ((128, depth), F32),
        ((128, depth), BF),
        ((depth, 128), BF),
        ((128, entries), F32),
        ((128, entries), BF),
        ((128, 128), F32),
        ((128, depth), F32),
        ((128, 128), F32),
        ((2, 4, 128, 128), BF),
        ((2, 2, 4, 128, frames), BF),
        ((8, 128), F32),
        ((8, 8, 128), F32),
        ((frames, 128), F32),
        ((2, 4, 2, 2, 2, 16, entries), BF),
        ((2, 4, 2, 2, 16, entries), BF),
        ((3, 2, 2, 16, entries), BF),
        ((2, 2, 16, entries), BF),
        ((2, 2, 2, 16, entries), BF),
        ((2, 2, 16, entries), BF),
        ((3, 16, entries), BF),
        ((3, 2, 2, 16, entries), BF),
        ((2, 2, 16, entries), BF),
        ((2, 2, 2, 16, entries), BF),
        ((4, 16, entries), BF),
        ((3, 16, entries), BF),
        ((16, entries), BF),
        ((16, entries), BF),
        ((16, entries), F32),
        ((8, entries), F32),
        ((2, 4, 2, 2, 64, units), BF),
        ((2, 4, 2, 64, units), BF),
        ((2, 3, 2, 64, units), BF),
        ((2, 2, 64, units), BF),
        ((2, 2, 2, 64, units), BF),
        ((2, 64, units), BF),
        ((2, 64, units), BF),
    ]
    grad_hidden, grad_in, grad_out = pl.pallas_call(
        functools.partial(kernel, loss_weight, width_in),
        out_shape=[
            jax.ShapeDtypeStruct((frames, units), BF),
            jax.ShapeDtypeStruct((2, 64, units), F32),
            jax.ShapeDtypeStruct((2, 8, entries), F32),
        ],
        in_specs=[anywhere] * 3 + [vmem] * 3,
        out_specs=[vmem] * 3,
        scratch_shapes=[pltpu.VMEM(shape, dtype) for shape, dtype in scratch]
        + [
            pltpu.SemaphoreType.DMA((4,)),
            pltpu.SemaphoreType.DMA((176,)),
            pltpu.SemaphoreType.DMA((176,)),
        ],
        compiler_params=pltpu.CompilerParams(
            collective_id=0, has_side_effects=True, vmem_limit_bytes=62 * 1024 * 1024
        ),
        name="whole",
    )(hidden, w_in, embedding[0], depth_gain, w_out, codebook_ids)
    grad_hidden, grad_in, grad_out = pl.pallas_call(
        finish,
        out_shape=[
            jax.ShapeDtypeStruct((frames, units), BF),
            jax.ShapeDtypeStruct((2, 64, units), F32),
            jax.ShapeDtypeStruct((8, 2, entries), F32),
        ],
        in_specs=[vmem] * 3,
        out_specs=[vmem] * 3,
        name="finish",
    )(grad_hidden, grad_in, grad_out)
    return grad_hidden, jnp.transpose(grad_in, (0, 2, 1)), grad_out


def solution(mesh):
    placed = (
        P("seq", "hid"),
        P(None, "hid", None),
        P(),
        P(),
        P(("seq", "hid"), None, None),
        P(None, ("seq", "hid")),
    )
    return jax.shard_map(
        shards,
        mesh=mesh,
        in_specs=placed,
        out_specs=(P("seq", "hid"), P(None, "hid", "seq"), P(("seq", "hid"), None, None)),
        check_vma=False,
    )
```

```python
import functools

import jax
import jax.numpy as jnp
from jax import lax
from jax.experimental import pallas as pl
from jax.experimental.pallas import tpu as pltpu
from jax.sharding import PartitionSpec as P

MESH = pl.DeviceIdType.MESH
BF = jnp.bfloat16
F32 = jnp.float32
NT = (((1,), (1,)), ((), ()))


def place():
    s, h = lax.axis_index("seq"), lax.axis_index("hid")
    x_lo, y, c = lax.div(s, 8), lax.rem(lax.div(s, 2), 4), lax.rem(s, 2)
    return 2 * lax.div(h, 4) + x_lo, y, lax.rem(h, 4), c


def device(x, y, z, c):
    x, y, z, c = lax.rem(x, 4), lax.rem(y, 4), lax.rem(z, 4), lax.rem(c, 2)
    return (lax.rem(x, 2) * 8 + y * 2 + c, lax.div(x, 2) * 4 + z)


def greet(peers):
    barrier = pltpu.get_barrier_semaphore()
    for peer in peers:
        pl.semaphore_signal(barrier, inc=1, device_id=peer, device_id_type=MESH)
    return lambda: pl.semaphore_wait(barrier, len(peers))


class Post:
    def __init__(self, send_sem, recv_sem):
        self.send_sem, self.recv_sem, self.copies = send_sem, recv_sem, []

    def send(self, src, dst, peer):
        i = len(self.copies)
        copy = pltpu.make_async_remote_copy(
            src_ref=src,
            dst_ref=dst,
            send_sem=self.send_sem.at[i],
            recv_sem=self.recv_sem.at[i],
            device_id=peer,
            device_id_type=MESH,
        )
        copy.start()
        self.copies.append(copy)
        return copy

    def close(self):
        for copy in self.copies:
            copy.wait_send()


def column(row):
    return jnp.transpose(jnp.broadcast_to(row, (128, 128)))


def at128(i):
    return pl.ds(pl.multiple_of(i * 128, 128), 128)


def kernel(loss_weight, width_in, hidden_in, w_in_in, embedding_in, gain_in, w_out, ids, *rest):
    grad_hidden, grad_in, grad_out = rest[:3]
    (
        hidden, w_in, embedding, part, relay, relay_sum, z_got, x_send, x_got,
        w_rows, w_got, w_full, ids_mine, ids_all,
        sq_mine, sq_all, ratio_rows, ratio_col, scaled, looked, x_rows, proj, normed, turned, logits,
        d_logit, scale_col, d_norm, dr_col, d_turn, d_all, small, small_all, corr_col,
        gp, gp_c, ga_y, ga_rel, ga_yg, ga_sum, ga_xg, gb_x, gb_rel, gb_xg, gb_sum, gb_yg,
        gp_z, gp_zg, gp_rows, gp_pair, ip, ip_c, ip_y, ip_rel, ip_yg, ip_x, ip_xg, local_sem, send_sem, recv_sem,
    ) = rest[3:]
    x, y, z, c = place()
    x_lo, x_hi, step, zh = lax.rem(x, 2), lax.div(x, 2), lax.rem(z, 2), lax.div(z, 2)
    hid = x_hi * 4 + z
    quarter = x_hi * 2 + zh
    pair = device(x, y, z + 1 - 2 * step, c)
    far = device(x + 2, y, z, c)
    twin = device(x, y, z, c + 1)
    beside = device(x + 1 - 2 * x_lo, y, z, c)
    xs = {d: device(x + d, y, z, c) for d in (1, 2, 3)}
    ys = {d: device(x, y + d, z, c) for d in (1, 2, 3)}
    zs = {d: device(x, y, z + d, c) for d in (1, 2, 3)}
    hid_peers = [device(x + dx, y, z + dz, c) for dz in (2, 1, 3, 0) for dx in (2, 0) if dx + dz]
    order = (2, 1, 3, 0)

    sources = (
        (hidden_in, hidden),
        (w_in_in.at[step], w_in.at[step]),
        (w_in_in.at[1 - step], w_in.at[1 - step]),
        (embedding_in, embedding),
    )
    loads = [
        pltpu.make_async_copy(src, dst, local_sem.at[i]) for i, (src, dst) in enumerate(sources)
    ]
    for load in loads:
        load.start()
    everyone_here = greet(hid_peers + [xs[1], xs[3]] + list(ys.values()) + [twin])
    w_rows[0] = w_out[:, 0, :]
    w_rows[1] = w_out[:, 1, :]
    ids_mine[...] = jnp.zeros_like(ids_mine)
    ids_mine[0:2, 0:64] = ids[...]
    ids_all[step] = ids_mine[...]
    w_got[z] = w_rows[step]

    def chunk(dz):
        to_z = lax.rem(z + dz, 4)
        rows = [hidden[at128(fx * 2 + lax.div(to_z, 2)), :] for fx in range(2)]
        product = jnp.dot(
            jnp.concatenate(rows, axis=0), w_in[lax.rem(to_z, 2)], preferred_element_type=F32
        ).astype(BF)
        part[dz, 0] = product[:128]
        part[dz, 1] = product[128:]

    loads[0].wait()
    loads[1].wait()
    chunk(2)
    everyone_here()
    post = Post(send_sem, recv_sem)

    bounds = ((0, 64), (64, 96), (96, 128))
    pieces = [pl.ds(a, b - a) for a, b in bounds]
    relays, z_copies = [[] for _ in pieces], [[] for _ in pieces]

    def send_opposite(p):
        rows = pieces[p]
        relays[p].append(post.send(part.at[2, 0, rows], relay.at[0, rows], zs[1]))
        relays[p].append(post.send(part.at[2, 1, rows], relay.at[1, rows], zs[3]))

    def send_direct(p, dz):
        rows, fx, slot = pieces[p], (1 if dz == 1 else 0), (0 if dz == 1 else 1)
        z_copies[p].append(post.send(part.at[dz, fx, rows], z_got.at[slot, fx, rows], zs[dz]))

    def send_sums(p):
        for fx, dz in ((0, 1), (1, 3)):
            rows = pieces[p]
            relays[p][fx].wait_recv()
            relay_sum[fx, rows, :] = (
                part[dz, fx, rows, :].astype(F32) + relay[fx, rows, :].astype(F32)
            ).astype(BF)
            z_copies[p].append(
                post.send(relay_sum.at[fx, rows], z_got.at[fx, fx, rows], zs[dz])
            )

    w_z = [post.send(w_rows.at[(step + d) % 2], w_got.at[z], zs[d]) for d in (2, 1, 3)]
    ids_swap = post.send(ids_mine, ids_all.at[step], pair)
    send_opposite(0)
    h = hidden[...].astype(F32)
    h2 = h * h
    top = h2.astype(BF)
    low = (h2 - top.astype(F32)).astype(BF)
    ones = jnp.ones((8, h2.shape[1]), BF)
    sq_mine[...] = lax.dot_general(ones, top, NT, preferred_element_type=F32) + lax.dot_general(
        ones, low, NT, preferred_element_type=F32
    )
    sq_all[hid] = sq_mine[...]
    loads[2].wait()
    chunk(1)
    send_direct(0, 1)
    sq_copies = [post.send(sq_mine, sq_all.at[hid], peer) for peer in hid_peers]
    chunk(3)
    send_direct(0, 3)
    for p in (1, 2):
        send_opposite(p)
        send_direct(p, 1)
        send_direct(p, 3)
    for copy in w_z:
        copy.wait_recv()
    for e in range(2):
        both = [w_got[2 * e + i].astype(F32) for i in range(2)]
        w_full[x_lo, y, c, x_hi, e] = jnp.concatenate(both, axis=0).astype(BF)
    block = w_full.at[x_lo, y, c, x_hi, zh]
    wa_x = [post.send(block, block, xs[d]) for d in (1, 3, 2)]
    block = w_full.at[x_lo, y, c, x_hi, 1 - zh]
    wb_y = [post.send(block, block, ys[d]) for d in (1, 3, 2)]
    chunk(0)
    send_sums(0)
    for copy in wa_x:
        copy.wait_recv()
    line = w_full.at[:, y, c, :, zh]
    wa_y = {d: post.send(line, line, ys[d]) for d in (2, 1, 3)}
    w_twin = [post.send(line, line, twin)]
    for copy in wb_y:
        copy.wait_recv()
    line = w_full.at[x_lo, :, c, x_hi, 1 - zh]
    wb_x = {d: post.send(line, line, xs[d]) for d in (2, 1, 3)}
    w_twin.append(post.send(line, line, twin))
    send_sums(1)
    send_sums(2)

    for copy in sq_copies:
        copy.wait_recv()
    squares = sq_all[0]
    for i in range(1, 8):
        squares = squares + sq_all[i]
    ratio_rows[...] = lax.rsqrt(squares / width_in + 1e-06)
    for q in range(4):
        wide = column(ratio_rows[0:1, q * 128 : (q + 1) * 128])
        scaled[q * 128 : (q + 1) * 128, :] = (
            hidden[q * 128 : (q + 1) * 128, :].astype(F32) * wide[:, :1]
        ).astype(BF)
    ratio_col[...] = column(ratio_rows[0:1, at128(quarter)])
    ids_swap.wait_recv()

    def tokens(k):
        parts = [column(ids_all[i, k : k + 1, :].astype(F32))[:64, :1] for i in range(2)]
        return jnp.concatenate(parts, axis=0).astype(jnp.int32)

    previous, current = tokens(0), tokens(1)
    target = jnp.where(step == 1, current, previous)
    entries = logits.shape[1]
    lanes = lax.broadcasted_iota(jnp.int32, (128, entries), 1)
    loads[3].wait()
    pick = jnp.where(lanes == previous, 1.0, 0.0).astype(BF)
    live = step.astype(F32)
    for n in range(2):
        cols = slice(n * 512, (n + 1) * 512)
        looked[:, cols] = jnp.dot(pick, embedding[:, cols], preferred_element_type=F32) * live

    def z_sum(fx, rows):
        return (
            part[0, fx, rows, :].astype(F32)
            + z_got[0, fx, rows, :].astype(F32)
            + z_got[1, fx, rows, :].astype(F32)
        )

    x_copies = []
    for p in range(3):
        for copy in z_copies[p]:
            copy.wait_recv()

        @pl.loop(bounds[p][0] // 16, bounds[p][1] // 16, unroll=True)
        def to_far(i):
            rows = pl.ds(pl.multiple_of(i * 16, 16), 16)
            x_send[rows, :] = z_sum(1 - x_hi, rows).astype(BF)

        x_copies.append(post.send(x_send.at[pieces[p]], x_got.at[pieces[p]], far))
    for d in (1, 3, 2):
        wa_y[d].wait_recv()
        line = w_full.at[:, lax.rem(y + 4 - d, 4), c, :, zh]
        w_twin.append(post.send(line, line, twin))
    for d in (1, 3, 2):
        wb_x[d].wait_recv()
        from_x = lax.rem(x + 4 - d, 4)
        line = w_full.at[lax.rem(from_x, 2), :, c, lax.div(from_x, 2), 1 - zh]
        w_twin.append(post.send(line, line, twin))
    gain = gain_in[pl.ds(step, 1), :]
    for p in range(3):
        x_copies[p].wait_recv()

        @pl.loop(bounds[p][0] // 16, bounds[p][1] // 16, unroll=True)
        def norm(i):
            rows = pl.ds(pl.multiple_of(i * 16, 16), 16)
            value = z_sum(x_hi, rows) + x_got[rows, :].astype(F32)
            proj[rows, :] = value
            value = ratio_col[rows, :1] * value + looked[rows, :]
            scale = lax.rsqrt(jnp.mean(value * value, axis=1, keepdims=True) + 1e-06)
            x_rows[rows, :] = value
            scale_col[rows, :] = jnp.broadcast_to(scale, (16, 128))
            normed[rows, :] = (value * scale * gain).astype(BF)

    for copy in w_twin:
        copy.wait_recv()

    depth = normed.shape[1]
    for n in range(4):
        cols = slice(n * 512, (n + 1) * 512)
        head = w_full[:, :, :, :, :, :, cols].reshape(depth, 512)
        logits[:, cols] = jnp.dot(normed[...], head, preferred_element_type=F32)
    dr_col[...] = jnp.broadcast_to(target.astype(F32), (128, 128))

    @pl.loop(0, 8, unroll=4)
    def soft(i):
        rows = pl.ds(pl.multiple_of(i * 16, 16), 16)
        value = logits[rows, :]
        value = jnp.exp(value - jnp.max(value, axis=1, keepdims=True))
        share = value * (loss_weight / jnp.sum(value, axis=1, keepdims=True))
        hot = lax.broadcasted_iota(jnp.int32, (16, entries), 1) == dr_col[rows, :1].astype(
            jnp.int32
        )
        d_logit[rows, :] = (share - jnp.where(hot, loss_weight, 0.0)).astype(BF)

    for k in range(4):
        a, b = k // 2, (k % 2) * 2
        head = w_full[a, b : b + 2].reshape(256, entries)
        d_norm[:, k * 256 : (k + 1) * 256] = lax.dot_general(
            d_logit[...], head, NT, preferred_element_type=F32
        )

    @pl.loop(0, 8, unroll=8)
    def unnorm(i):
        rows = pl.ds(pl.multiple_of(i * 16, 16), 16)
        value, scale = x_rows[rows, :], scale_col[rows, :1]
        gated = gain * d_norm[rows, :]
        inner = jnp.mean(gated * value, axis=1, keepdims=True)
        d_x = scale * gated - value * (scale * scale * scale * inner)
        d_norm[rows, :] = d_x
        total = jnp.sum(d_x * proj[rows, :], axis=1, keepdims=True)
        dr_col[rows, :] = jnp.broadcast_to(total, (16, 128))

    for k in range(8):
        d_turn[k // 4, k % 4] = jnp.transpose(d_norm[:, k * 128 : (k + 1) * 128]).astype(BF)
    lane, far_lane = at128(quarter), at128((1 - x_hi) * 2 + zh)

    def piece(k):
        return (1 - x_lo if k < 4 else x_lo), lax.rem(y + order[k % 4], 4)

    d_x_copies, d_z_copies = {}, [[] for _ in range(8)]
    for k in (0, 1, 2, 4, 5, 6):
        b, to_y = piece(k)
        d_x_copies[k] = post.send(d_turn.at[b, to_y], d_all.at[step, b, to_y, :, lane], far)

    def send_across(k):
        b, to_y = piece(k)
        for copy in d_z_copies[k]:
            copy.wait_recv()
        d_z_copies[k] = [
            post.send(d_turn.at[b, to_y], d_all.at[step, b, to_y, :, lane], far)
        ]
        for dz in (1, 2, 3):
            to_z = lax.rem(z + dz, 4)
            view = d_all.at[
                lax.rem(to_z, 2), b, to_y, :, at128(x_hi * 2 + lax.div(to_z, 2))
            ]
            d_z_copies[k].append(post.send(view, view, far))

    def send_own(k):
        b, to_y = piece(k)
        view = d_all.at[step, b, to_y, :, lane]
        d_z_copies[k] += [post.send(d_turn.at[b, to_y], view, zs[d]) for d in (2, 1, 3)]

    def send_far(k):
        b, to_y = piece(k)
        d_x_copies[k].wait_recv()
        view = d_all.at[step, b, to_y, :, far_lane]
        d_z_copies[k] += [post.send(view, view, zs[d]) for d in (2, 1, 3)]

    for k in range(3):
        send_own(k)
    small[...] = jnp.transpose(dr_col[...])[:8]
    small_copies = [post.send(small, small_all.at[hid], peer) for peer in hid_peers]
    for b in range(4):
        for a in range(2):
            d_all[step, a, b, :, lane] = d_turn[a, b]
    small_all[hid] = small[...]

    for k in range(8):
        cols = slice(k * 128, (k + 1) * 128)
        turned[cols, :] = jnp.transpose(normed[:, cols].astype(F32)).astype(BF)
    gp_swap = []

    def product_out(i):
        to_y = lax.rem(y + order[i], 4)
        for a in range(2):
            rows = at128(a * 4 + to_y)
            gp[a, to_y] = (
                jnp.dot(turned[rows, :], d_logit[...], preferred_element_type=F32)
                .astype(BF)
                .reshape(2, 2, 2, 16, entries)
            )
        gp_swap.append(post.send(gp.at[:, to_y, 1 - c], gp_c.at[:, to_y], twin))

    for i in range(4):
        product_out(i)
    def core_sum(a, b, e, f):
        return gp[a, b, c, e, f].astype(F32) + gp_c[a, b, e, f].astype(F32)

    def ga_part(i, a, more=None):
        to_y = lax.rem(y + order[i], 4)
        for e in range(2):
            value = core_sum(a, to_y, e, zh)
            if more is not None:
                value = value + ga_rel[more, e].astype(F32)
            ga_y[i, a, e] = value.astype(BF)
        return ga_y.at[i, a]

    def gb_part(i, k, more=None):
        to_x = lax.rem(x + order[i], 4)
        for b in range(2):
            value = core_sum(lax.rem(to_x, 2), 2 * k + b, lax.div(to_x, 2), 1 - zh)
            if more is not None:
                value = value + gb_rel[more, b].astype(F32)
            gb_x[i, k, b] = value.astype(BF)
        return gb_x.at[i, k]

    gp_swap[0].wait_recv()
    ga_relay = [post.send(ga_part(0, a), ga_rel.at[a], ys[d]) for a, d in ((0, 1), (1, 3))]
    gp_swap[1].wait_recv()
    ga_ys = [post.send(ga_part(1, 1), ga_yg.at[0, 1], ys[1])]
    gp_swap[2].wait_recv()
    ga_ys.append(post.send(ga_part(2, 0), ga_yg.at[1, 0], ys[3]))
    gp_swap[3].wait_recv()
    gb_relay = [post.send(gb_part(0, k), gb_rel.at[k], xs[d]) for k, d in ((0, 1), (1, 3))]
    gb_xs = [
        post.send(gb_part(1, 1), gb_xg.at[0, 1], xs[1]),
        post.send(gb_part(2, 0), gb_xg.at[1, 0], xs[3]),
    ]
    for k in range(8):
        if k % 4 != 3:
            send_far(k)
        if k < 5:
            send_own(k + 3)
    ga_relay[0].wait_recv()
    ga_ys.append(post.send(ga_part(1, 0, 0), ga_yg.at[0, 0], ys[1]))
    ga_relay[1].wait_recv()
    ga_ys.append(post.send(ga_part(2, 1, 1), ga_yg.at[1, 1], ys[3]))

    ip_ys, ip_relay = [[], []], [[], []]

    def grad_in_piece(k):
        for copy in d_z_copies[k]:
            copy.wait_recv()
        b, to_y = piece(k)
        late, i = k // 4, k % 4
        rows = [d_all[s, b, to_y] for s in range(2)]
        product = jnp.dot(
            jnp.concatenate(rows, axis=0), scaled[...], preferred_element_type=F32
        ).astype(BF)
        for s in range(2):
            for e in range(2):
                start = s * 128 + e * 64
                ip[late, to_y, e, s] = product[start : start + 64]
        swap = post.send(ip.at[late, to_y, 1 - c], ip_c.at[late, to_y], twin)
        swap.wait_recv()
        if i == 3:
            return
        if i:
            ip_relay[late][i - 1].wait_recv()
        for s in range(2):
            value = ip[late, to_y, c, s].astype(F32) + ip_c[late, to_y, s].astype(F32)
            if s == i - 1:
                value = value + ip_rel[late, s].astype(F32)
            ip_y[late, i, s] = value.astype(BF)
        if i:
            ip_ys[late].append(
                post.send(ip_y.at[late, i], ip_yg.at[late, i - 1], ys[order[i]])
            )
        else:
            for s, d in ((0, 1), (1, 3)):
                ip_relay[late].append(post.send(ip_y.at[late, 0, s], ip_rel.at[late, s], ys[d]))

    def in_block(late, s):
        value = ip[late, y, c, s].astype(F32) + ip_c[late, y, s].astype(F32)
        for i in range(2):
            value = value + ip_yg[late, i, s].astype(F32)
        return value

    grad_in_piece(0)
    gb_relay[0].wait_recv()
    gb_xs.append(post.send(gb_part(1, 0, 0), gb_xg.at[0, 0], xs[1]))
    gb_relay[1].wait_recv()
    gb_xs.append(post.send(gb_part(2, 1, 1), gb_xg.at[1, 1], xs[3]))
    send_across(3)
    grad_in_piece(1)
    grad_in_piece(2)
    for copy in ga_ys:
        copy.wait_recv()
    for a in range(2):
        for e in range(2):
            value = core_sum(a, y, e, zh)
            for i in range(2):
                value = value + ga_yg[i, a, e].astype(F32)
            ga_sum[a, e] = value.astype(BF)
    ga_xs = []
    for i, d in enumerate(order[:3]):
        to_x = lax.rem(x + d, 4)
        ga_xs.append(
            post.send(ga_sum.at[lax.rem(to_x, 2), lax.div(to_x, 2)], ga_xg.at[i], xs[d])
        )
    for copy in gb_xs:
        copy.wait_recv()
    for b in range(4):
        value = core_sum(x_lo, b, x_hi, 1 - zh)
        for i in range(2):
            value = value + gb_xg[i, b // 2, b % 2].astype(F32)
        gb_sum[b] = value.astype(BF)
    gb_ys = []
    for i, d in enumerate(order[:3]):
        gb_ys.append(post.send(gb_sum.at[lax.rem(y + d, 4)], gb_yg.at[i], ys[d]))
    grad_in_piece(3)
    send_across(7)
    grad_in_piece(4)
    for copy in ip_ys[0]:
        copy.wait_recv()
    for s in range(2):
        ip_x[s] = in_block(0, s).astype(BF)
    ip_beside = post.send(ip_x, ip_xg, beside)
    for copy in gb_ys:
        copy.wait_recv()
    value = gb_sum[y].astype(F32)
    for i in range(3):
        value = value + gb_yg[i].astype(F32)
    gp_z[...] = value.astype(BF)
    gp_across = post.send(gp_z, gp_zg, zs[2])
    grad_in_piece(5)
    grad_in_piece(6)
    for copy in ga_xs:
        copy.wait_recv()
    value = ga_sum[x_lo, x_hi].astype(F32)
    for i in range(3):
        value = value + ga_xg[i].astype(F32)
    gp_across.wait_recv()
    gp_rows[...] = value + gp_zg[...].astype(F32)
    theirs = gp_rows.at[pl.ds(pl.multiple_of((1 - step) * 8, 8), 8), :]
    gp_swap_rows = post.send(theirs, gp_pair, pair)
    grad_in_piece(7)

    ratio_row = ratio_rows[0:1, :]
    for copy in small_copies:
        copy.wait_recv()
    for q in range(4):
        cols = slice(q * 128, (q + 1) * 128)
        r = ratio_rows[0:1, cols]
        total_dr = small_all[2 * q, 0:1, :] + small_all[2 * q + 1, 0:1, :]
        corr_col[cols, :] = column(r * r * r * total_dr * (1.0 / width_in))

    def back(k):
        cols = slice(k * 128, (k + 1) * 128)
        value = sum(
            jnp.dot(w_in[s, cols, :], d_all[s].reshape(depth, -1), preferred_element_type=F32)
            for s in range(2)
        )
        grad_hidden[:, cols] = (
            jnp.transpose(value * ratio_row)
            - corr_col[:, :1] * hidden[:, cols].astype(F32)
        ).astype(BF)

    back(0)
    back(1)
    back(2)
    back(3)
    ip_beside.wait_recv()
    for copy in ip_ys[1]:
        copy.wait_recv()
    for s in range(2):
        grad_in[s] = in_block(1, s) + ip_xg[s].astype(F32)
    gp_swap_rows.wait_recv()
    grad_out[step] = gp_rows[pl.ds(pl.multiple_of(step * 8, 8), 8), :]
    grad_out[1 - step] = gp_pair[...]
    post.close()


def finish(gh, gi, go, grad_hidden, grad_in, grad_out):
    grad_hidden[...] = gh[...]
    grad_in[...] = gi[...]
    grad_out[:, 0, :] = go[0]
    grad_out[:, 1, :] = go[1]


def shards(hidden, w_in, embedding, depth_gain, w_out, codebook_ids):
    hid_count = lax.axis_size("hid")
    seq_count = lax.axis_size("seq")
    width_in = hidden.shape[1] * hid_count
    depth = w_in.shape[2]
    entries = w_out.shape[2]
    frames, units = hidden.shape
    loss_weight = 2.0 * entries / (frames * seq_count)
    vmem = pl.BlockSpec(memory_space=pltpu.VMEM)
    anywhere = pl.BlockSpec(memory_space=pl.ANY)
    scratch = [
        ((frames, units), BF),
        ((2, units, depth), BF),
        ((entries, depth), BF),
        ((4, 2, 128, depth), BF),
        ((2, 128, depth), BF),
        ((2, 128, depth), BF),
        ((2, 2, 128, depth), BF),
        ((128, depth), BF),
        ((128, depth), BF),
        ((2, 8, entries), BF),
        ((4, 8, entries), BF),
        ((2, 4, 2, 2, 2, 16, entries), BF),
        ((8, 128), jnp.int32),
        ((2, 8, 128), jnp.int32),
        ((8, frames), F32),
        ((8, 8, frames), F32),
        ((8, frames), F32),
        ((128, 128), F32),
        ((frames, units), BF),
        ((128, depth), F32),
        ((128, depth), F32),
        ((128, depth), F32),
        ((128, depth), BF),
        ((depth, 128), BF),
        ((128, entries), F32),
        ((128, entries), BF),
        ((128, 128), F32),
        ((128, depth), F32),
        ((128, 128), F32),
        ((2, 4, 128, 128), BF),
        ((2, 2, 4, 128, frames), BF),
        ((8, 128), F32),
        ((8, 8, 128), F32),
        ((frames, 128), F32),
        ((2, 4, 2, 2, 2, 16, entries), BF),
        ((2, 4, 2, 2, 16, entries), BF),
        ((3, 2, 2, 16, entries), BF),
        ((2, 2, 16, entries), BF),
        ((2, 2, 2, 16, entries), BF),
        ((2, 2, 16, entries), BF),
        ((3, 16, entries), BF),
        ((3, 2, 2, 16, entries), BF),
        ((2, 2, 16, entries), BF),
        ((2, 2, 2, 16, entries), BF),
        ((4, 16, entries), BF),
        ((3, 16, entries), BF),
        ((16, entries), BF),
        ((16, entries), BF),
        ((16, entries), F32),
        ((8, entries), F32),
        ((2, 4, 2, 2, 64, units), BF),
        ((2, 4, 2, 64, units), BF),
        ((2, 3, 2, 64, units), BF),
        ((2, 2, 64, units), BF),
        ((2, 2, 2, 64, units), BF),
        ((2, 64, units), BF),
        ((2, 64, units), BF),
    ]
    grad_hidden, grad_in, grad_out = pl.pallas_call(
        functools.partial(kernel, loss_weight, width_in),
        out_shape=[
            jax.ShapeDtypeStruct((frames, units), BF),
            jax.ShapeDtypeStruct((2, 64, units), F32),
            jax.ShapeDtypeStruct((2, 8, entries), F32),
        ],
        in_specs=[anywhere] * 3 + [vmem] * 3,
        out_specs=[vmem] * 3,
        scratch_shapes=[pltpu.VMEM(shape, dtype) for shape, dtype in scratch]
        + [
            pltpu.SemaphoreType.DMA((4,)),
            pltpu.SemaphoreType.DMA((176,)),
            pltpu.SemaphoreType.DMA((176,)),
        ],
        compiler_params=pltpu.CompilerParams(
            collective_id=0, has_side_effects=True, vmem_limit_bytes=62 * 1024 * 1024
        ),
        name="whole",
    )(hidden, w_in, embedding[0], depth_gain, w_out, codebook_ids)
    grad_hidden, grad_in, grad_out = pl.pallas_call(
        finish,
        out_shape=[
            jax.ShapeDtypeStruct((frames, units), BF),
            jax.ShapeDtypeStruct((2, 64, units), F32),
            jax.ShapeDtypeStruct((8, 2, entries), F32),
        ],
        in_specs=[vmem] * 3,
        out_specs=[vmem] * 3,
        name="finish",
    )(grad_hidden, grad_in, grad_out)
    return grad_hidden, jnp.transpose(grad_in, (0, 2, 1)), grad_out


def solution(mesh):
    placed = (
        P("seq", "hid"),
        P(None, "hid", None),
        P(),
        P(),
        P(("seq", "hid"), None, None),
        P(None, ("seq", "hid")),
    )
    return jax.shard_map(
        shards,
        mesh=mesh,
        in_specs=placed,
        out_specs=(P("seq", "hid"), P(None, "hid", "seq"), P(("seq", "hid"), None, None)),
        check_vma=False,
    )
```
